64 devices in a mesh: dp: 4 (over x, y), sp: 16 (over z, core).
Axes of the slice: x: 2, y: 2, z: 8, core: 2. Of those that a mesh axis runs over, the one named last changes fastest.
The devices are a block of a 4x4x8 slice.
Arguments:
- signal: bfloat16 [16, 1024, 512], P('dp', 'sp'), parts along dimension 0
- cond_feats: bfloat16 [16, 1024, 128], P('dp', 'sp'), parts along dimension 0
- w_now: bfloat16 [10, 512, 1024], replicated
- w_past: bfloat16 [10, 512, 1024], replicated
- w_cond: bfloat16 [10, 128, 1024], replicated
- b_gate: float32 [10, 1024], replicated
- w_res: bfloat16 [10, 512, 512], replicated
- w_skip: bfloat16 [10, 512, 256], replicated
Outputs:
- output 1: float32 [16, 1024, 512], P('dp', 'sp'), parts along dimension 0
- output 2: float32 [16, 1024, 256], P('dp', 'sp'), parts along dimension 0
There are 4 independent parts. The reference program is written for one: setup_inputs(seed, part) draws one part's arguments, and reference() takes and returns one part's arrays. A program takes and returns all parts, laid end to end along the dimension named above; an argument that names none is the same for every part.
All inputs are finite; a program needn't handle non-finite values.
Results may differ from the reference program's by a relative error of at most 0.00672435.
Values are sent between devices in bfloat16 or wider.
A program may use at most 768 MiB of HBM per device.

```python
import jax
import jax.numpy as jnp

BATCH = 4
SEQ_LEN = 1024
CHANNELS = 512
SKIP_CH = 256
COND_CH = 128
LAYERS = 10


def setup_inputs(seed: int = 0, part: int = 0) -> dict:
    part_key = jax.random.fold_in(jax.random.key(seed), part)
    sig_key, cond_key = jax.random.split(part_key, 2)
    weight_keys = jax.random.split(jax.random.key(seed + 1), 6)
    gate_scale = (2 * CHANNELS + COND_CH) ** -0.5
    out_scale = CHANNELS ** -0.5
    signal = jax.random.normal(sig_key, (BATCH, SEQ_LEN, CHANNELS), jnp.float32)
    cond_feats = jax.random.normal(cond_key, (BATCH, SEQ_LEN, COND_CH), jnp.float32)
    w_now = jax.random.normal(weight_keys[0], (LAYERS, CHANNELS, 2 * CHANNELS), jnp.float32) * gate_scale
    w_past = jax.random.normal(weight_keys[1], (LAYERS, CHANNELS, 2 * CHANNELS), jnp.float32) * gate_scale
    w_cond = jax.random.normal(weight_keys[2], (LAYERS, COND_CH, 2 * CHANNELS), jnp.float32) * gate_scale
    b_gate = 0.5 * jax.random.normal(weight_keys[3], (LAYERS, 2 * CHANNELS), jnp.float32)
    w_res = jax.random.normal(weight_keys[4], (LAYERS, CHANNELS, CHANNELS), jnp.float32) * out_scale
    w_skip = jax.random.normal(weight_keys[5], (LAYERS, CHANNELS, SKIP_CH), jnp.float32) * out_scale
    return {
        'signal': signal.astype(jnp.bfloat16),
        'cond_feats': cond_feats.astype(jnp.bfloat16),
        'w_now': w_now.astype(jnp.bfloat16),
        'w_past': w_past.astype(jnp.bfloat16),
        'w_cond': w_cond.astype(jnp.bfloat16),
        'b_gate': b_gate,
        'w_res': w_res.astype(jnp.bfloat16),
        'w_skip': w_skip.astype(jnp.bfloat16),
    }


def reference(signal, cond_feats, w_now, w_past, w_cond, b_gate, w_res, w_skip):
    resid = signal.astype(jnp.float32)
    skip_sum = jnp.zeros((BATCH, SEQ_LEN, SKIP_CH), jnp.float32)
    cond_wide = cond_feats.astype(jnp.float32)
    for layer in range(LAYERS):
        dilation = 2 ** layer
        now_in = resid.astype(jnp.bfloat16)
        past_in = jnp.concatenate([jnp.zeros((BATCH, dilation, CHANNELS), jnp.bfloat16), now_in[:, :SEQ_LEN - dilation]], axis=1)
        gate_pre = (jnp.einsum('bsc,cg->bsg', now_in.astype(jnp.float32), w_now[layer].astype(jnp.float32))
                    + jnp.einsum('bsc,cg->bsg', past_in.astype(jnp.float32), w_past[layer].astype(jnp.float32))
                    + jnp.einsum('bsc,cg->bsg', cond_wide, w_cond[layer].astype(jnp.float32))
                    + b_gate[layer])
        gated = (jnp.tanh(gate_pre[..., :CHANNELS]) * jax.nn.sigmoid(gate_pre[..., CHANNELS:])).astype(jnp.bfloat16)
        gated_wide = gated.astype(jnp.float32)
        resid = resid + jnp.einsum('bsc,cd->bsd', gated_wide, w_res[layer].astype(jnp.float32))
        skip_sum = skip_sum + jnp.einsum('bsc,cd->bsd', gated_wide, w_skip[layer].astype(jnp.float32))
    return resid, skip_sum
```

```python
import functools

import jax
import jax.numpy as jnp
from jax import lax
from jax.experimental import pallas as pl
from jax.experimental.pallas import tpu as pltpu
from jax.sharding import PartitionSpec as P

MESH = pl.DeviceIdType.MESH
NEAR = 3
RES = 2 ** NEAR
HALO = 16
f32, bf16 = jnp.float32, jnp.bfloat16


def _iota(shape, dim):
    return lax.broadcasted_iota(jnp.int32, shape, dim)


def _kernel(n, sig_hbm, cond_hbm, wn_hbm, wp_hbm, wc_hbm, bg_hbm, wr_hbm, ws_hbm,
            hout_hbm, sout_hbm,
            sig_v, cond_v, halo_s, halo_c, w1, w2, bias,
            hsend, skip0, csend, crecv, hs, orecv, obuf,
            w_sem, in_sem, halo_send, halo_recv, c_send, c_recv, h_send, h_recv, o_send, o_recv, out_sem):
    me = lax.axis_index("sp")
    batch, span, ch = sig_v.shape
    cch = cond_v.shape[2]
    layers = w1.shape[0]
    own = batch * span
    per = span // RES
    ncls = batch * RES
    chunks = ncls // n
    rows = n * per
    wide = w2.shape[2]
    hrows = batch * RES

    ins = [pltpu.make_async_copy(sig_hbm, sig_v, in_sem.at[0]),
           pltpu.make_async_copy(cond_hbm, cond_v, in_sem.at[1]),
           pltpu.make_async_copy(bg_hbm, bias, in_sem.at[2])]
    for c in ins:
        c.start()

    def wcopies(k):
        return [pltpu.make_async_copy(wn_hbm.at[k], w1.at[k, pl.ds(0, ch)], w_sem.at[k, 0]),
                pltpu.make_async_copy(wp_hbm.at[k], w1.at[k, pl.ds(ch, ch)], w_sem.at[k, 1]),
                pltpu.make_async_copy(wc_hbm.at[k], w1.at[k, pl.ds(2 * ch, cch)], w_sem.at[k, 2]),
                pltpu.make_async_copy(wr_hbm.at[k], w2.at[k, :, pl.ds(0, ch)], w_sem.at[k, 3]),
                pltpu.make_async_copy(ws_hbm.at[k], w2.at[k, :, pl.ds(ch, wide - ch)], w_sem.at[k, 4])]

    for k in range(layers):
        for c in wcopies(k):
            c.start()

    barrier = pltpu.get_barrier_semaphore()
    for d in range(1, n):
        pl.semaphore_signal(barrier, inc=1, device_id={"sp": lax.rem(me + d, n)}, device_id_type=MESH)

    ins[0].wait()
    ins[1].wait()
    sig = sig_v[...].reshape(own, ch)
    cnd = cond_v[...].reshape(own, cch)

    r, c = _iota((own, own), 0), _iota((own, own), 1)
    sh_span = span.bit_length() - 1
    sh_per = per.bit_length() - 1
    seq, rho, step = r >> sh_span, (r >> sh_per) & (RES - 1), r & (per - 1)
    perm = (c == seq * span + step * RES + rho).astype(bf16)
    csend[...] = jnp.dot(perm, cnd, preferred_element_type=f32).astype(bf16)
    hsend[...] = jnp.dot(perm, sig, preferred_element_type=f32)

    pl.semaphore_wait(barrier, n - 1)

    def halo_copies():
        nxt = lax.rem(me + 1, n)
        return [pltpu.make_async_remote_copy(sig_v.at[:, pl.ds(span - HALO, HALO)], halo_s, halo_send.at[0],
                                             halo_recv.at[0], device_id={"sp": nxt}, device_id_type=MESH),
                pltpu.make_async_remote_copy(cond_v.at[:, pl.ds(span - HALO, HALO)], halo_c, halo_send.at[1],
                                             halo_recv.at[1], device_id={"sp": nxt}, device_id_type=MESH)]

    for cp in halo_copies():
        cp.start()

    order = [n // 2]
    for d in range(n // 2 - 1, 0, -1):
        order += [n - d, d]
    order += [0]
    crow = chunks * per

    def push(src, dst, send_sem, recv_sem, d, to):
        if d == 0:
            pltpu.make_async_copy(src, dst, recv_sem).start()
        else:
            pltpu.make_async_remote_copy(src, dst, send_sem, recv_sem, device_id={"sp": to},
                                         device_id_type=MESH).start()

    for d in order:
        to = lax.rem(me + d, n)
        push(csend.at[pl.ds(pl.multiple_of(to * crow, crow), crow)], crecv.at[me], c_send, c_recv, d, to)

    for cp in halo_copies():
        cp.wait_recv()
    ins[2].wait()

    hr, hc = _iota((hrows, batch * HALO), 0), _iota((hrows, batch * HALO), 1)
    sh_res = NEAR
    pick = (hc == (hr >> sh_res) * HALO + (HALO - RES) + (hr & (RES - 1))).astype(bf16)
    live = me > 0
    halo_h = jnp.dot(pick, halo_s[...].reshape(batch * HALO, ch), preferred_element_type=f32)
    halo_k = jnp.dot(pick, halo_c[...].reshape(batch * HALO, cch), preferred_element_type=f32).astype(bf16)
    call = jnp.concatenate([csend[...], halo_k], axis=0)
    allr = own + hrows
    half = ch // 2

    def gate(x, k):
        parts = []
        for q in range(2):
            zf = jnp.dot(x, w1[k, :, q * half:(q + 1) * half], preferred_element_type=f32)
            zg = jnp.dot(x, w1[k, :, ch + q * half:ch + (q + 1) * half], preferred_element_type=f32)
            zf = zf + bias[k:k + 1, q * half:(q + 1) * half]
            zg = zg + bias[k:k + 1, ch + q * half:ch + (q + 1) * half]
            parts.append((jnp.tanh(zf) * (0.5 * jnp.tanh(0.5 * zg) + 0.5)).astype(bf16))
        return jnp.concatenate(parts, axis=1)

    for k in range(NEAR):
        d = 2 ** k
        u_own = hsend[...].astype(bf16)
        u_halo = jnp.where(live, halo_h, 0.0).astype(bf16)
        u = jnp.concatenate([u_own, u_halo], axis=0)
        r, c = _iota((allr, allr), 0), _iota((allr, allr), 1)
        seq, rho, step = r >> sh_span, (r >> sh_per) & (RES - 1), r & (per - 1)
        src = step * RES + rho - d
        own_col = seq * span + ((src & (RES - 1)) << sh_per) + (src >> NEAR)
        halo_col = own + seq * RES + src + RES
        col = jnp.where(src >= 0, own_col, halo_col)
        hseq, hrho = (r - own) >> sh_res, (r - own) & (RES - 1)
        col = jnp.where(r < own, col, jnp.where(hrho >= d, own + hseq * RES + hrho - d, -1))
        p = jnp.dot((c == col).astype(bf16), u, preferred_element_type=f32).astype(bf16)
        for cp in wcopies(k):
            cp.wait()
        a = gate(jnp.concatenate([u, p, call], axis=1), k)
        dlt = jnp.dot(a, w2[k], preferred_element_type=f32)
        hsend[...] += dlt[:own, :ch]
        if k == 0:
            skip0[...] = dlt[:own, ch:]
        else:
            skip0[...] += dlt[:own, ch:]
        if k < NEAR - 1:
            halo_h = halo_h + dlt[own:, :ch]

    for ck in range(chunks):
        for d in order:
            to = lax.rem(me + d, n)
            push(hsend.at[pl.ds(pl.multiple_of((to * chunks + ck) * per, per), per)],
                 hs.at[ck, pl.ds(pl.multiple_of(me * per, per), per), pl.ds(0, ch)],
                 h_send, h_recv.at[ck], d, to)

    pltpu.make_async_copy(crecv, crecv, c_recv).wait()
    for k in range(NEAR, layers):
        for cp in wcopies(k):
            cp.wait()

    row = _iota((rows, ch), 0)
    for ck in range(chunks):
        pltpu.make_async_copy(hs.at[ck, :, pl.ds(0, ch)], hs.at[ck, :, pl.ds(0, ch)], h_recv.at[ck]).wait()
        cq = crecv[...].astype(f32)[:, ck * per:(ck + 1) * per].reshape(rows, cch).astype(bf16)
        for k in range(NEAR, layers):
            sft = 2 ** (k - NEAR)
            h = hs[ck, :, 0:ch]
            if sft < 8:
                past = jnp.where(row >= sft, pltpu.roll(h, sft, 0), 0.0)
            else:
                past = jnp.concatenate([jnp.zeros((sft, ch), f32), h[:rows - sft]], axis=0)
            a = gate(jnp.concatenate([h.astype(bf16), past.astype(bf16), cq], axis=1), k)
            dlt = jnp.dot(a, w2[k], preferred_element_type=f32)
            if k == NEAR:
                hs[ck, :, 0:ch] = h + dlt[:, :ch]
                hs[ck, :, ch:wide] = dlt[:, ch:]
            else:
                hs[ck] += dlt
        for d in order:
            to = lax.rem(me + d, n)
            push(hs.at[ck, pl.ds(pl.multiple_of(to * per, per), per)], orecv.at[ck, me],
                 o_send, o_recv.at[ck], d, to)

    for ck in range(chunks):
        pltpu.make_async_copy(orecv.at[ck], orecv.at[ck], o_recv.at[ck]).wait()
        for j in range(n):
            cl = j * chunks + ck
            s, rho = cl // RES, cl % RES
            blk = orecv[ck, j]
            blk = jnp.concatenate([blk[:, :ch], blk[:, ch:] + skip0[cl * per:(cl + 1) * per, :]], axis=1)
            for t in range(wide // 128):
                obuf[t, pl.ds(s * span + rho, per, RES), :] = blk[:, t * 128:(t + 1) * 128]

    outs = []
    for t in range(wide // 128):
        dst = hout_hbm.at[:, pl.ds(t * 128, 128)] if t * 128 < ch else sout_hbm.at[:, pl.ds(t * 128 - ch, 128)]
        outs.append(pltpu.make_async_copy(obuf.at[t], dst, out_sem.at[t]))
        outs[-1].start()
    for cp in outs:
        cp.wait()

    for cp in halo_copies():
        cp.wait_send()
    for buf, sem in ((csend.at[pl.ds(0, own - crow)], c_send), (hsend.at[pl.ds(0, own - crow)], h_send),
                     (hs.at[:, pl.ds(0, rows - per)], o_send)):
        pltpu.make_async_copy(buf, buf, sem).wait()


def solution(mesh):
    n = mesh.shape['sp']

    def local_stack(signal, cond_feats, w_now, w_past, w_cond, b_gate, w_res, w_skip):
        batch, span, ch = signal.shape
        cch = cond_feats.shape[2]
        layers = w_now.shape[0]
        sk = w_skip.shape[2]
        wide = ch + sk
        own = batch * span
        per = span // RES
        chunks = batch * RES // n
        rows = n * per
        any_spec = pl.BlockSpec(memory_space=pl.ANY)
        dma = pltpu.SemaphoreType.DMA
        h_out, skip_out = pl.pallas_call(
            functools.partial(_kernel, n),
            name="stack",
            out_shape=(jax.ShapeDtypeStruct((own, ch), f32), jax.ShapeDtypeStruct((own, sk), f32)),
            in_specs=[any_spec] * 8,
            out_specs=(any_spec, any_spec),
            scratch_shapes=[
                pltpu.VMEM((batch, span, ch), bf16), pltpu.VMEM((batch, span, cch), bf16),
                pltpu.VMEM((batch, HALO, ch), bf16), pltpu.VMEM((batch, HALO, cch), bf16),
                pltpu.VMEM((layers, 2 * ch + cch, 2 * ch), bf16), pltpu.VMEM((layers, ch, wide), bf16),
                pltpu.VMEM((layers, 2 * ch), f32),
                pltpu.VMEM((own, ch), f32), pltpu.VMEM((own, sk), f32),
                pltpu.VMEM((own, cch), bf16), pltpu.VMEM((n, chunks * per, cch), bf16),
                pltpu.VMEM((chunks, rows, wide), f32), pltpu.VMEM((chunks, n, per, wide), f32),
                pltpu.VMEM((wide // 128, own, 128), f32),
                dma((layers, 5)), dma((3,)), dma((2,)), dma((2,)), dma, dma, dma, dma((chunks,)), dma, dma((chunks,)), dma((wide // 128,)),
            ],
            compiler_params=pltpu.CompilerParams(collective_id=0, has_side_effects=True,
                                                 vmem_limit_bytes=60 * 1024 * 1024),
        )(signal, cond_feats, w_now, w_past, w_cond, b_gate, w_res, w_skip)
        return h_out.reshape(batch, span, ch), skip_out.reshape(batch, span, sk)

    seq_spec = P('dp', 'sp', None)
    return jax.shard_map(local_stack, mesh=mesh,
                         in_specs=(seq_spec, seq_spec, P(), P(), P(), P(), P(), P()),
                         out_specs=(seq_spec, seq_spec), check_vma=False)
```

```python
import functools

import jax
import jax.numpy as jnp
from jax import lax
from jax.experimental import pallas as pl
from jax.experimental.pallas import tpu as pltpu
from jax.sharding import PartitionSpec as P

MESH = pl.DeviceIdType.MESH
NEAR = 3
RES = 2 ** NEAR
HALO = 16
f32, bf16 = jnp.float32, jnp.bfloat16
TRAVEL = f32


def _iota(shape, dim):
    return lax.broadcasted_iota(jnp.int32, shape, dim)


def _stack(n, sig_hbm, cond_hbm, wn_hbm, wp_hbm, wc_hbm, bg_hbm, wr_hbm, ws_hbm,
           recv_hbm, h3_hbm, s3_hbm,
           sig_v, cond_v, halo_s, halo_c, w1, w2, bias,
           near, ssend, csend, dsend, h3, srecv, crecv, drecv, far, osend,
           w_sem, in_sem, halo_send, halo_recv, x_send, x_recv, d_send, d_recv, o_send, o_recv, out_sem):
    me = lax.axis_index("sp")
    batch, span, ch = sig_v.shape
    cch = cond_v.shape[2]
    layers = w1.shape[0]
    own = batch * span
    per = span // RES
    ncls = batch * RES
    chunks = ncls // n
    rows = n * per
    wide = w2.shape[2]
    hrows = batch * RES
    sh_span, sh_per = span.bit_length() - 1, per.bit_length() - 1

    ins = [pltpu.make_async_copy(sig_hbm, sig_v, in_sem.at[0]),
           pltpu.make_async_copy(cond_hbm, cond_v, in_sem.at[1]),
           pltpu.make_async_copy(bg_hbm, bias, in_sem.at[2])]
    for c in ins:
        c.start()

    def wcopies(k):
        return [pltpu.make_async_copy(wn_hbm.at[k], w1.at[k, pl.ds(0, ch)], w_sem.at[k, 0]),
                pltpu.make_async_copy(wp_hbm.at[k], w1.at[k, pl.ds(ch, ch)], w_sem.at[k, 1]),
                pltpu.make_async_copy(wc_hbm.at[k], w1.at[k, pl.ds(2 * ch, cch)], w_sem.at[k, 2]),
                pltpu.make_async_copy(wr_hbm.at[k], w2.at[k, :, pl.ds(0, ch)], w_sem.at[k, 3]),
                pltpu.make_async_copy(ws_hbm.at[k], w2.at[k, :, pl.ds(ch, wide - ch)], w_sem.at[k, 4])]

    for k in range(layers):
        for c in wcopies(k):
            c.start()

    barrier = pltpu.get_barrier_semaphore()
    for d in range(1, n):
        pl.semaphore_signal(barrier, inc=1, device_id={"sp": lax.rem(me + d, n)}, device_id_type=MESH)

    ins[0].wait()
    ins[1].wait()
    r, c = _iota((own, own), 0), _iota((own, own), 1)
    seq, rho, step = r >> sh_span, (r >> sh_per) & (RES - 1), r & (per - 1)
    perm = (c == seq * span + step * RES + rho).astype(bf16)
    cnd = jnp.dot(perm, cond_v[...].reshape(own, cch), preferred_element_type=f32)
    sig = jnp.dot(perm, sig_v[...].reshape(own, ch), preferred_element_type=f32)
    csend[...] = cnd.reshape(n, chunks, per, cch).astype(bf16)
    ssend[...] = sig.reshape(n, chunks, per, ch).astype(bf16)
    h3[...] = sig

    pl.semaphore_wait(barrier, n - 1)

    def halo_copies():
        nxt = lax.rem(me + 1, n)
        return [pltpu.make_async_remote_copy(sig_v.at[:, pl.ds(span - HALO, HALO)], halo_s, halo_send.at[0],
                                             halo_recv.at[0], device_id={"sp": nxt}, device_id_type=MESH),
                pltpu.make_async_remote_copy(cond_v.at[:, pl.ds(span - HALO, HALO)], halo_c, halo_send.at[1],
                                             halo_recv.at[1], device_id={"sp": nxt}, device_id_type=MESH)]

    for cp in halo_copies():
        cp.start()

    order = [n // 2]
    for d in range(n // 2 - 1, 0, -1):
        order += [n - d, d]
    order += [0]

    def push(src, dst, send_sem, recv_sem, d, to):
        if d == 0:
            pltpu.make_async_copy(src, dst, recv_sem).start()
        else:
            pltpu.make_async_remote_copy(src, dst, send_sem, recv_sem, device_id={"sp": to},
                                         device_id_type=MESH).start()

    def drain(buf, sem):
        pltpu.make_async_copy(buf, buf, sem).wait()

    for d in order:
        to = lax.rem(me + d, n)
        push(ssend.at[to], srecv.at[me], x_send.at[0], x_recv.at[0], d, to)
        push(csend.at[to], crecv.at[me], x_send.at[1], x_recv.at[1], d, to)

    for cp in halo_copies():
        cp.wait_recv()
    ins[2].wait()

    hr, hc = _iota((hrows, batch * HALO), 0), _iota((hrows, batch * HALO), 1)
    pick = (hc == (hr >> NEAR) * HALO + (HALO - RES) + (hr & (RES - 1))).astype(bf16)
    live = me > 0
    halo_h = jnp.dot(pick, halo_s[...].reshape(batch * HALO, ch), preferred_element_type=f32)
    halo_k = jnp.dot(pick, halo_c[...].reshape(batch * HALO, cch), preferred_element_type=f32)
    call = jnp.concatenate([cnd, halo_k], axis=0).astype(bf16)
    allr = own + hrows
    half = ch // 2

    def gate(x, k):
        parts = []
        for q in range(2):
            zf = jnp.dot(x, w1[k, :, q * half:(q + 1) * half], preferred_element_type=f32)
            zg = jnp.dot(x, w1[k, :, ch + q * half:ch + (q + 1) * half], preferred_element_type=f32)
            zf = zf + bias[k:k + 1, q * half:(q + 1) * half]
            zg = zg + bias[k:k + 1, ch + q * half:ch + (q + 1) * half]
            parts.append((jnp.tanh(zf) * (0.5 * jnp.tanh(0.5 * zg) + 0.5)).astype(bf16))
        return jnp.concatenate(parts, axis=1)

    for k in range(NEAR):
        d = 2 ** k
        u_halo = jnp.where(live, halo_h, 0.0)
        u = jnp.concatenate([h3[...], u_halo], axis=0).astype(bf16)
        r, c = _iota((allr, allr), 0), _iota((allr, allr), 1)
        seq, rho, step = r >> sh_span, (r >> sh_per) & (RES - 1), r & (per - 1)
        src = step * RES + rho - d
        own_col = seq * span + ((src & (RES - 1)) << sh_per) + (src >> NEAR)
        halo_col = own + seq * RES + src + RES
        col = jnp.where(src >= 0, own_col, halo_col)
        hseq, hrho = (r - own) >> NEAR, (r - own) & (RES - 1)
        col = jnp.where(r < own, col, jnp.where(hrho >= d, own + hseq * RES + hrho - d, -1))
        p = jnp.dot((c == col).astype(bf16), u, preferred_element_type=f32).astype(bf16)
        for cp in wcopies(k):
            cp.wait()
        a = gate(jnp.concatenate([u, p, call], axis=1), k)
        dlt = jnp.dot(a, w2[k], preferred_element_type=f32)
        if k == 0:
            near[...] = dlt[:own]
        else:
            near[...] += dlt[:own]
        h3[...] += dlt[:own, :ch]
        if k < NEAR - 1:
            halo_h = halo_h + dlt[own:, :ch]

    dsend[...] = near[:, 0:ch].reshape(n, chunks, per, ch).astype(TRAVEL)
    for ck in range(chunks):
        for d in order:
            to = lax.rem(me + d, n)
            push(dsend.at[to, ck], drecv.at[ck, me], d_send, d_recv.at[ck], d, to)

    outs = [pltpu.make_async_copy(h3, h3_hbm, out_sem.at[0]),
            pltpu.make_async_copy(near.at[:, pl.ds(ch, wide - ch)], s3_hbm, out_sem.at[1])]
    for cp in outs:
        cp.start()

    drain(srecv, x_recv.at[0])
    drain(crecv, x_recv.at[1])
    for k in range(NEAR, layers):
        for cp in wcopies(k):
            cp.wait()

    row = _iota((rows, ch), 0)
    for ck in range(chunks):
        drain(drecv.at[ck], d_recv.at[ck])
        base = (srecv[:, ck].astype(f32) + drecv[ck].astype(f32)).reshape(rows, ch)
        cq = crecv[:, ck].astype(f32).reshape(rows, cch).astype(bf16)
        h = base
        for k in range(NEAR, layers):
            sft = 2 ** (k - NEAR)
            if k > NEAR:
                h = base + far[:, 0:ch]
            if sft < 8:
                past = jnp.where(row >= sft, pltpu.roll(h, sft, 0), 0.0)
            else:
                past = jnp.concatenate([jnp.zeros((sft, ch), f32), h[:rows - sft]], axis=0)
            a = gate(jnp.concatenate([h.astype(bf16), past.astype(bf16), cq], axis=1), k)
            dlt = jnp.dot(a, w2[k], preferred_element_type=f32)
            if k == NEAR:
                far[...] = dlt
            elif k < layers - 1:
                far[...] += dlt
            else:
                osend[ck] = (far[...] + dlt).reshape(n, per, wide).astype(TRAVEL)
        for d in order:
            to = lax.rem(me + d, n)
            push(osend.at[ck, to], recv_hbm.at[ck, me], o_send, o_recv.at[ck], d, to)

    for cp in halo_copies():
        cp.wait_send()
    for cp in outs:
        cp.wait()
    for buf, sem in ((ssend.at[pl.ds(0, n - 1)], x_send.at[0]), (csend.at[pl.ds(0, n - 1)], x_send.at[1]),
                     (dsend.at[pl.ds(0, n - 1)], d_send), (osend.at[:, pl.ds(0, n - 1)], o_send)):
        drain(buf, sem)
    for ck in range(chunks):
        drain(recv_hbm.at[ck], o_recv.at[ck])


def _finish(recv_hbm, h3_hbm, s3_hbm, hout_hbm, sout_hbm, recv, h3, s3, obuf, in_sem, out_sem):
    chunks, n, per, wide = recv.shape
    own, ch = h3.shape
    span = per * RES
    ins = [pltpu.make_async_copy(h3_hbm, h3, in_sem.at[0]), pltpu.make_async_copy(s3_hbm, s3, in_sem.at[1]),
           pltpu.make_async_copy(recv_hbm, recv, in_sem.at[2])]
    for cp in ins:
        cp.start()
    for cp in ins:
        cp.wait()
    outs = []
    for t in range(wide // 128):
        lo = t * 128
        base, off = (h3, lo) if lo < ch else (s3, lo - ch)
        for ck in range(chunks):
            for j in range(n):
                cl = j * chunks + ck
                s, rho = cl // RES, cl % RES
                obuf[t, pl.ds(s * span + rho, per, RES), :] = (
                    recv[ck, j, :, lo:lo + 128].astype(f32) + base[cl * per:(cl + 1) * per, off:off + 128])
        dst = hout_hbm if lo < ch else sout_hbm
        outs.append(pltpu.make_async_copy(obuf.at[t], dst.at[:, pl.ds(off, 128)], out_sem.at[t]))
        outs[-1].start()
    for cp in outs:
        cp.wait()


def solution(mesh):
    n = mesh.shape['sp']

    def local_stack(signal, cond_feats, w_now, w_past, w_cond, b_gate, w_res, w_skip):
        batch, span, ch = signal.shape
        cch = cond_feats.shape[2]
        layers = w_now.shape[0]
        sk = w_skip.shape[2]
        wide = ch + sk
        own = batch * span
        per = span // RES
        chunks = batch * RES // n
        rows = n * per
        any_spec = pl.BlockSpec(memory_space=pl.ANY)
        dma = pltpu.SemaphoreType.DMA
        sds = jax.ShapeDtypeStruct
        recv, h3, s3 = pl.pallas_call(
            functools.partial(_stack, n),
            name="stack",
            out_shape=(sds((chunks, n, per, wide), TRAVEL), sds((own, ch), f32), sds((own, sk), f32)),
            in_specs=[any_spec] * 8,
            out_specs=(any_spec,) * 3,
            scratch_shapes=[
                pltpu.VMEM((batch, span, ch), bf16), pltpu.VMEM((batch, span, cch), bf16),
                pltpu.VMEM((batch, HALO, ch), bf16), pltpu.VMEM((batch, HALO, cch), bf16),
                pltpu.VMEM((layers, 2 * ch + cch, 2 * ch), bf16), pltpu.VMEM((layers, ch, wide), bf16),
                pltpu.VMEM((layers, 2 * ch), f32),
                pltpu.VMEM((own, wide), f32),
                pltpu.VMEM((n, chunks, per, ch), bf16), pltpu.VMEM((n, chunks, per, cch), bf16),
                pltpu.VMEM((n, chunks, per, ch), TRAVEL), pltpu.VMEM((own, ch), f32),
                pltpu.VMEM((n, chunks, per, ch), bf16), pltpu.VMEM((n, chunks, per, cch), bf16),
                pltpu.VMEM((chunks, n, per, ch), TRAVEL),
                pltpu.VMEM((rows, wide), f32), pltpu.VMEM((chunks, n, per, wide), TRAVEL),
                dma((layers, 5)), dma((3,)), dma((2,)), dma((2,)), dma((2,)), dma((2,)),
                dma, dma((chunks,)), dma, dma((chunks,)), dma((2,)),
            ],
            compiler_params=pltpu.CompilerParams(collective_id=0, has_side_effects=True,
                                                 vmem_limit_bytes=56 * 1024 * 1024),
        )(signal, cond_feats, w_now, w_past, w_cond, b_gate, w_res, w_skip)
        h_out, skip_out = pl.pallas_call(
            _finish,
            name="finish",
            out_shape=(sds((own, ch), f32), sds((own, sk), f32)),
            in_specs=[any_spec] * 3,
            out_specs=(any_spec,) * 2,
            scratch_shapes=[
                pltpu.VMEM((chunks, n, per, wide), TRAVEL), pltpu.VMEM((own, ch), f32), pltpu.VMEM((own, sk), f32),
                pltpu.VMEM((wide // 128, own, 128), f32), dma((3,)), dma((wide // 128,)),
            ],
        )(recv, h3, s3)
        return h_out.reshape(batch, span, ch), skip_out.reshape(batch, span, sk)

    seq_spec = P('dp', 'sp', None)
    return jax.shard_map(local_stack, mesh=mesh,
                         in_specs=(seq_spec, seq_spec, P(), P(), P(), P(), P(), P()),
                         out_specs=(seq_spec, seq_spec), check_vma=False)
```

```python
import functools

import jax
import jax.numpy as jnp
from jax import lax
from jax.experimental import pallas as pl
from jax.experimental.pallas import tpu as pltpu
from jax.sharding import PartitionSpec as P

MESH = pl.DeviceIdType.MESH
NEAR = 3
RES = 2 ** NEAR
HALO = 16
f32, bf16 = jnp.float32, jnp.bfloat16
TRAVEL = bf16


def _iota(shape, dim):
    return lax.broadcasted_iota(jnp.int32, shape, dim)


def _stack(n, sig_hbm, cond_hbm, wn_hbm, wp_hbm, wc_hbm, bg_hbm, wr_hbm, ws_hbm,
           recv_hbm, h3_hbm, s3_hbm,
           sig_v, cond_v, halo_s, halo_c, w1, w2, bias,
           near, ssend, csend, dsend, h3, srecv, crecv, drecv, far, osend,
           w_sem, in_sem, halo_send, halo_recv, x_send, x_recv, d_send, d_recv, o_send, o_recv, out_sem):
    me = lax.axis_index("sp")
    batch, span, ch = sig_v.shape
    cch = cond_v.shape[2]
    layers = w1.shape[0]
    own = batch * span
    per = span // RES
    ncls = batch * RES
    chunks = ncls // n
    rows = n * per
    wide = w2.shape[2]
    hrows = batch * RES
    sh_span, sh_per = span.bit_length() - 1, per.bit_length() - 1

    ins = [pltpu.make_async_copy(sig_hbm, sig_v, in_sem.at[0]),
           pltpu.make_async_copy(cond_hbm, cond_v, in_sem.at[1]),
           pltpu.make_async_copy(bg_hbm, bias, in_sem.at[2])]
    for c in ins:
        c.start()

    def wcopies(k):
        return [pltpu.make_async_copy(wn_hbm.at[k], w1.at[k, pl.ds(0, ch)], w_sem.at[k, 0]),
                pltpu.make_async_copy(wp_hbm.at[k], w1.at[k, pl.ds(ch, ch)], w_sem.at[k, 1]),
                pltpu.make_async_copy(wc_hbm.at[k], w1.at[k, pl.ds(2 * ch, cch)], w_sem.at[k, 2]),
                pltpu.make_async_copy(wr_hbm.at[k], w2.at[k, :, pl.ds(0, ch)], w_sem.at[k, 3]),
                pltpu.make_async_copy(ws_hbm.at[k], w2.at[k, :, pl.ds(ch, wide - ch)], w_sem.at[k, 4])]

    for k in range(layers):
        for c in wcopies(k):
            c.start()

    barrier = pltpu.get_barrier_semaphore()
    for d in range(1, n):
        pl.semaphore_signal(barrier, inc=1, device_id={"sp": lax.rem(me + d, n)}, device_id_type=MESH)

    ins[0].wait()
    ins[1].wait()
    r, c = _iota((own, own), 0), _iota((own, own), 1)
    seq, rho, step = r >> sh_span, (r >> sh_per) & (RES - 1), r & (per - 1)
    perm = (c == seq * span + step * RES + rho).astype(bf16)
    cnd = jnp.dot(perm, cond_v[...].reshape(own, cch), preferred_element_type=f32)
    sig = jnp.dot(perm, sig_v[...].reshape(own, ch), preferred_element_type=f32)
    csend[...] = cnd.reshape(n, chunks, per, cch).astype(bf16)
    ssend[...] = sig.reshape(n, chunks, per, ch).astype(bf16)
    h3[...] = sig

    pl.semaphore_wait(barrier, n - 1)

    def halo_copies():
        nxt = lax.rem(me + 1, n)
        return [pltpu.make_async_remote_copy(sig_v.at[:, pl.ds(span - HALO, HALO)], halo_s, halo_send.at[0],
                                             halo_recv.at[0], device_id={"sp": nxt}, device_id_type=MESH),
                pltpu.make_async_remote_copy(cond_v.at[:, pl.ds(span - HALO, HALO)], halo_c, halo_send.at[1],
                                             halo_recv.at[1], device_id={"sp": nxt}, device_id_type=MESH)]

    for cp in halo_copies():
        cp.start()

    order = [n // 2]
    for d in range(n // 2 - 1, 0, -1):
        order += [n - d, d]
    order += [0]

    def push(src, dst, send_sem, recv_sem, d, to):
        if d == 0:
            pltpu.make_async_copy(src, dst, recv_sem).start()
        else:
            pltpu.make_async_remote_copy(src, dst, send_sem, recv_sem, device_id={"sp": to},
                                         device_id_type=MESH).start()

    def drain(buf, sem):
        pltpu.make_async_copy(buf, buf, sem).wait()

    for d in order:
        to = lax.rem(me + d, n)
        push(ssend.at[to], srecv.at[me], x_send.at[0], x_recv.at[0], d, to)
        push(csend.at[to], crecv.at[me], x_send.at[1], x_recv.at[1], d, to)

    for cp in halo_copies():
        cp.wait_recv()
    ins[2].wait()

    hr, hc = _iota((hrows, batch * HALO), 0), _iota((hrows, batch * HALO), 1)
    pick = (hc == (hr >> NEAR) * HALO + (HALO - RES) + (hr & (RES - 1))).astype(bf16)
    live = me > 0
    halo_h = jnp.dot(pick, halo_s[...].reshape(batch * HALO, ch), preferred_element_type=f32)
    halo_k = jnp.dot(pick, halo_c[...].reshape(batch * HALO, cch), preferred_element_type=f32)
    call = jnp.concatenate([cnd, halo_k], axis=0).astype(bf16)
    allr = own + hrows
    half = ch // 2

    def gate(x, k):
        parts = []
        for q in range(2):
            zf = jnp.dot(x, w1[k, :, q * half:(q + 1) * half], preferred_element_type=f32)
            zg = jnp.dot(x, w1[k, :, ch + q * half:ch + (q + 1) * half], preferred_element_type=f32)
            zf = zf + bias[k:k + 1, q * half:(q + 1) * half]
            zg = zg + bias[k:k + 1, ch + q * half:ch + (q + 1) * half]
            parts.append((jnp.tanh(zf) * (0.5 * jnp.tanh(0.5 * zg) + 0.5)).astype(bf16))
        return jnp.concatenate(parts, axis=1)

    for k in range(NEAR):
        d = 2 ** k
        u_halo = jnp.where(live, halo_h, 0.0)
        u = jnp.concatenate([h3[...], u_halo], axis=0).astype(bf16)
        r, c = _iota((allr, allr), 0), _iota((allr, allr), 1)
        seq, rho, step = r >> sh_span, (r >> sh_per) & (RES - 1), r & (per - 1)
        src = step * RES + rho - d
        own_col = seq * span + ((src & (RES - 1)) << sh_per) + (src >> NEAR)
        halo_col = own + seq * RES + src + RES
        col = jnp.where(src >= 0, own_col, halo_col)
        hseq, hrho = (r - own) >> NEAR, (r - own) & (RES - 1)
        col = jnp.where(r < own, col, jnp.where(hrho >= d, own + hseq * RES + hrho - d, -1))
        p = jnp.dot((c == col).astype(bf16), u, preferred_element_type=f32).astype(bf16)
        for cp in wcopies(k):
            cp.wait()
        a = gate(jnp.concatenate([u, p, call], axis=1), k)
        dlt = jnp.dot(a, w2[k], preferred_element_type=f32)
        if k == 0:
            near[...] = dlt[:own]
        else:
            near[...] += dlt[:own]
        h3[...] += dlt[:own, :ch]
        if k < NEAR - 1:
            halo_h = halo_h + dlt[own:, :ch]

    dsend[...] = near[:, 0:ch].reshape(n, chunks, per, ch).astype(TRAVEL)
    for ck in range(chunks):
        for d in order:
            to = lax.rem(me + d, n)
            push(dsend.at[to, ck], drecv.at[ck, me], d_send, d_recv.at[ck], d, to)

    outs = [pltpu.make_async_copy(h3, h3_hbm, out_sem.at[0]),
            pltpu.make_async_copy(near.at[:, pl.ds(ch, wide - ch)], s3_hbm, out_sem.at[1])]
    for cp in outs:
        cp.start()

    drain(srecv, x_recv.at[0])
    drain(crecv, x_recv.at[1])
    for k in range(NEAR, layers):
        for cp in wcopies(k):
            cp.wait()

    row = _iota((rows, ch), 0)
    for ck in range(chunks):
        drain(drecv.at[ck], d_recv.at[ck])
        base = (srecv[:, ck].astype(f32) + drecv[ck].astype(f32)).reshape(rows, ch)
        cq = crecv[:, ck].astype(f32).reshape(rows, cch).astype(bf16)
        h = base
        for k in range(NEAR, layers):
            sft = 2 ** (k - NEAR)
            if k > NEAR:
                h = base + far[:, 0:ch]
            if sft < 8:
                past = jnp.where(row >= sft, pltpu.roll(h, sft, 0), 0.0)
            else:
                past = jnp.concatenate([jnp.zeros((sft, ch), f32), h[:rows - sft]], axis=0)
            a = gate(jnp.concatenate([h.astype(bf16), past.astype(bf16), cq], axis=1), k)
            dlt = jnp.dot(a, w2[k], preferred_element_type=f32)
            if k == NEAR:
                far[...] = dlt
            elif k < layers - 1:
                far[...] += dlt
            else:
                osend[ck] = (far[...] + dlt).reshape(n, per, wide).astype(TRAVEL)
        for d in order:
            to = lax.rem(me + d, n)
            push(osend.at[ck, to], recv_hbm.at[ck, me], o_send, o_recv.at[ck], d, to)

    for cp in halo_copies():
        cp.wait_send()
    for cp in outs:
        cp.wait()
    for buf, sem in ((ssend.at[pl.ds(0, n - 1)], x_send.at[0]), (csend.at[pl.ds(0, n - 1)], x_send.at[1]),
                     (dsend.at[pl.ds(0, n - 1)], d_send), (osend.at[:, pl.ds(0, n - 1)], o_send)):
        drain(buf, sem)
    for ck in range(chunks):
        drain(recv_hbm.at[ck], o_recv.at[ck])


def _finish(recv_hbm, h3_hbm, s3_hbm, hout_hbm, sout_hbm, recv, h3, s3, obuf, in_sem, out_sem):
    chunks, n, per, wide = recv.shape
    own, ch = h3.shape
    span = per * RES
    ins = [pltpu.make_async_copy(h3_hbm, h3, in_sem.at[0]), pltpu.make_async_copy(s3_hbm, s3, in_sem.at[1]),
           pltpu.make_async_copy(recv_hbm, recv, in_sem.at[2])]
    for cp in ins:
        cp.start()
    for cp in ins:
        cp.wait()
    outs = []
    for t in range(wide // 128):
        lo = t * 128
        base, off = (h3, lo) if lo < ch else (s3, lo - ch)
        for ck in range(chunks):
            for j in range(n):
                cl = j * chunks + ck
                s, rho = cl // RES, cl % RES
                obuf[t, pl.ds(s * span + rho, per, RES), :] = (
                    recv[ck, j, :, lo:lo + 128].astype(f32) + base[cl * per:(cl + 1) * per, off:off + 128])
        dst = hout_hbm if lo < ch else sout_hbm
        outs.append(pltpu.make_async_copy(obuf.at[t], dst.at[:, pl.ds(off, 128)], out_sem.at[t]))
        outs[-1].start()
    for cp in outs:
        cp.wait()


def solution(mesh):
    n = mesh.shape['sp']

    def local_stack(signal, cond_feats, w_now, w_past, w_cond, b_gate, w_res, w_skip):
        batch, span, ch = signal.shape
        cch = cond_feats.shape[2]
        layers = w_now.shape[0]
        sk = w_skip.shape[2]
        wide = ch + sk
        own = batch * span
        per = span // RES
        chunks = batch * RES // n
        rows = n * per
        any_spec = pl.BlockSpec(memory_space=pl.ANY)
        dma = pltpu.SemaphoreType.DMA
        sds = jax.ShapeDtypeStruct
        recv, h3, s3 = pl.pallas_call(
            functools.partial(_stack, n),
            name="stack",
            out_shape=(sds((chunks, n, per, wide), TRAVEL), sds((own, ch), f32), sds((own, sk), f32)),
            in_specs=[any_spec] * 8,
            out_specs=(any_spec,) * 3,
            scratch_shapes=[
                pltpu.VMEM((batch, span, ch), bf16), pltpu.VMEM((batch, span, cch), bf16),
                pltpu.VMEM((batch, HALO, ch), bf16), pltpu.VMEM((batch, HALO, cch), bf16),
                pltpu.VMEM((layers, 2 * ch + cch, 2 * ch), bf16), pltpu.VMEM((layers, ch, wide), bf16),
                pltpu.VMEM((layers, 2 * ch), f32),
                pltpu.VMEM((own, wide), f32),
                pltpu.VMEM((n, chunks, per, ch), bf16), pltpu.VMEM((n, chunks, per, cch), bf16),
                pltpu.VMEM((n, chunks, per, ch), TRAVEL), pltpu.VMEM((own, ch), f32),
                pltpu.VMEM((n, chunks, per, ch), bf16), pltpu.VMEM((n, chunks, per, cch), bf16),
                pltpu.VMEM((chunks, n, per, ch), TRAVEL),
                pltpu.VMEM((rows, wide), f32), pltpu.VMEM((chunks, n, per, wide), TRAVEL),
                dma((layers, 5)), dma((3,)), dma((2,)), dma((2,)), dma((2,)), dma((2,)),
                dma, dma((chunks,)), dma, dma((chunks,)), dma((2,)),
            ],
            compiler_params=pltpu.CompilerParams(collective_id=0, has_side_effects=True,
                                                 vmem_limit_bytes=56 * 1024 * 1024),
        )(signal, cond_feats, w_now, w_past, w_cond, b_gate, w_res, w_skip)
        h_out, skip_out = pl.pallas_call(
            _finish,
            name="finish",
            out_shape=(sds((own, ch), f32), sds((own, sk), f32)),
            in_specs=[any_spec] * 3,
            out_specs=(any_spec,) * 2,
            scratch_shapes=[
                pltpu.VMEM((chunks, n, per, wide), TRAVEL), pltpu.VMEM((own, ch), f32), pltpu.VMEM((own, sk), f32),
                pltpu.VMEM((wide // 128, own, 128), f32), dma((3,)), dma((wide // 128,)),
            ],
        )(recv, h3, s3)
        return h_out.reshape(batch, span, ch), skip_out.reshape(batch, span, sk)

    seq_spec = P('dp', 'sp', None)
    return jax.shard_map(local_stack, mesh=mesh,
                         in_specs=(seq_spec, seq_spec, P(), P(), P(), P(), P(), P()),
                         out_specs=(seq_spec, seq_spec), check_vma=False)
```

```python
import functools

import jax
import jax.numpy as jnp
from jax import lax
from jax.experimental import pallas as pl
from jax.experimental.pallas import tpu as pltpu
from jax.sharding import PartitionSpec as P

MESH = pl.DeviceIdType.MESH
NEAR = 3
RES = 2 ** NEAR
HALO = 16
f32, bf16 = jnp.float32, jnp.bfloat16
TRAVEL = bf16


def _iota(shape, dim):
    return lax.broadcasted_iota(jnp.int32, shape, dim)


def _stack(n, sig_hbm, cond_hbm, wn_hbm, wp_hbm, wc_hbm, bg_hbm, wr_hbm, ws_hbm,
           recv_hbm, h3_hbm, s3_hbm,
           sig_v, cond_v, halo_s, halo_c, w1, w2, bias,
           near, ssend, csend, dsend, h3, srecv, crecv, drecv, far, osend,
           w_sem, in_sem, halo_send, halo_recv, x_send, x_recv, d_send, d_recv, o_send, o_recv, out_sem):
    me = lax.axis_index("sp")
    batch, span, ch = sig_v.shape
    cch = cond_v.shape[2]
    layers = w1.shape[0]
    own = batch * span
    per = span // RES
    ncls = batch * RES
    chunks = ncls // n
    rows = n * per
    wide = w2.shape[2]
    hrows = batch * RES
    sh_span, sh_per = span.bit_length() - 1, per.bit_length() - 1

    ins = [pltpu.make_async_copy(sig_hbm, sig_v, in_sem.at[0]),
           pltpu.make_async_copy(cond_hbm, cond_v, in_sem.at[1]),
           pltpu.make_async_copy(bg_hbm, bias, in_sem.at[2])]
    for c in ins:
        c.start()

    def wcopies(k):
        return [pltpu.make_async_copy(wn_hbm.at[k], w1.at[k, pl.ds(0, ch)], w_sem.at[k, 0]),
                pltpu.make_async_copy(wp_hbm.at[k], w1.at[k, pl.ds(ch, ch)], w_sem.at[k, 1]),
                pltpu.make_async_copy(wc_hbm.at[k], w1.at[k, pl.ds(2 * ch, cch)], w_sem.at[k, 2]),
                pltpu.make_async_copy(wr_hbm.at[k], w2.at[k, :, pl.ds(0, ch)], w_sem.at[k, 3]),
                pltpu.make_async_copy(ws_hbm.at[k], w2.at[k, :, pl.ds(ch, wide - ch)], w_sem.at[k, 4])]

    def fetch(*ks):
        for k in ks:
            for c in wcopies(k):
                c.start()

    fetch(*range(NEAR))

    barrier = pltpu.get_barrier_semaphore()
    for d in range(1, n):
        pl.semaphore_signal(barrier, inc=1, device_id={"sp": lax.rem(me + d, n)}, device_id_type=MESH)

    ins[0].wait()
    ins[1].wait()
    r, c = _iota((own, own), 0), _iota((own, own), 1)
    seq, rho, step = r >> sh_span, (r >> sh_per) & (RES - 1), r & (per - 1)
    perm = (c == seq * span + step * RES + rho).astype(bf16)
    cnd = jnp.dot(perm, cond_v[...].reshape(own, cch), preferred_element_type=f32)
    sig = jnp.dot(perm, sig_v[...].reshape(own, ch), preferred_element_type=f32)
    csend[...] = cnd.reshape(n, chunks, per, cch).astype(bf16)
    ssend[...] = sig.reshape(n, chunks, per, ch).astype(bf16)
    h3[...] = sig

    pl.semaphore_wait(barrier, n - 1)

    def halo_copies():
        nxt = lax.rem(me + 1, n)
        return [pltpu.make_async_remote_copy(sig_v.at[:, pl.ds(span - HALO, HALO)], halo_s, halo_send.at[0],
                                             halo_recv.at[0], device_id={"sp": nxt}, device_id_type=MESH),
                pltpu.make_async_remote_copy(cond_v.at[:, pl.ds(span - HALO, HALO)], halo_c, halo_send.at[1],
                                             halo_recv.at[1], device_id={"sp": nxt}, device_id_type=MESH)]

    for cp in halo_copies():
        cp.start()

    order = [n // 2]
    for d in range(n // 2 - 1, 0, -1):
        order += [n - d, d]
    order += [0]

    def push(src, dst, send_sem, recv_sem, d, to):
        if d == 0:
            pltpu.make_async_copy(src, dst, recv_sem).start()
        else:
            pltpu.make_async_remote_copy(src, dst, send_sem, recv_sem, device_id={"sp": to},
                                         device_id_type=MESH).start()

    def drain(buf, sem):
        pltpu.make_async_copy(buf, buf, sem).wait()

    for d in order:
        to = lax.rem(me + d, n)
        push(ssend.at[to], srecv.at[me], x_send.at[0], x_recv.at[0], d, to)
        push(csend.at[to], crecv.at[me], x_send.at[1], x_recv.at[1], d, to)

    for cp in halo_copies():
        cp.wait_recv()
    ins[2].wait()

    hr, hc = _iota((hrows, batch * HALO), 0), _iota((hrows, batch * HALO), 1)
    pick = (hc == (hr >> NEAR) * HALO + (HALO - RES) + (hr & (RES - 1))).astype(bf16)
    live = me > 0
    halo_h = jnp.dot(pick, halo_s[...].reshape(batch * HALO, ch), preferred_element_type=f32)
    halo_k = jnp.dot(pick, halo_c[...].reshape(batch * HALO, cch), preferred_element_type=f32)
    call = jnp.concatenate([cnd, halo_k], axis=0).astype(bf16)
    allr = own + hrows
    half = ch // 2

    def gate(x, k):
        parts = []
        for q in range(2):
            zf = jnp.dot(x, w1[k, :, q * half:(q + 1) * half], preferred_element_type=f32)
            zg = jnp.dot(x, w1[k, :, ch + q * half:ch + (q + 1) * half], preferred_element_type=f32)
            zf = zf + bias[k:k + 1, q * half:(q + 1) * half]
            zg = zg + bias[k:k + 1, ch + q * half:ch + (q + 1) * half]
            parts.append((jnp.tanh(zf) * (0.5 * jnp.tanh(0.5 * zg) + 0.5)).astype(bf16))
        return jnp.concatenate(parts, axis=1)

    for k in range(NEAR):
        d = 2 ** k
        u_halo = jnp.where(live, halo_h, 0.0)
        u = jnp.concatenate([h3[...], u_halo], axis=0).astype(bf16)
        r, c = _iota((allr, allr), 0), _iota((allr, allr), 1)
        seq, rho, step = r >> sh_span, (r >> sh_per) & (RES - 1), r & (per - 1)
        src = step * RES + rho - d
        own_col = seq * span + ((src & (RES - 1)) << sh_per) + (src >> NEAR)
        halo_col = own + seq * RES + src + RES
        col = jnp.where(src >= 0, own_col, halo_col)
        hseq, hrho = (r - own) >> NEAR, (r - own) & (RES - 1)
        col = jnp.where(r < own, col, jnp.where(hrho >= d, own + hseq * RES + hrho - d, -1))
        p = jnp.dot((c == col).astype(bf16), u, preferred_element_type=f32).astype(bf16)
        for cp in wcopies(k):
            cp.wait()
        fetch(*range(NEAR + 2 * k, min(NEAR + 2 * k + 2, layers - 2)))
        a = gate(jnp.concatenate([u, p, call], axis=1), k)
        dlt = jnp.dot(a, w2[k], preferred_element_type=f32)
        if k == 0:
            near[...] = dlt[:own]
        else:
            near[...] += dlt[:own]
        h3[...] += dlt[:own, :ch]
        if k < NEAR - 1:
            halo_h = halo_h + dlt[own:, :ch]

    dsend[...] = near[:, 0:ch].reshape(n, chunks, per, ch).astype(TRAVEL)
    for ck in range(chunks):
        for d in order:
            to = lax.rem(me + d, n)
            push(dsend.at[to, ck], drecv.at[ck, me], d_send, d_recv.at[ck], d, to)

    fetch(layers - 2, layers - 1)
    outs = [pltpu.make_async_copy(h3, h3_hbm, out_sem.at[0]),
            pltpu.make_async_copy(near.at[:, pl.ds(ch, wide - ch)], s3_hbm, out_sem.at[1])]
    for cp in outs:
        cp.start()

    drain(srecv, x_recv.at[0])
    drain(crecv, x_recv.at[1])
    row = _iota((rows, ch), 0)
    for ck in range(chunks):
        drain(drecv.at[ck], d_recv.at[ck])
        base = (srecv[:, ck].astype(f32) + drecv[ck].astype(f32)).reshape(rows, ch)
        cq = crecv[:, ck].astype(f32).reshape(rows, cch).astype(bf16)
        h = base
        for k in range(NEAR, layers):
            sft = 2 ** (k - NEAR)
            if k > NEAR:
                h = base + far[:, 0:ch]
            if sft < 8:
                past = jnp.where(row >= sft, pltpu.roll(h, sft, 0), 0.0)
            else:
                past = jnp.concatenate([jnp.zeros((sft, ch), f32), h[:rows - sft]], axis=0)
            if ck == 0:
                for cp in wcopies(k):
                    cp.wait()
            a = gate(jnp.concatenate([h.astype(bf16), past.astype(bf16), cq], axis=1), k)
            dlt = jnp.dot(a, w2[k], preferred_element_type=f32)
            if k == NEAR:
                far[...] = dlt
            elif k < layers - 1:
                far[...] += dlt
            else:
                osend[ck] = (far[...] + dlt).reshape(n, per, wide).astype(TRAVEL)
        for d in order:
            to = lax.rem(me + d, n)
            push(osend.at[ck, to], recv_hbm.at[ck, me], o_send, o_recv.at[ck], d, to)

    for cp in halo_copies():
        cp.wait_send()
    for cp in outs:
        cp.wait()
    for buf, sem in ((ssend.at[pl.ds(0, n - 1)], x_send.at[0]), (csend.at[pl.ds(0, n - 1)], x_send.at[1]),
                     (dsend.at[pl.ds(0, n - 1)], d_send), (osend.at[:, pl.ds(0, n - 1)], o_send)):
        drain(buf, sem)
    for ck in range(chunks):
        drain(recv_hbm.at[ck], o_recv.at[ck])


def _finish(recv_hbm, h3_hbm, s3_hbm, hout_hbm, sout_hbm, recv, h3, s3, obuf, in_sem, out_sem):
    chunks, n, per, wide = recv.shape
    own, ch = h3.shape
    span = per * RES
    ins = [pltpu.make_async_copy(h3_hbm, h3, in_sem.at[0]), pltpu.make_async_copy(s3_hbm, s3, in_sem.at[1]),
           pltpu.make_async_copy(recv_hbm, recv, in_sem.at[2])]
    for cp in ins:
        cp.start()
    for cp in ins:
        cp.wait()
    outs = []
    for t in range(wide // 128):
        lo = t * 128
        base, off = (h3, lo) if lo < ch else (s3, lo - ch)
        for ck in range(chunks):
            for j in range(n):
                cl = j * chunks + ck
                s, rho = cl // RES, cl % RES
                obuf[t, pl.ds(s * span + rho, per, RES), :] = (
                    recv[ck, j, :, lo:lo + 128].astype(f32) + base[cl * per:(cl + 1) * per, off:off + 128])
        dst = hout_hbm if lo < ch else sout_hbm
        outs.append(pltpu.make_async_copy(obuf.at[t], dst.at[:, pl.ds(off, 128)], out_sem.at[t]))
        outs[-1].start()
    for cp in outs:
        cp.wait()


def solution(mesh):
    n = mesh.shape['sp']

    def local_stack(signal, cond_feats, w_now, w_past, w_cond, b_gate, w_res, w_skip):
        batch, span, ch = signal.shape
        cch = cond_feats.shape[2]
        layers = w_now.shape[0]
        sk = w_skip.shape[2]
        wide = ch + sk
        own = batch * span
        per = span // RES
        chunks = batch * RES // n
        rows = n * per
        any_spec = pl.BlockSpec(memory_space=pl.ANY)
        dma = pltpu.SemaphoreType.DMA
        sds = jax.ShapeDtypeStruct
        recv, h3, s3 = pl.pallas_call(
            functools.partial(_stack, n),
            name="stack",
            out_shape=(sds((chunks, n, per, wide), TRAVEL), sds((own, ch), f32), sds((own, sk), f32)),
            in_specs=[any_spec] * 8,
            out_specs=(any_spec,) * 3,
            scratch_shapes=[
                pltpu.VMEM((batch, span, ch), bf16), pltpu.VMEM((batch, span, cch), bf16),
                pltpu.VMEM((batch, HALO, ch), bf16), pltpu.VMEM((batch, HALO, cch), bf16),
                pltpu.VMEM((layers, 2 * ch + cch, 2 * ch), bf16), pltpu.VMEM((layers, ch, wide), bf16),
                pltpu.VMEM((layers, 2 * ch), f32),
                pltpu.VMEM((own, wide), f32),
                pltpu.VMEM((n, chunks, per, ch), bf16), pltpu.VMEM((n, chunks, per, cch), bf16),
                pltpu.VMEM((n, chunks, per, ch), TRAVEL), pltpu.VMEM((own, ch), f32),
                pltpu.VMEM((n, chunks, per, ch), bf16), pltpu.VMEM((n, chunks, per, cch), bf16),
                pltpu.VMEM((chunks, n, per, ch), TRAVEL),
                pltpu.VMEM((rows, wide), f32), pltpu.VMEM((chunks, n, per, wide), TRAVEL),
                dma((layers, 5)), dma((3,)), dma((2,)), dma((2,)), dma((2,)), dma((2,)),
                dma, dma((chunks,)), dma, dma((chunks,)), dma((2,)),
            ],
            compiler_params=pltpu.CompilerParams(collective_id=0, has_side_effects=True,
                                                 vmem_limit_bytes=56 * 1024 * 1024),
        )(signal, cond_feats, w_now, w_past, w_cond, b_gate, w_res, w_skip)
        h_out, skip_out = pl.pallas_call(
            _finish,
            name="finish",
            out_shape=(sds((own, ch), f32), sds((own, sk), f32)),
            in_specs=[any_spec] * 3,
            out_specs=(any_spec,) * 2,
            scratch_shapes=[
                pltpu.VMEM((chunks, n, per, wide), TRAVEL), pltpu.VMEM((own, ch), f32), pltpu.VMEM((own, sk), f32),
                pltpu.VMEM((wide // 128, own, 128), f32), dma((3,)), dma((wide // 128,)),
            ],
        )(recv, h3, s3)
        return h_out.reshape(batch, span, ch), skip_out.reshape(batch, span, sk)

    seq_spec = P('dp', 'sp', None)
    return jax.shard_map(local_stack, mesh=mesh,
                         in_specs=(seq_spec, seq_spec, P(), P(), P(), P(), P(), P()),
                         out_specs=(seq_spec, seq_spec), check_vma=False)
```

```python
import functools

import jax
import jax.numpy as jnp
from jax import lax
from jax.experimental import pallas as pl
from jax.experimental.pallas import tpu as pltpu
from jax.sharding import PartitionSpec as P

MESH = pl.DeviceIdType.MESH
NEAR = 3
RES = 2 ** NEAR
HALO = 16
f32, bf16 = jnp.float32, jnp.bfloat16
TRAVEL = bf16


def _iota(shape, dim):
    return lax.broadcasted_iota(jnp.int32, shape, dim)


def _stack(n, sig_hbm, cond_hbm, wn_hbm, wp_hbm, wc_hbm, bg_hbm, wr_hbm, ws_hbm,
           recv_hbm, h3_hbm, s3_hbm,
           sig_v, cond_v, halo_s, halo_c, w1, w2, bias,
           near, ssend, csend, dsend, h3, srecv, crecv, drecv, far, osend,
           w_sem, in_sem, halo_send, halo_recv, x_send, x_recv, d_send, d_recv, o_send, o_recv, out_sem, round_sem):
    me = lax.axis_index("sp")
    batch, span, ch = sig_v.shape
    cch = cond_v.shape[2]
    layers = w1.shape[0]
    own = batch * span
    per = span // RES
    ncls = batch * RES
    chunks = ncls // n
    rows = n * per
    wide = w2.shape[2]
    hrows = batch * RES
    sh_span, sh_per = span.bit_length() - 1, per.bit_length() - 1

    def tell(sem, d):
        for to in (lax.rem(me + d, n), lax.rem(me + n - d, n)):
            pl.semaphore_signal(sem, inc=1, device_id={"sp": to}, device_id_type=MESH)

    barrier = pltpu.get_barrier_semaphore()
    tell(barrier, 1)

    ins = [pltpu.make_async_copy(sig_hbm, sig_v, in_sem.at[0]),
           pltpu.make_async_copy(cond_hbm, cond_v, in_sem.at[1]),
           pltpu.make_async_copy(bg_hbm, bias, in_sem.at[2])]
    for c in ins:
        c.start()

    def wcopies(k):
        return [pltpu.make_async_copy(wn_hbm.at[k], w1.at[k, pl.ds(0, ch)], w_sem.at[k, 0]),
                pltpu.make_async_copy(wp_hbm.at[k], w1.at[k, pl.ds(ch, ch)], w_sem.at[k, 1]),
                pltpu.make_async_copy(wc_hbm.at[k], w1.at[k, pl.ds(2 * ch, cch)], w_sem.at[k, 2]),
                pltpu.make_async_copy(wr_hbm.at[k], w2.at[k, :, pl.ds(0, ch)], w_sem.at[k, 3]),
                pltpu.make_async_copy(ws_hbm.at[k], w2.at[k, :, pl.ds(ch, wide - ch)], w_sem.at[k, 4])]

    def fetch(*ks):
        for k in ks:
            for c in wcopies(k):
                c.start()

    fetch(0)

    def halo_copies():
        nxt = lax.rem(me + 1, n)
        return [pltpu.make_async_remote_copy(sig_v.at[:, pl.ds(span - HALO, HALO)], halo_s, halo_send.at[0],
                                             halo_recv.at[0], device_id={"sp": nxt}, device_id_type=MESH),
                pltpu.make_async_remote_copy(cond_v.at[:, pl.ds(span - HALO, HALO)], halo_c, halo_send.at[1],
                                             halo_recv.at[1], device_id={"sp": nxt}, device_id_type=MESH)]

    pl.semaphore_wait(barrier, 2)
    ins[0].wait()
    ins[1].wait()
    for cp in halo_copies():
        cp.start()
    tell(round_sem.at[0], 1)
    fetch(1, 2)
    r, c = _iota((own, own), 0), _iota((own, own), 1)
    seq, rho, step = r >> sh_span, (r >> sh_per) & (RES - 1), r & (per - 1)
    perm = (c == seq * span + step * RES + rho).astype(bf16)
    cnd = jnp.dot(perm, cond_v[...].reshape(own, cch), preferred_element_type=f32)
    sig = jnp.dot(perm, sig_v[...].reshape(own, ch), preferred_element_type=f32)
    csend[...] = cnd.reshape(n, chunks, per, cch).astype(bf16)
    ssend[...] = sig.reshape(n, chunks, per, ch).astype(bf16)
    h3[...] = sig

    reach, rnd = 2, 0
    while True:
        pl.semaphore_wait(round_sem.at[rnd], 2)
        if reach >= n // 2:
            break
        rnd += 1
        tell(round_sem.at[rnd], reach)
        reach *= 2

    order = [n // 2]
    for d in range(n // 2 - 1, 0, -1):
        order += [n - d, d]
    order += [0]

    def push(src, dst, send_sem, recv_sem, d, to):
        if d == 0:
            pltpu.make_async_copy(src, dst, recv_sem).start()
        else:
            pltpu.make_async_remote_copy(src, dst, send_sem, recv_sem, device_id={"sp": to},
                                         device_id_type=MESH).start()

    def drain(buf, sem):
        pltpu.make_async_copy(buf, buf, sem).wait()

    for d in order:
        to = lax.rem(me + d, n)
        push(csend.at[to], crecv.at[me], x_send.at[chunks], x_recv.at[chunks], d, to)
        push(ssend.at[to, 0], srecv.at[0, me], x_send.at[0], x_recv.at[0], d, to)
    fetch(NEAR, NEAR + 1)

    for cp in halo_copies():
        cp.wait_recv()
    ins[2].wait()

    hr, hc = _iota((hrows, batch * HALO), 0), _iota((hrows, batch * HALO), 1)
    pick = (hc == (hr >> NEAR) * HALO + (HALO - RES) + (hr & (RES - 1))).astype(bf16)
    live = me > 0
    halo_h = jnp.dot(pick, halo_s[...].reshape(batch * HALO, ch), preferred_element_type=f32)
    halo_k = jnp.dot(pick, halo_c[...].reshape(batch * HALO, cch), preferred_element_type=f32)
    call = jnp.concatenate([cnd, halo_k], axis=0).astype(bf16)
    allr = own + hrows
    half = ch // 2

    def gate(x, k):
        parts = []
        for q in range(2):
            zf = jnp.dot(x, w1[k, :, q * half:(q + 1) * half], preferred_element_type=f32)
            zg = jnp.dot(x, w1[k, :, ch + q * half:ch + (q + 1) * half], preferred_element_type=f32)
            zf = zf + bias[k:k + 1, q * half:(q + 1) * half]
            zg = zg + bias[k:k + 1, ch + q * half:ch + (q + 1) * half]
            parts.append((jnp.tanh(zf) * (0.5 * jnp.tanh(0.5 * zg) + 0.5)).astype(bf16))
        return jnp.concatenate(parts, axis=1)

    for k in range(NEAR):
        d = 2 ** k
        u_halo = jnp.where(live, halo_h, 0.0)
        u = jnp.concatenate([h3[...], u_halo], axis=0).astype(bf16)
        r, c = _iota((allr, allr), 0), _iota((allr, allr), 1)
        seq, rho, step = r >> sh_span, (r >> sh_per) & (RES - 1), r & (per - 1)
        src = step * RES + rho - d
        own_col = seq * span + ((src & (RES - 1)) << sh_per) + (src >> NEAR)
        halo_col = own + seq * RES + src + RES
        col = jnp.where(src >= 0, own_col, halo_col)
        hseq, hrho = (r - own) >> NEAR, (r - own) & (RES - 1)
        col = jnp.where(r < own, col, jnp.where(hrho >= d, own + hseq * RES + hrho - d, -1))
        p = jnp.dot((c == col).astype(bf16), u, preferred_element_type=f32).astype(bf16)
        for cp in wcopies(k):
            cp.wait()
        a = gate(jnp.concatenate([u, p, call], axis=1), k)
        dlt = jnp.dot(a, w2[k], preferred_element_type=f32)
        if k == 0:
            near[...] = dlt[:own]
        else:
            near[...] += dlt[:own]
        h3[...] += dlt[:own, :ch]
        if k < NEAR - 1:
            halo_h = halo_h + dlt[own:, :ch]

    dsend[...] = near[:, 0:ch].reshape(n, chunks, per, ch).astype(TRAVEL)
    for ck in range(chunks):
        for d in order:
            to = lax.rem(me + d, n)
            if ck > 0:
                push(ssend.at[to, ck], srecv.at[ck, me], x_send.at[ck], x_recv.at[ck], d, to)
            push(dsend.at[to, ck], drecv.at[ck, me], d_send, d_recv.at[ck], d, to)
        if ck == 0:
            fetch(NEAR + 2, NEAR + 3)

    fetch(*range(NEAR + 4, layers))
    outs = [pltpu.make_async_copy(h3, h3_hbm, out_sem.at[0]),
            pltpu.make_async_copy(near.at[:, pl.ds(ch, wide - ch)], s3_hbm, out_sem.at[1])]
    for cp in outs:
        cp.start()

    drain(crecv, x_recv.at[chunks])
    row = _iota((rows, ch), 0)
    for ck in range(chunks):
        drain(srecv.at[ck], x_recv.at[ck])
        drain(drecv.at[ck], d_recv.at[ck])
        base = (srecv[ck].astype(f32) + drecv[ck].astype(f32)).reshape(rows, ch)
        cq = crecv[:, ck].astype(f32).reshape(rows, cch).astype(bf16)
        h = base
        for k in range(NEAR, layers):
            sft = 2 ** (k - NEAR)
            if k > NEAR:
                h = base + far[:, 0:ch]
            if sft < 8:
                past = jnp.where(row >= sft, pltpu.roll(h, sft, 0), 0.0)
            else:
                past = jnp.concatenate([jnp.zeros((sft, ch), f32), h[:rows - sft]], axis=0)
            if ck == 0:
                for cp in wcopies(k):
                    cp.wait()
            a = gate(jnp.concatenate([h.astype(bf16), past.astype(bf16), cq], axis=1), k)
            dlt = jnp.dot(a, w2[k], preferred_element_type=f32)
            if k == NEAR:
                far[...] = dlt
            elif k < layers - 1:
                far[...] += dlt
            else:
                osend[ck] = (far[...] + dlt).reshape(n, per, wide).astype(TRAVEL)
        for d in order:
            to = lax.rem(me + d, n)
            push(osend.at[ck, to], recv_hbm.at[ck, me], o_send, o_recv.at[ck], d, to)

    for cp in halo_copies():
        cp.wait_send()
    for cp in outs:
        cp.wait()
    for ck in range(chunks):
        drain(ssend.at[pl.ds(0, n - 1), ck], x_send.at[ck])
    for buf, sem in ((csend.at[pl.ds(0, n - 1)], x_send.at[chunks]), (dsend.at[pl.ds(0, n - 1)], d_send), (osend.at[:, pl.ds(0, n - 1)], o_send)):
        drain(buf, sem)
    for ck in range(chunks):
        drain(recv_hbm.at[ck], o_recv.at[ck])


def _finish(recv_hbm, h3_hbm, s3_hbm, hout_hbm, sout_hbm, recv, h3, s3, obuf, in_sem, out_sem):
    chunks, n, per, wide = recv.shape
    own, ch = h3.shape
    span = per * RES
    ins = [pltpu.make_async_copy(h3_hbm, h3, in_sem.at[0]), pltpu.make_async_copy(s3_hbm, s3, in_sem.at[1]),
           pltpu.make_async_copy(recv_hbm, recv, in_sem.at[2])]
    for cp in ins:
        cp.start()
    for cp in ins:
        cp.wait()
    outs = []
    for t in range(wide // 128):
        lo = t * 128
        base, off = (h3, lo) if lo < ch else (s3, lo - ch)
        for ck in range(chunks):
            for j in range(n):
                cl = j * chunks + ck
                s, rho = cl // RES, cl % RES
                obuf[t, pl.ds(s * span + rho, per, RES), :] = (
                    recv[ck, j, :, lo:lo + 128].astype(f32) + base[cl * per:(cl + 1) * per, off:off + 128])
        dst = hout_hbm if lo < ch else sout_hbm
        outs.append(pltpu.make_async_copy(obuf.at[t], dst.at[:, pl.ds(off, 128)], out_sem.at[t]))
        outs[-1].start()
    for cp in outs:
        cp.wait()


def solution(mesh):
    n = mesh.shape['sp']

    def local_stack(signal, cond_feats, w_now, w_past, w_cond, b_gate, w_res, w_skip):
        batch, span, ch = signal.shape
        cch = cond_feats.shape[2]
        layers = w_now.shape[0]
        sk = w_skip.shape[2]
        wide = ch + sk
        own = batch * span
        per = span // RES
        chunks = batch * RES // n
        rows = n * per
        any_spec = pl.BlockSpec(memory_space=pl.ANY)
        dma = pltpu.SemaphoreType.DMA
        sds = jax.ShapeDtypeStruct
        recv, h3, s3 = pl.pallas_call(
            functools.partial(_stack, n),
            name="stack",
            out_shape=(sds((chunks, n, per, wide), TRAVEL), sds((own, ch), f32), sds((own, sk), f32)),
            in_specs=[any_spec] * 8,
            out_specs=(any_spec,) * 3,
            scratch_shapes=[
                pltpu.VMEM((batch, span, ch), bf16), pltpu.VMEM((batch, span, cch), bf16),
                pltpu.VMEM((batch, HALO, ch), bf16), pltpu.VMEM((batch, HALO, cch), bf16),
                pltpu.VMEM((layers, 2 * ch + cch, 2 * ch), bf16), pltpu.VMEM((layers, ch, wide), bf16),
                pltpu.VMEM((layers, 2 * ch), f32),
                pltpu.VMEM((own, wide), f32),
                pltpu.VMEM((n, chunks, per, ch), bf16), pltpu.VMEM((n, chunks, per, cch), bf16),
                pltpu.VMEM((n, chunks, per, ch), TRAVEL), pltpu.VMEM((own, ch), f32),
                pltpu.VMEM((chunks, n, per, ch), bf16), pltpu.VMEM((n, chunks, per, cch), bf16),
                pltpu.VMEM((chunks, n, per, ch), TRAVEL),
                pltpu.VMEM((rows, wide), f32), pltpu.VMEM((chunks, n, per, wide), TRAVEL),
                dma((layers, 5)), dma((3,)), dma((2,)), dma((2,)), dma((chunks + 1,)), dma((chunks + 1,)),
                dma, dma((chunks,)), dma, dma((chunks,)), dma((2,)), pltpu.SemaphoreType.REGULAR((4,)),
            ],
            compiler_params=pltpu.CompilerParams(collective_id=0, has_side_effects=True,
                                                 vmem_limit_bytes=56 * 1024 * 1024),
        )(signal, cond_feats, w_now, w_past, w_cond, b_gate, w_res, w_skip)
        h_out, skip_out = pl.pallas_call(
            _finish,
            name="finish",
            out_shape=(sds((own, ch), f32), sds((own, sk), f32)),
            in_specs=[any_spec] * 3,
            out_specs=(any_spec,) * 2,
            scratch_shapes=[
                pltpu.VMEM((chunks, n, per, wide), TRAVEL), pltpu.VMEM((own, ch), f32), pltpu.VMEM((own, sk), f32),
                pltpu.VMEM((wide // 128, own, 128), f32), dma((3,)), dma((wide // 128,)),
            ],
        )(recv, h3, s3)
        return h_out.reshape(batch, span, ch), skip_out.reshape(batch, span, sk)

    seq_spec = P('dp', 'sp', None)
    return jax.shard_map(local_stack, mesh=mesh,
                         in_specs=(seq_spec, seq_spec, P(), P(), P(), P(), P(), P()),
                         out_specs=(seq_spec, seq_spec), check_vma=False)
```

```python
import functools

import jax
import jax.numpy as jnp
from jax import lax
from jax.experimental import pallas as pl
from jax.experimental.pallas import tpu as pltpu
from jax.sharding import PartitionSpec as P

MESH = pl.DeviceIdType.MESH
NEAR = 3
RES = 2 ** NEAR
HALO = 16
f32, bf16 = jnp.float32, jnp.bfloat16
TRAVEL = bf16


def _iota(shape, dim):
    return lax.broadcasted_iota(jnp.int32, shape, dim)


def _stack(n, sig_hbm, cond_hbm, wn_hbm, wp_hbm, wc_hbm, bg_hbm, wr_hbm, ws_hbm,
           recv, h3, s3,
           sig_v, cond_v, halo_s, halo_c, w1, w2, bias,
           near, ssend, csend, dsend, srecv, crecv, drecv, far, osend,
           w_sem, in_sem, halo_send, halo_recv, x_send, x_recv, d_send, d_recv, o_send, o_recv):
    me = lax.axis_index("sp")
    batch, span, ch = sig_v.shape
    cch = cond_v.shape[2]
    layers = w1.shape[0]
    own = batch * span
    per = span // RES
    ncls = batch * RES
    chunks = ncls // n
    rows = n * per
    wide = w2.shape[2]
    hrows = batch * RES
    sh_span, sh_per = span.bit_length() - 1, per.bit_length() - 1

    barrier = pltpu.get_barrier_semaphore()
    for d in range(1, n):
        pl.semaphore_signal(barrier, inc=1, device_id={"sp": lax.rem(me + d, n)}, device_id_type=MESH)

    ins = [pltpu.make_async_copy(sig_hbm, sig_v, in_sem.at[0]),
           pltpu.make_async_copy(cond_hbm, cond_v, in_sem.at[1]),
           pltpu.make_async_copy(bg_hbm, bias, in_sem.at[2])]
    for c in ins:
        c.start()

    def wcopies(k):
        return [pltpu.make_async_copy(wn_hbm.at[k], w1.at[k, pl.ds(0, ch)], w_sem.at[k, 0]),
                pltpu.make_async_copy(wp_hbm.at[k], w1.at[k, pl.ds(ch, ch)], w_sem.at[k, 1]),
                pltpu.make_async_copy(wc_hbm.at[k], w1.at[k, pl.ds(2 * ch, cch)], w_sem.at[k, 2]),
                pltpu.make_async_copy(wr_hbm.at[k], w2.at[k, :, pl.ds(0, ch)], w_sem.at[k, 3]),
                pltpu.make_async_copy(ws_hbm.at[k], w2.at[k, :, pl.ds(ch, wide - ch)], w_sem.at[k, 4])]

    def fetch(*ks):
        for k in ks:
            for c in wcopies(k):
                c.start()

    fetch(0)

    def halo_copies():
        nxt = lax.rem(me + 1, n)
        return [pltpu.make_async_remote_copy(sig_v.at[:, pl.ds(span - HALO, HALO)], halo_s, halo_send.at[0],
                                             halo_recv.at[0], device_id={"sp": nxt}, device_id_type=MESH),
                pltpu.make_async_remote_copy(cond_v.at[:, pl.ds(span - HALO, HALO)], halo_c, halo_send.at[1],
                                             halo_recv.at[1], device_id={"sp": nxt}, device_id_type=MESH)]

    fetch(1, 2)
    ins[0].wait()
    ins[1].wait()
    r, c = _iota((own, own), 0), _iota((own, own), 1)
    seq, rho, step = r >> sh_span, (r >> sh_per) & (RES - 1), r & (per - 1)
    perm = (c == seq * span + step * RES + rho).astype(bf16)
    cnd = jnp.dot(perm, cond_v[...].reshape(own, cch), preferred_element_type=f32)
    sig = jnp.dot(perm, sig_v[...].reshape(own, ch), preferred_element_type=f32)
    csend[...] = cnd.reshape(n, chunks, per, cch).astype(bf16)
    ssend[...] = sig.reshape(n, chunks, per, ch).astype(bf16)
    h3[...] = sig

    pl.semaphore_wait(barrier, n - 1)
    for cp in halo_copies():
        cp.start()

    order = [n // 2]
    for d in range(n // 2 - 1, 0, -1):
        order += [n - d, d]
    order += [0]

    def push(src, dst, send_sem, recv_sem, d, to):
        if d == 0:
            pltpu.make_async_copy(src, dst, recv_sem).start()
        else:
            pltpu.make_async_remote_copy(src, dst, send_sem, recv_sem, device_id={"sp": to},
                                         device_id_type=MESH).start()

    def drain(buf, sem):
        pltpu.make_async_copy(buf, buf, sem).wait()

    for d in order:
        to = lax.rem(me + d, n)
        push(csend.at[to], crecv.at[me], x_send.at[chunks], x_recv.at[chunks], d, to)
        push(ssend.at[to, 0], srecv.at[0, me], x_send.at[0], x_recv.at[0], d, to)
    fetch(NEAR, NEAR + 1)

    for cp in halo_copies():
        cp.wait_recv()
    ins[2].wait()

    hr, hc = _iota((hrows, batch * HALO), 0), _iota((hrows, batch * HALO), 1)
    pick = (hc == (hr >> NEAR) * HALO + (HALO - RES) + (hr & (RES - 1))).astype(bf16)
    live = me > 0
    halo_h = jnp.dot(pick, halo_s[...].reshape(batch * HALO, ch), preferred_element_type=f32)
    halo_k = jnp.dot(pick, halo_c[...].reshape(batch * HALO, cch), preferred_element_type=f32)
    call = jnp.concatenate([cnd, halo_k], axis=0).astype(bf16)
    allr = own + hrows
    half = ch // 2

    def gate(x, k):
        parts = []
        for q in range(2):
            zf = jnp.dot(x, w1[k, :, q * half:(q + 1) * half], preferred_element_type=f32)
            zg = jnp.dot(x, w1[k, :, ch + q * half:ch + (q + 1) * half], preferred_element_type=f32)
            zf = zf + bias[k:k + 1, q * half:(q + 1) * half]
            zg = zg + bias[k:k + 1, ch + q * half:ch + (q + 1) * half]
            parts.append((jnp.tanh(zf) * (0.5 * jnp.tanh(0.5 * zg) + 0.5)).astype(bf16))
        return jnp.concatenate(parts, axis=1)

    for k in range(NEAR):
        d = 2 ** k
        u_halo = jnp.where(live, halo_h, 0.0)
        u = jnp.concatenate([h3[...], u_halo], axis=0).astype(bf16)
        r, c = _iota((allr, allr), 0), _iota((allr, allr), 1)
        seq, rho, step = r >> sh_span, (r >> sh_per) & (RES - 1), r & (per - 1)
        src = step * RES + rho - d
        own_col = seq * span + ((src & (RES - 1)) << sh_per) + (src >> NEAR)
        halo_col = own + seq * RES + src + RES
        col = jnp.where(src >= 0, own_col, halo_col)
        hseq, hrho = (r - own) >> NEAR, (r - own) & (RES - 1)
        col = jnp.where(r < own, col, jnp.where(hrho >= d, own + hseq * RES + hrho - d, -1))
        p = jnp.dot((c == col).astype(bf16), u, preferred_element_type=f32).astype(bf16)
        for cp in wcopies(k):
            cp.wait()
        a = gate(jnp.concatenate([u, p, call], axis=1), k)
        dlt = jnp.dot(a, w2[k], preferred_element_type=f32)
        if k == 0:
            near[...] = dlt[:own, :ch]
            s3[...] = dlt[:own, ch:]
        else:
            near[...] += dlt[:own, :ch]
            s3[...] += dlt[:own, ch:]
        h3[...] += dlt[:own, :ch]
        if k < NEAR - 1:
            halo_h = halo_h + dlt[own:, :ch]

    dsend[...] = near[...].reshape(n, chunks, per, ch).astype(TRAVEL)
    for ck in range(chunks):
        for d in order:
            to = lax.rem(me + d, n)
            if ck > 0:
                push(ssend.at[to, ck], srecv.at[ck, me], x_send.at[ck], x_recv.at[ck], d, to)
            push(dsend.at[to, ck], drecv.at[ck, me], d_send, d_recv.at[ck], d, to)
        if ck == 0:
            fetch(NEAR + 2, NEAR + 3)

    fetch(*range(NEAR + 4, layers))
    drain(crecv, x_recv.at[chunks])
    row = _iota((rows, ch), 0)
    for ck in range(chunks):
        drain(srecv.at[ck], x_recv.at[ck])
        drain(drecv.at[ck], d_recv.at[ck])
        base = (srecv[ck].astype(f32) + drecv[ck].astype(f32)).reshape(rows, ch)
        cq = crecv[:, ck].astype(f32).reshape(rows, cch).astype(bf16)
        h = base
        for k in range(NEAR, layers):
            sft = 2 ** (k - NEAR)
            if k > NEAR:
                h = base + far[:, 0:ch]
            if sft < 8:
                past = jnp.where(row >= sft, pltpu.roll(h, sft, 0), 0.0)
            else:
                past = jnp.concatenate([jnp.zeros((sft, ch), f32), h[:rows - sft]], axis=0)
            if ck == 0:
                for cp in wcopies(k):
                    cp.wait()
            a = gate(jnp.concatenate([h.astype(bf16), past.astype(bf16), cq], axis=1), k)
            dlt = jnp.dot(a, w2[k], preferred_element_type=f32)
            if k == NEAR:
                far[...] = dlt
            elif k < layers - 1:
                far[...] += dlt
            else:
                osend[ck] = (far[...] + dlt).reshape(n, per, wide).astype(TRAVEL)
        for d in order:
            to = lax.rem(me + d, n)
            push(osend.at[ck, to], recv.at[ck, me], o_send, o_recv.at[ck], d, to)

    for cp in halo_copies():
        cp.wait_send()
    for ck in range(chunks):
        drain(ssend.at[pl.ds(0, n - 1), ck], x_send.at[ck])
    for buf, sem in ((csend.at[pl.ds(0, n - 1)], x_send.at[chunks]), (dsend.at[pl.ds(0, n - 1)], d_send), (osend.at[:, pl.ds(0, n - 1)], o_send)):
        drain(buf, sem)
    for ck in range(chunks):
        drain(recv.at[ck], o_recv.at[ck])


def _finish(recv, h3, s3, hout_hbm, sout_hbm, obuf, out_sem):
    chunks, n, per, wide = recv.shape
    own, ch = h3.shape
    span = per * RES
    outs = []
    for t in range(wide // 128):
        lo = t * 128
        base, off = (h3, lo) if lo < ch else (s3, lo - ch)
        for ck in range(chunks):
            for j in range(n):
                cl = j * chunks + ck
                s, rho = cl // RES, cl % RES
                obuf[t, pl.ds(s * span + rho, per, RES), :] = (
                    recv[ck, j, :, lo:lo + 128].astype(f32) + base[cl * per:(cl + 1) * per, off:off + 128])
        dst = hout_hbm if lo < ch else sout_hbm
        outs.append(pltpu.make_async_copy(obuf.at[t], dst.at[:, pl.ds(off, 128)], out_sem.at[t]))
        outs[-1].start()
    for cp in outs:
        cp.wait()


def solution(mesh):
    n = mesh.shape['sp']

    def local_stack(signal, cond_feats, w_now, w_past, w_cond, b_gate, w_res, w_skip):
        batch, span, ch = signal.shape
        cch = cond_feats.shape[2]
        layers = w_now.shape[0]
        sk = w_skip.shape[2]
        wide = ch + sk
        own = batch * span
        per = span // RES
        chunks = batch * RES // n
        rows = n * per
        any_spec = pl.BlockSpec(memory_space=pl.ANY)
        dma = pltpu.SemaphoreType.DMA
        sds = jax.ShapeDtypeStruct
        recv, h3, s3 = pl.pallas_call(
            functools.partial(_stack, n),
            name="stack",
            out_shape=(pltpu.VMEM((chunks, n, per, wide), TRAVEL), pltpu.VMEM((own, ch), f32), pltpu.VMEM((own, sk), f32)),
            in_specs=[any_spec] * 8,
            out_specs=(pl.BlockSpec(memory_space=pltpu.VMEM),) * 3,
            scratch_shapes=[
                pltpu.VMEM((batch, span, ch), bf16), pltpu.VMEM((batch, span, cch), bf16),
                pltpu.VMEM((batch, HALO, ch), bf16), pltpu.VMEM((batch, HALO, cch), bf16),
                pltpu.VMEM((layers, 2 * ch + cch, 2 * ch), bf16), pltpu.VMEM((layers, ch, wide), bf16),
                pltpu.VMEM((layers, 2 * ch), f32),
                pltpu.VMEM((own, ch), f32),
                pltpu.VMEM((n, chunks, per, ch), bf16), pltpu.VMEM((n, chunks, per, cch), bf16),
                pltpu.VMEM((n, chunks, per, ch), TRAVEL),
                pltpu.VMEM((chunks, n, per, ch), bf16), pltpu.VMEM((n, chunks, per, cch), bf16),
                pltpu.VMEM((chunks, n, per, ch), TRAVEL),
                pltpu.VMEM((rows, wide), f32), pltpu.VMEM((chunks, n, per, wide), TRAVEL),
                dma((layers, 5)), dma((3,)), dma((2,)), dma((2,)), dma((chunks + 1,)), dma((chunks + 1,)),
                dma, dma((chunks,)), dma, dma((chunks,)),
            ],
            compiler_params=pltpu.CompilerParams(collective_id=0, has_side_effects=True,
                                                 vmem_limit_bytes=56 * 1024 * 1024),
        )(signal, cond_feats, w_now, w_past, w_cond, b_gate, w_res, w_skip)
        h_out, skip_out = pl.pallas_call(
            _finish,
            name="finish",
            out_shape=(sds((own, ch), f32), sds((own, sk), f32)),
            in_specs=[pl.BlockSpec(memory_space=pltpu.VMEM)] * 3,
            out_specs=(any_spec,) * 2,
            scratch_shapes=[
                pltpu.VMEM((wide // 128, own, 128), f32), dma((wide // 128,)),
            ],
        )(*(pltpu.with_memory_space_constraint(x, pltpu.VMEM) for x in (recv, h3, s3)))
        return h_out.reshape(batch, span, ch), skip_out.reshape(batch, span, sk)

    seq_spec = P('dp', 'sp', None)
    return jax.shard_map(local_stack, mesh=mesh,
                         in_specs=(seq_spec, seq_spec, P(), P(), P(), P(), P(), P()),
                         out_specs=(seq_spec, seq_spec), check_vma=False)
```

```python
import functools

import jax
import jax.numpy as jnp
from jax import lax
from jax.experimental import pallas as pl
from jax.experimental.pallas import tpu as pltpu
from jax.sharding import PartitionSpec as P

MESH = pl.DeviceIdType.MESH
NEAR = 3
RES = 2 ** NEAR
HALO = 16
f32, bf16 = jnp.float32, jnp.bfloat16
TRAVEL = bf16


def _iota(shape, dim):
    return lax.broadcasted_iota(jnp.int32, shape, dim)


def _stack(n, sig_hbm, cond_hbm, wn_hbm, wp_hbm, wc_hbm, bg_hbm, wr_hbm, ws_hbm,
           recv, h3, s3,
           sig_v, cond_v, halo_s, halo_c, w1, wc, w2, bias, zc, gates,
           near, ssend, csend, dsend, srecv, crecv, drecv, far, osend,
           w_sem, in_sem, halo_send, halo_recv, x_send, x_recv, d_send, d_recv, o_send, o_recv):
    me = lax.axis_index("sp")
    batch, span, ch = sig_v.shape
    cch = cond_v.shape[2]
    layers = w1.shape[0]
    own = batch * span
    per = span // RES
    ncls = batch * RES
    chunks = ncls // n
    rows = n * per
    wide = w2.shape[2]
    hrows = batch * RES
    sh_span, sh_per = span.bit_length() - 1, per.bit_length() - 1

    barrier = pltpu.get_barrier_semaphore()
    for d in range(1, n):
        pl.semaphore_signal(barrier, inc=1, device_id={"sp": lax.rem(me + d, n)}, device_id_type=MESH)

    ins = [pltpu.make_async_copy(sig_hbm, sig_v, in_sem.at[0]),
           pltpu.make_async_copy(cond_hbm, cond_v, in_sem.at[1]),
           pltpu.make_async_copy(bg_hbm, bias, in_sem.at[2])]
    for c in ins:
        c.start()

    def wcopies(k):
        return [pltpu.make_async_copy(wn_hbm.at[k], w1.at[k, pl.ds(0, ch)], w_sem.at[k, 0]),
                pltpu.make_async_copy(wp_hbm.at[k], w1.at[k, pl.ds(ch, ch)], w_sem.at[k, 1]),
                pltpu.make_async_copy(wr_hbm.at[k], w2.at[k, :, pl.ds(0, ch)], w_sem.at[k, 2]),
                pltpu.make_async_copy(ws_hbm.at[k], w2.at[k, :, pl.ds(ch, wide - ch)], w_sem.at[k, 3])]

    def ccopy(k):
        return pltpu.make_async_copy(wc_hbm.at[k], wc.at[k], w_sem.at[k, 4])

    def fetch(*ks):
        for k in ks:
            for c in wcopies(k):
                c.start()

    for k in range(NEAR):
        ccopy(k).start()
    fetch(0)

    def halo_copies():
        nxt = lax.rem(me + 1, n)
        return [pltpu.make_async_remote_copy(sig_v.at[:, pl.ds(span - HALO, HALO)], halo_s, halo_send.at[0],
                                             halo_recv.at[0], device_id={"sp": nxt}, device_id_type=MESH),
                pltpu.make_async_remote_copy(cond_v.at[:, pl.ds(span - HALO, HALO)], halo_c, halo_send.at[1],
                                             halo_recv.at[1], device_id={"sp": nxt}, device_id_type=MESH)]

    fetch(*range(1, NEAR))
    for k in range(NEAR, layers):
        ccopy(k).start()
    ins[0].wait()
    ins[1].wait()
    r, c = _iota((own, own), 0), _iota((own, own), 1)
    seq, rho, step = r >> sh_span, (r >> sh_per) & (RES - 1), r & (per - 1)
    perm = (c == seq * span + step * RES + rho).astype(bf16)
    cnd = jnp.dot(perm, cond_v[...].reshape(own, cch), preferred_element_type=f32)
    sig = jnp.dot(perm, sig_v[...].reshape(own, ch), preferred_element_type=f32)
    csend[...] = cnd.reshape(n, chunks, per, cch).astype(bf16)
    ssend[...] = sig.reshape(n, chunks, per, ch).astype(bf16)
    h3[...] = sig

    pl.semaphore_wait(barrier, n - 1)
    for cp in halo_copies():
        cp.start()

    order = [n // 2]
    for d in range(n // 2 - 1, 0, -1):
        order += [n - d, d]
    order += [0]

    def push(src, dst, send_sem, recv_sem, d, to):
        if d == 0:
            pltpu.make_async_copy(src, dst, recv_sem).start()
        else:
            pltpu.make_async_remote_copy(src, dst, send_sem, recv_sem, device_id={"sp": to},
                                         device_id_type=MESH).start()

    def drain(buf, sem):
        pltpu.make_async_copy(buf, buf, sem).wait()

    for d in order:
        to = lax.rem(me + d, n)
        push(csend.at[to], crecv.at[me], x_send.at[chunks], x_recv.at[chunks], d, to)
        push(ssend.at[to, 0], srecv.at[0, me], x_send.at[0], x_recv.at[0], d, to)
    fetch(NEAR, NEAR + 1)

    for cp in halo_copies():
        cp.wait_recv()
    ins[2].wait()

    hr, hc = _iota((hrows, batch * HALO), 0), _iota((hrows, batch * HALO), 1)
    pick = (hc == (hr >> NEAR) * HALO + (HALO - RES) + (hr & (RES - 1))).astype(bf16)
    live = me > 0
    halo_h = jnp.dot(pick, halo_s[...].reshape(batch * HALO, ch), preferred_element_type=f32)
    halo_k = jnp.dot(pick, halo_c[...].reshape(batch * HALO, cch), preferred_element_type=f32)
    call = jnp.concatenate([cnd, halo_k], axis=0).astype(bf16)
    allr = own + hrows
    half = ch // 2

    def gate(x, k, z0):
        parts = []
        for q in range(2):
            lo, hi = q * half, (q + 1) * half
            zf = jnp.dot(x, w1[k, :, lo:hi], preferred_element_type=f32) + z0(lo, hi)
            zg = jnp.dot(x, w1[k, :, ch + lo:ch + hi], preferred_element_type=f32) + z0(ch + lo, ch + hi)
            parts.append((jnp.tanh(zf) * (0.5 * jnp.tanh(0.5 * zg) + 0.5)).astype(bf16))
        return jnp.concatenate(parts, axis=1)

    for k in range(NEAR):
        d = 2 ** k
        u_halo = jnp.where(live, halo_h, 0.0)
        u = jnp.concatenate([h3[...], u_halo], axis=0).astype(bf16)
        r, c = _iota((allr, allr), 0), _iota((allr, allr), 1)
        seq, rho, step = r >> sh_span, (r >> sh_per) & (RES - 1), r & (per - 1)
        src = step * RES + rho - d
        own_col = seq * span + ((src & (RES - 1)) << sh_per) + (src >> NEAR)
        halo_col = own + seq * RES + src + RES
        col = jnp.where(src >= 0, own_col, halo_col)
        hseq, hrho = (r - own) >> NEAR, (r - own) & (RES - 1)
        col = jnp.where(r < own, col, jnp.where(hrho >= d, own + hseq * RES + hrho - d, -1))
        p = jnp.dot((c == col).astype(bf16), u, preferred_element_type=f32).astype(bf16)
        m = allr if k < NEAR - 1 else own
        ccopy(k).wait()
        zk = jnp.dot(call[:m], wc[k], preferred_element_type=f32) + bias[k:k + 1]
        for cp in wcopies(k):
            cp.wait()
        a = gate(jnp.concatenate([u[:m], p[:m]], axis=1), k, lambda lo, hi: zk[:, lo:hi])
        gates[k] = a[:own]
        dlt = jnp.dot(a, w2[k, :, 0:ch], preferred_element_type=f32)
        if k == 0:
            near[...] = dlt[:own]
        else:
            near[...] += dlt[:own]
        h3[...] += dlt[:own]
        if k < NEAR - 1:
            halo_h = halo_h + dlt[own:]

    dsend[...] = near[...].reshape(n, chunks, per, ch).astype(TRAVEL)
    for ck in range(chunks):
        for d in order:
            to = lax.rem(me + d, n)
            if ck > 0:
                push(ssend.at[to, ck], srecv.at[ck, me], x_send.at[ck], x_recv.at[ck], d, to)
            push(dsend.at[to, ck], drecv.at[ck, me], d_send, d_recv.at[ck], d, to)
        if ck == 0:
            fetch(NEAR + 2, NEAR + 3)

    fetch(*range(NEAR + 4, layers))
    skp = jnp.dot(gates[0], w2[0, :, ch:wide], preferred_element_type=f32)
    for k in range(1, NEAR):
        skp = skp + jnp.dot(gates[k], w2[k, :, ch:wide], preferred_element_type=f32)
    s3[...] = skp
    drain(crecv, x_recv.at[chunks])
    cq = jnp.concatenate([crecv[:, ck].astype(f32).reshape(rows, cch) for ck in range(chunks)], axis=0).astype(bf16)
    for k in range(NEAR, layers):
        ccopy(k).wait()
        zc[k - NEAR] = jnp.dot(cq, wc[k], preferred_element_type=f32) + bias[k:k + 1]

    row = _iota((rows, ch), 0)
    for ck in range(chunks):
        drain(srecv.at[ck], x_recv.at[ck])
        drain(drecv.at[ck], d_recv.at[ck])
        base = (srecv[ck].astype(f32) + drecv[ck].astype(f32)).reshape(rows, ch)
        h, a = base, None
        for k in range(NEAR, layers):
            sft = 2 ** (k - NEAR)
            if sft < 8:
                past = jnp.where(row >= sft, pltpu.roll(h, sft, 0), 0.0)
            else:
                past = jnp.concatenate([jnp.zeros((sft, ch), f32), h[:rows - sft]], axis=0)
            if ck == 0:
                for cp in wcopies(k):
                    cp.wait()
            was, z_rows = a, slice(ck * rows, (ck + 1) * rows)
            a = gate(jnp.concatenate([h.astype(bf16), past.astype(bf16)], axis=1), k,
                     lambda lo, hi: zc[k - NEAR, z_rows, lo:hi])
            if k == NEAR + 1:
                far[:, ch:wide] = jnp.dot(was, w2[k - 1, :, ch:wide], preferred_element_type=f32)
            elif k > NEAR + 1:
                far[:, ch:wide] += jnp.dot(was, w2[k - 1, :, ch:wide], preferred_element_type=f32)
            dlt = jnp.dot(a, w2[k, :, 0:ch], preferred_element_type=f32)
            if k == NEAR:
                far[:, 0:ch] = dlt
            elif k < layers - 1:
                far[:, 0:ch] += dlt
            if k < layers - 1:
                h = base + far[:, 0:ch]
        osend[ck, :, :, 0:ch] = (far[:, 0:ch] + dlt).reshape(n, per, ch).astype(TRAVEL)
        dlt = jnp.dot(a, w2[layers - 1, :, ch:wide], preferred_element_type=f32)
        osend[ck, :, :, ch:wide] = (far[:, ch:wide] + dlt).reshape(n, per, wide - ch).astype(TRAVEL)
        for d in order:
            to = lax.rem(me + d, n)
            push(osend.at[ck, to], recv.at[ck, me], o_send, o_recv.at[ck], d, to)

    for cp in halo_copies():
        cp.wait_send()
    for ck in range(chunks):
        drain(ssend.at[pl.ds(0, n - 1), ck], x_send.at[ck])
    for buf, sem in ((csend.at[pl.ds(0, n - 1)], x_send.at[chunks]), (dsend.at[pl.ds(0, n - 1)], d_send), (osend.at[:, pl.ds(0, n - 1)], o_send)):
        drain(buf, sem)
    for ck in range(chunks):
        drain(recv.at[ck], o_recv.at[ck])


def _finish(recv, h3, s3, hout_hbm, sout_hbm, obuf, out_sem):
    chunks, n, per, wide = recv.shape
    own, ch = h3.shape
    span = per * RES
    outs = []
    for t in range(wide // 128):
        lo = t * 128
        base, off = (h3, lo) if lo < ch else (s3, lo - ch)
        for ck in range(chunks):
            for j in range(n):
                cl = j * chunks + ck
                s, rho = cl // RES, cl % RES
                obuf[t, pl.ds(s * span + rho, per, RES), :] = (
                    recv[ck, j, :, lo:lo + 128].astype(f32) + base[cl * per:(cl + 1) * per, off:off + 128])
        dst = hout_hbm if lo < ch else sout_hbm
        outs.append(pltpu.make_async_copy(obuf.at[t], dst.at[:, pl.ds(off, 128)], out_sem.at[t]))
        outs[-1].start()
    for cp in outs:
        cp.wait()


def solution(mesh):
    n = mesh.shape['sp']

    def local_stack(signal, cond_feats, w_now, w_past, w_cond, b_gate, w_res, w_skip):
        batch, span, ch = signal.shape
        cch = cond_feats.shape[2]
        layers = w_now.shape[0]
        sk = w_skip.shape[2]
        wide = ch + sk
        own = batch * span
        per = span // RES
        chunks = batch * RES // n
        rows = n * per
        any_spec = pl.BlockSpec(memory_space=pl.ANY)
        dma = pltpu.SemaphoreType.DMA
        sds = jax.ShapeDtypeStruct
        recv, h3, s3 = pl.pallas_call(
            functools.partial(_stack, n),
            name="stack",
            out_shape=(pltpu.VMEM((chunks, n, per, wide), TRAVEL), pltpu.VMEM((own, ch), f32), pltpu.VMEM((own, sk), f32)),
            in_specs=[any_spec] * 8,
            out_specs=(pl.BlockSpec(memory_space=pltpu.VMEM),) * 3,
            scratch_shapes=[
                pltpu.VMEM((batch, span, ch), bf16), pltpu.VMEM((batch, span, cch), bf16),
                pltpu.VMEM((batch, HALO, ch), bf16), pltpu.VMEM((batch, HALO, cch), bf16),
                pltpu.VMEM((layers, 2 * ch, 2 * ch), bf16), pltpu.VMEM((layers, cch, 2 * ch), bf16),
                pltpu.VMEM((layers, ch, wide), bf16),
                pltpu.VMEM((layers, 2 * ch), f32), pltpu.VMEM((layers - NEAR, chunks * rows, 2 * ch), f32),
                pltpu.VMEM((NEAR, own, ch), bf16),
                pltpu.VMEM((own, ch), f32),
                pltpu.VMEM((n, chunks, per, ch), bf16), pltpu.VMEM((n, chunks, per, cch), bf16),
                pltpu.VMEM((n, chunks, per, ch), TRAVEL),
                pltpu.VMEM((chunks, n, per, ch), bf16), pltpu.VMEM((n, chunks, per, cch), bf16),
                pltpu.VMEM((chunks, n, per, ch), TRAVEL),
                pltpu.VMEM((rows, wide), f32), pltpu.VMEM((chunks, n, per, wide), TRAVEL),
                dma((layers, 5)), dma((3,)), dma((2,)), dma((2,)), dma((chunks + 1,)), dma((chunks + 1,)),
                dma, dma((chunks,)), dma, dma((chunks,)),
            ],
            compiler_params=pltpu.CompilerParams(collective_id=0, has_side_effects=True,
                                                 vmem_limit_bytes=56 * 1024 * 1024),
        )(signal, cond_feats, w_now, w_past, w_cond, b_gate, w_res, w_skip)
        h_out, skip_out = pl.pallas_call(
            _finish,
            name="finish",
            out_shape=(sds((own, ch), f32), sds((own, sk), f32)),
            in_specs=[pl.BlockSpec(memory_space=pltpu.VMEM)] * 3,
            out_specs=(any_spec,) * 2,
            scratch_shapes=[
                pltpu.VMEM((wide // 128, own, 128), f32), dma((wide // 128,)),
            ],
        )(*(pltpu.with_memory_space_constraint(x, pltpu.VMEM) for x in (recv, h3, s3)))
        return h_out.reshape(batch, span, ch), skip_out.reshape(batch, span, sk)

    seq_spec = P('dp', 'sp', None)
    return jax.shard_map(local_stack, mesh=mesh,
                         in_specs=(seq_spec, seq_spec, P(), P(), P(), P(), P(), P()),
                         out_specs=(seq_spec, seq_spec), check_vma=False)
```

```python
import functools

import jax
import jax.numpy as jnp
from jax import lax
from jax.experimental import pallas as pl
from jax.experimental.pallas import tpu as pltpu
from jax.sharding import PartitionSpec as P

MESH = pl.DeviceIdType.MESH
NEAR = 3
RES = 2 ** NEAR
HALO = 16
f32, bf16 = jnp.float32, jnp.bfloat16
TRAVEL = bf16


def _iota(shape, dim):
    return lax.broadcasted_iota(jnp.int32, shape, dim)


def _stack(n, sig_hbm, cond_hbm, wn_hbm, wp_hbm, wc_hbm, bg_hbm, wr_hbm, ws_hbm,
           recv, h3, s3,
           sig_v, cond_v, halo_s, halo_c, w1, wc, w2, bias, zc, gates,
           near, ssend, csend, dsend, srecv, crecv, drecv, osend,
           w_sem, in_sem, halo_send, halo_recv, x_send, x_recv, d_send, d_recv, o_send, o_recv):
    me = lax.axis_index("sp")
    batch, span, ch = sig_v.shape
    cch = cond_v.shape[2]
    layers = w1.shape[0]
    own = batch * span
    per = span // RES
    ncls = batch * RES
    chunks = ncls // n
    rows = n * per
    wide = w2.shape[2]
    hrows = batch * RES
    sh_span, sh_per = span.bit_length() - 1, per.bit_length() - 1

    barrier = pltpu.get_barrier_semaphore()
    for d in range(1, n):
        pl.semaphore_signal(barrier, inc=1, device_id={"sp": lax.rem(me + d, n)}, device_id_type=MESH)

    ins = [pltpu.make_async_copy(sig_hbm, sig_v, in_sem.at[0]),
           pltpu.make_async_copy(cond_hbm, cond_v, in_sem.at[1]),
           pltpu.make_async_copy(bg_hbm, bias, in_sem.at[2])]
    for c in ins:
        c.start()

    def wcopies(k):
        return [pltpu.make_async_copy(wn_hbm.at[k], w1.at[k, pl.ds(0, ch)], w_sem.at[k, 0]),
                pltpu.make_async_copy(wp_hbm.at[k], w1.at[k, pl.ds(ch, ch)], w_sem.at[k, 1]),
                pltpu.make_async_copy(wr_hbm.at[k], w2.at[k, :, pl.ds(0, ch)], w_sem.at[k, 2]),
                pltpu.make_async_copy(ws_hbm.at[k], w2.at[k, :, pl.ds(ch, wide - ch)], w_sem.at[k, 3])]

    def ccopy(k):
        return pltpu.make_async_copy(wc_hbm.at[k], wc.at[k], w_sem.at[k, 4])

    def fetch(*ks):
        for k in ks:
            for c in wcopies(k):
                c.start()

    for k in range(NEAR):
        ccopy(k).start()
    fetch(0)

    def halo_copies():
        nxt = lax.rem(me + 1, n)
        return [pltpu.make_async_remote_copy(sig_v.at[:, pl.ds(span - HALO, HALO)], halo_s, halo_send.at[0],
                                             halo_recv.at[0], device_id={"sp": nxt}, device_id_type=MESH),
                pltpu.make_async_remote_copy(cond_v.at[:, pl.ds(span - HALO, HALO)], halo_c, halo_send.at[1],
                                             halo_recv.at[1], device_id={"sp": nxt}, device_id_type=MESH)]

    fetch(*range(1, NEAR))
    for k in range(NEAR, layers):
        ccopy(k).start()
    ins[0].wait()
    ins[1].wait()
    blk = rows + hrows // chunks
    lg = (RES // chunks).bit_length() - 1

    def place(r):
        ck = (r >= blk).astype(jnp.int32)
        rr = r - ck * blk
        on_own = rr < rows
        o = jnp.where(on_own, rr >> sh_per, rr - rows)
        step = jnp.where(on_own, rr & (per - 1), -1)
        return o >> lg, (o & ((1 << lg) - 1)) * chunks + ck, step

    def row_of(seq, rho, step, one_chunk=False):
        ck = 0 if one_chunk else rho & (chunks - 1)
        o = seq * (1 << lg) + (rho >> (chunks.bit_length() - 1))
        return ck * blk + jnp.where(step >= 0, o * per + step, rows + o)

    r, c = _iota((own, own), 0), _iota((own, own), 1)
    seq, rho, step = place(r + hrows // chunks * (r >= rows).astype(jnp.int32))
    perm = (c == seq * span + step * RES + rho).astype(bf16)
    cnd = jnp.dot(perm, cond_v[...].reshape(own, cch), preferred_element_type=f32)
    sig = jnp.dot(perm, sig_v[...].reshape(own, ch), preferred_element_type=f32)
    csend[...] = cnd.reshape(chunks, n, per, cch).astype(bf16)
    ssend[...] = sig.reshape(chunks, n, per, ch).astype(bf16)
    h3[...] = sig

    pl.semaphore_wait(barrier, n - 1)
    for cp in halo_copies():
        cp.start()

    order = [n // 2]
    for d in range(n // 2 - 1, 0, -1):
        order += [n - d, d]
    order += [0]

    def push(src, dst, send_sem, recv_sem, d, to):
        if d == 0:
            pltpu.make_async_copy(src, dst, recv_sem).start()
        else:
            pltpu.make_async_remote_copy(src, dst, send_sem, recv_sem, device_id={"sp": to},
                                         device_id_type=MESH).start()

    def drain(buf, sem):
        pltpu.make_async_copy(buf, buf, sem).wait()

    for d in order:
        to = lax.rem(me + d, n)
        push(csend.at[:, to], crecv.at[:, me], x_send.at[chunks], x_recv.at[chunks], d, to)
        push(ssend.at[0, to], srecv.at[0, me], x_send.at[0], x_recv.at[0], d, to)
    fetch(NEAR, NEAR + 1)

    for cp in halo_copies():
        cp.wait_recv()
    ins[2].wait()

    hh = hrows // chunks
    hr, hc = _iota((hrows, batch * HALO), 0), _iota((hrows, batch * HALO), 1)
    hck = (hr >= hh).astype(jnp.int32)
    ho = hr - hck * hh
    pick = (hc == (ho >> lg) * HALO + (HALO - RES) + (ho & ((1 << lg) - 1)) * chunks + hck).astype(bf16)
    live = me > 0
    halo_h = jnp.dot(pick, halo_s[...].reshape(batch * HALO, ch), preferred_element_type=f32)
    halo_k = jnp.dot(pick, halo_c[...].reshape(batch * HALO, cch), preferred_element_type=f32)
    halo_h = jnp.where(live, halo_h, 0.0)
    mix = lambda x, y: jnp.concatenate([x[:rows], y[:hh], x[rows:], y[hh:]], axis=0)
    call = mix(cnd, halo_k).astype(bf16)
    half = ch // 2

    def gate(x, k, z0):
        parts = []
        for q in range(2):
            lo, hi = q * half, (q + 1) * half
            zf = jnp.dot(x, w1[k, :, lo:hi], preferred_element_type=f32) + z0(lo, hi)
            zg = jnp.dot(x, w1[k, :, ch + lo:ch + hi], preferred_element_type=f32) + z0(ch + lo, ch + hi)
            parts.append((jnp.tanh(zf) * (0.5 * jnp.tanh(0.5 * zg) + 0.5)).astype(bf16))
        return jnp.concatenate(parts, axis=1)

    def narrow(a, w, lo, hi):
        return [jnp.dot(a, w[:, c:min(c + 256, hi)], preferred_element_type=f32) for c in range(lo, hi, 256)]

    def near_layer(k, h, cnd_rows, halo_out):
        m = h.shape[0]
        u = h.astype(bf16)
        r, c = _iota((m, m), 0), _iota((m, m), 1)
        seq, rho, step = place(r)
        if m > blk:
            src = step * RES + rho - 2 ** k
            col = row_of(seq, src & (RES - 1), src >> NEAR)
        else:
            src = step * RES + rho - 2 ** k
            col = row_of(seq, src & (RES - 1), src >> NEAR, True)
        col = jnp.where(src >= -RES, col, -1)
        p = jnp.dot((c == col).astype(bf16), u, preferred_element_type=f32).astype(bf16)
        keep = m if halo_out else rows
        zk = jnp.dot(cnd_rows[:keep], wc[k], preferred_element_type=f32) + bias[k:k + 1]
        a = gate(jnp.concatenate([u[:keep], p[:keep]], axis=1), k, lambda lo, hi: zk[:, lo:hi])
        return a, jnp.concatenate(narrow(a, w2.at[k], 0, ch), axis=1)

    ccopy(0).wait()
    for cp in wcopies(0):
        cp.wait()
    h0 = mix(h3[...], halo_h)
    a, d0 = near_layer(0, h0, call, True)
    for ck in range(chunks):
        gates[0, ck * rows:(ck + 1) * rows] = a[ck * blk:ck * blk + rows]
    edge = (_iota((blk, ch), 0) < rows) | live
    for ck in range(chunks):
        part = slice(ck * blk, (ck + 1) * blk)
        out = slice(ck * rows, (ck + 1) * rows)
        acc = d0[part]
        for k in range(1, NEAR):
            if ck == 0:
                ccopy(k).wait()
                for cp in wcopies(k):
                    cp.wait()
            a, dk = near_layer(k, jnp.where(edge, h0[part] + acc, 0.0), call[part], k < NEAR - 1)
            gates[k, out] = a[:rows]
            acc = acc[:dk.shape[0]] + dk
        dsend[ck] = acc.reshape(n, per, ch).astype(TRAVEL)
        near[out] = acc
        for d in order:
            to = lax.rem(me + d, n)
            if ck > 0:
                push(ssend.at[ck, to], srecv.at[ck, me], x_send.at[ck], x_recv.at[ck], d, to)
            push(dsend.at[ck, to], drecv.at[ck, me], d_send, d_recv.at[ck], d, to)
        if ck == 0:
            fetch(NEAR + 2, NEAR + 3)
    fetch(*range(NEAR + 4, layers))

    skp = jnp.dot(gates[0], w2[0, :, ch:wide], preferred_element_type=f32)
    for k in range(1, NEAR):
        skp = skp + jnp.dot(gates[k], w2[k, :, ch:wide], preferred_element_type=f32)
    s3[...] = skp
    h3[...] += near[...]
    drain(crecv, x_recv.at[chunks])
    cq = jnp.concatenate([crecv[ck].astype(f32).reshape(rows, cch) for ck in range(chunks)], axis=0).astype(bf16)
    for k in range(NEAR, layers):
        ccopy(k).wait()
        zc[k - NEAR] = jnp.dot(cq, wc[k], preferred_element_type=f32) + bias[k:k + 1]

    def late_skip(a, k):
        return (jnp.dot(a[:, :half], w2[k, :half, ch:wide], preferred_element_type=f32)
                + jnp.dot(a[:, half:], w2[k, half:, ch:wide], preferred_element_type=f32))

    row = _iota((rows, ch), 0)
    for ck in range(chunks):
        drain(srecv.at[ck], x_recv.at[ck])
        drain(drecv.at[ck], d_recv.at[ck])
        base = (srecv[ck].astype(f32) + drecv[ck].astype(f32)).reshape(rows, ch)
        h, a, acc, skips = base, None, None, []
        for k in range(NEAR, layers):
            sft = 2 ** (k - NEAR)
            if sft < 8:
                past = jnp.where(row >= sft, pltpu.roll(h, sft, 0), 0.0)
            else:
                past = jnp.concatenate([jnp.zeros((sft, ch), f32), h[:rows - sft]], axis=0)
            if ck == 0:
                for cp in wcopies(k):
                    cp.wait()
            was, z_rows = a, slice(ck * rows, (ck + 1) * rows)
            a = gate(jnp.concatenate([h.astype(bf16), past.astype(bf16)], axis=1), k,
                     lambda lo, hi: zc[k - NEAR, z_rows, lo:hi])
            if k > NEAR:
                skips.append(late_skip(was, k - 1))
            dlt = jnp.concatenate(narrow(a, w2.at[k], 0, ch), axis=1)
            acc = dlt if k == NEAR else acc + dlt
            h = base + acc
        osend[ck, :, :, 0:ch] = acc.reshape(n, per, ch).astype(TRAVEL)
        skips.append(late_skip(a, layers - 1))
        osend[ck, :, :, ch:wide] = sum(skips[1:], skips[0]).reshape(n, per, wide - ch).astype(TRAVEL)
        for d in order:
            to = lax.rem(me + d, n)
            push(osend.at[ck, to], recv.at[ck, me], o_send, o_recv.at[ck], d, to)

    for cp in halo_copies():
        cp.wait_send()
    for ck in range(chunks):
        drain(ssend.at[ck, pl.ds(0, n - 1)], x_send.at[ck])
    for buf, sem in ((csend.at[:, pl.ds(0, n - 1)], x_send.at[chunks]), (dsend.at[:, pl.ds(0, n - 1)], d_send), (osend.at[:, pl.ds(0, n - 1)], o_send)):
        drain(buf, sem)
    for ck in range(chunks):
        drain(recv.at[ck], o_recv.at[ck])


def _finish(recv, h3, s3, hout_hbm, sout_hbm, obuf, out_sem):
    chunks, n, per, wide = recv.shape
    own, ch = h3.shape
    span = per * RES
    outs = []
    for t in range(wide // 128):
        lo = t * 128
        base, off = (h3, lo) if lo < ch else (s3, lo - ch)
        for ck in range(chunks):
            for j in range(n):
                cl = j * chunks + ck
                s, rho = cl // RES, cl % RES
                at = (ck * n + j) * per
                obuf[t, pl.ds(s * span + rho, per, RES), :] = (
                    recv[ck, j, :, lo:lo + 128].astype(f32) + base[at:at + per, off:off + 128])
        dst = hout_hbm if lo < ch else sout_hbm
        outs.append(pltpu.make_async_copy(obuf.at[t], dst.at[:, pl.ds(off, 128)], out_sem.at[t]))
        outs[-1].start()
    for cp in outs:
        cp.wait()


def solution(mesh):
    n = mesh.shape['sp']

    def local_stack(signal, cond_feats, w_now, w_past, w_cond, b_gate, w_res, w_skip):
        batch, span, ch = signal.shape
        cch = cond_feats.shape[2]
        layers = w_now.shape[0]
        sk = w_skip.shape[2]
        wide = ch + sk
        own = batch * span
        per = span // RES
        chunks = batch * RES // n
        rows = n * per
        any_spec = pl.BlockSpec(memory_space=pl.ANY)
        dma = pltpu.SemaphoreType.DMA
        sds = jax.ShapeDtypeStruct
        recv, h3, s3 = pl.pallas_call(
            functools.partial(_stack, n),
            name="stack",
            out_shape=(pltpu.VMEM((chunks, n, per, wide), TRAVEL), pltpu.VMEM((own, ch), f32), pltpu.VMEM((own, sk), f32)),
            in_specs=[any_spec] * 8,
            out_specs=(pl.BlockSpec(memory_space=pltpu.VMEM),) * 3,
            scratch_shapes=[
                pltpu.VMEM((batch, span, ch), bf16), pltpu.VMEM((batch, span, cch), bf16),
                pltpu.VMEM((batch, HALO, ch), bf16), pltpu.VMEM((batch, HALO, cch), bf16),
                pltpu.VMEM((layers, 2 * ch, 2 * ch), bf16), pltpu.VMEM((layers, cch, 2 * ch), bf16),
                pltpu.VMEM((layers, ch, wide), bf16),
                pltpu.VMEM((layers, 2 * ch), f32), pltpu.VMEM((layers - NEAR, chunks * rows, 2 * ch), f32),
                pltpu.VMEM((NEAR, own, ch), bf16),
                pltpu.VMEM((own, ch), f32),
                pltpu.VMEM((chunks, n, per, ch), bf16), pltpu.VMEM((chunks, n, per, cch), bf16),
                pltpu.VMEM((chunks, n, per, ch), TRAVEL),
                pltpu.VMEM((chunks, n, per, ch), bf16), pltpu.VMEM((chunks, n, per, cch), bf16),
                pltpu.VMEM((chunks, n, per, ch), TRAVEL),
                pltpu.VMEM((chunks, n, per, wide), TRAVEL),
                dma((layers, 5)), dma((3,)), dma((2,)), dma((2,)), dma((chunks + 1,)), dma((chunks + 1,)),
                dma, dma((chunks,)), dma, dma((chunks,)),
            ],
            compiler_params=pltpu.CompilerParams(collective_id=0, has_side_effects=True,
                                                 vmem_limit_bytes=56 * 1024 * 1024),
        )(signal, cond_feats, w_now, w_past, w_cond, b_gate, w_res, w_skip)
        h_out, skip_out = pl.pallas_call(
            _finish,
            name="finish",
            out_shape=(sds((own, ch), f32), sds((own, sk), f32)),
            in_specs=[pl.BlockSpec(memory_space=pltpu.VMEM)] * 3,
            out_specs=(any_spec,) * 2,
            scratch_shapes=[
                pltpu.VMEM((wide // 128, own, 128), f32), dma((wide // 128,)),
            ],
        )(*(pltpu.with_memory_space_constraint(x, pltpu.VMEM) for x in (recv, h3, s3)))
        return h_out.reshape(batch, span, ch), skip_out.reshape(batch, span, sk)

    seq_spec = P('dp', 'sp', None)
    return jax.shard_map(local_stack, mesh=mesh,
                         in_specs=(seq_spec, seq_spec, P(), P(), P(), P(), P(), P()),
                         out_specs=(seq_spec, seq_spec), check_vma=False)
```

```python
import functools

import jax
import jax.numpy as jnp
from jax import lax
from jax.experimental import pallas as pl
from jax.experimental.pallas import tpu as pltpu
from jax.sharding import PartitionSpec as P

MESH = pl.DeviceIdType.MESH
NEAR = 3
RES = 2 ** NEAR
HALO = 16
f32, bf16 = jnp.float32, jnp.bfloat16
LEAD = 3
TRAVEL = bf16


def _iota(shape, dim):
    return lax.broadcasted_iota(jnp.int32, shape, dim)


def _stack(n, sig_hbm, cond_hbm, wn_hbm, wp_hbm, wc_hbm, bg_hbm, wr_hbm, ws_hbm,
           recv, h3, s3,
           sig_v, cond_v, halo_s, halo_c, w1, wc, w2, bias, zc, gates,
           near, ssend, csend, dsend, srecv, crecv, drecv, osend,
           w_sem, in_sem, halo_send, halo_recv, x_send, x_recv, d_send, d_recv, o_send, o_recv):
    me = lax.axis_index("sp")
    batch, span, ch = sig_v.shape
    cch = cond_v.shape[2]
    layers = w1.shape[0]
    own = batch * span
    per = span // RES
    ncls = batch * RES
    chunks = ncls // n
    rows = n * per
    wide = w2.shape[2]
    hrows = batch * RES
    sh_span, sh_per = span.bit_length() - 1, per.bit_length() - 1

    barrier = pltpu.get_barrier_semaphore()
    for d in range(1, n):
        pl.semaphore_signal(barrier, inc=1, device_id={"sp": lax.rem(me + d, n)}, device_id_type=MESH)

    ins = [pltpu.make_async_copy(sig_hbm, sig_v, in_sem.at[0]),
           pltpu.make_async_copy(cond_hbm, cond_v, in_sem.at[1]),
           pltpu.make_async_copy(bg_hbm, bias, in_sem.at[2])]
    for c in ins:
        c.start()

    def wcopies(k):
        return [pltpu.make_async_copy(wn_hbm.at[k], w1.at[k, pl.ds(0, ch)], w_sem.at[k, 0]),
                pltpu.make_async_copy(wp_hbm.at[k], w1.at[k, pl.ds(ch, ch)], w_sem.at[k, 1]),
                pltpu.make_async_copy(wr_hbm.at[k], w2.at[k, :, pl.ds(0, ch)], w_sem.at[k, 2]),
                pltpu.make_async_copy(ws_hbm.at[k], w2.at[k, :, pl.ds(ch, wide - ch)], w_sem.at[k, 3])]

    def ccopy(k):
        return pltpu.make_async_copy(wc_hbm.at[k], wc.at[k], w_sem.at[k, 4])

    def fetch(*ks):
        for k in ks:
            for c in wcopies(k):
                c.start()

    for k in range(NEAR):
        ccopy(k).start()
    fetch(0)

    def halo_copies():
        nxt = lax.rem(me + 1, n)
        return [pltpu.make_async_remote_copy(sig_v.at[:, pl.ds(span - HALO, HALO)], halo_s, halo_send.at[0],
                                             halo_recv.at[0], device_id={"sp": nxt}, device_id_type=MESH),
                pltpu.make_async_remote_copy(cond_v.at[:, pl.ds(span - HALO, HALO)], halo_c, halo_send.at[1],
                                             halo_recv.at[1], device_id={"sp": nxt}, device_id_type=MESH)]

    fetch(*range(1, NEAR))
    for k in range(NEAR, layers):
        ccopy(k).start()
    ins[0].wait()
    ins[1].wait()
    blk = rows + hrows // chunks
    lg = (RES // chunks).bit_length() - 1

    def place(r):
        ck = (r >= blk).astype(jnp.int32)
        rr = r - ck * blk
        on_own = rr < rows
        o = jnp.where(on_own, rr >> sh_per, rr - rows)
        step = jnp.where(on_own, rr & (per - 1), -1)
        return o >> lg, (o & ((1 << lg) - 1)) * chunks + ck, step

    def row_of(seq, rho, step, one_chunk=False):
        ck = 0 if one_chunk else rho & (chunks - 1)
        o = seq * (1 << lg) + (rho >> (chunks.bit_length() - 1))
        return ck * blk + jnp.where(step >= 0, o * per + step, rows + o)

    r, c = _iota((own, own), 0), _iota((own, own), 1)
    seq, rho, step = place(r + hrows // chunks * (r >= rows).astype(jnp.int32))
    perm = (c == seq * span + step * RES + rho).astype(bf16)
    cnd = jnp.dot(perm, cond_v[...].reshape(own, cch), preferred_element_type=f32)
    sig = jnp.dot(perm, sig_v[...].reshape(own, ch), preferred_element_type=f32)
    csend[...] = cnd.reshape(chunks, n, per, cch).astype(bf16)
    ssend[...] = sig.reshape(chunks, n, per, ch).astype(bf16)
    h3[...] = sig

    pl.semaphore_wait(barrier, n - 1)
    for cp in halo_copies():
        cp.start()

    order = [n // 2]
    for d in range(n // 2 - 1, 0, -1):
        order += [n - d, d]
    order += [0]

    def push(src, dst, send_sem, recv_sem, d, to):
        if d == 0:
            pltpu.make_async_copy(src, dst, recv_sem).start()
        else:
            pltpu.make_async_remote_copy(src, dst, send_sem, recv_sem, device_id={"sp": to},
                                         device_id_type=MESH).start()

    def drain(buf, sem):
        pltpu.make_async_copy(buf, buf, sem).wait()

    for d in order:
        to = lax.rem(me + d, n)
        push(ssend.at[:, to], srecv.at[:, me], x_send.at[0], x_recv.at[0], d, to)
        push(csend.at[:, to], crecv.at[:, me], x_send.at[1], x_recv.at[1], d, to)
    fetch(NEAR, NEAR + 1)

    for cp in halo_copies():
        cp.wait_recv()
    ins[2].wait()

    hh = hrows // chunks
    hr, hc = _iota((hrows, batch * HALO), 0), _iota((hrows, batch * HALO), 1)
    hck = (hr >= hh).astype(jnp.int32)
    ho = hr - hck * hh
    pick = (hc == (ho >> lg) * HALO + (HALO - RES) + (ho & ((1 << lg) - 1)) * chunks + hck).astype(bf16)
    live = me > 0
    halo_h = jnp.dot(pick, halo_s[...].reshape(batch * HALO, ch), preferred_element_type=f32)
    halo_k = jnp.dot(pick, halo_c[...].reshape(batch * HALO, cch), preferred_element_type=f32)
    halo_h = jnp.where(live, halo_h, 0.0)
    mix = lambda x, y: jnp.concatenate([x[:rows], y[:hh], x[rows:], y[hh:]], axis=0)
    call = mix(cnd, halo_k).astype(bf16)
    half = ch // 2

    def gate(x, k, z0):
        parts = []
        for q in range(2):
            lo, hi = q * half, (q + 1) * half
            zf = jnp.dot(x, w1[k, :, lo:hi], preferred_element_type=f32) + z0(lo, hi)
            zg = jnp.dot(x, w1[k, :, ch + lo:ch + hi], preferred_element_type=f32) + z0(ch + lo, ch + hi)
            parts.append((jnp.tanh(zf) * (0.5 * jnp.tanh(0.5 * zg) + 0.5)).astype(bf16))
        return jnp.concatenate(parts, axis=1)

    def narrow(a, w, lo, hi):
        return [jnp.dot(a, w[:, c:min(c + 256, hi)], preferred_element_type=f32) for c in range(lo, hi, 256)]

    def near_layer(k, h, cnd_rows, halo_out):
        m = h.shape[0]
        u = h.astype(bf16)
        r, c = _iota((m, m), 0), _iota((m, m), 1)
        seq, rho, step = place(r)
        if m > blk:
            src = step * RES + rho - 2 ** k
            col = row_of(seq, src & (RES - 1), src >> NEAR)
        else:
            src = step * RES + rho - 2 ** k
            col = row_of(seq, src & (RES - 1), src >> NEAR, True)
        col = jnp.where(src >= -RES, col, -1)
        p = jnp.dot((c == col).astype(bf16), u, preferred_element_type=f32).astype(bf16)
        keep = m if halo_out else rows
        zk = jnp.dot(cnd_rows[:keep], wc[k], preferred_element_type=f32) + bias[k:k + 1]
        a = gate(jnp.concatenate([u[:keep], p[:keep]], axis=1), k, lambda lo, hi: zk[:, lo:hi])
        return a, jnp.concatenate(narrow(a, w2.at[k], 0, ch), axis=1)

    ccopy(0).wait()
    for cp in wcopies(0):
        cp.wait()
    h0 = mix(h3[...], halo_h)
    a, d0 = near_layer(0, h0, call, True)
    for ck in range(chunks):
        gates[0, ck * rows:(ck + 1) * rows] = a[ck * blk:ck * blk + rows]
    edge = (_iota((blk, ch), 0) < rows) | live
    for ck in range(chunks):
        part = slice(ck * blk, (ck + 1) * blk)
        out = slice(ck * rows, (ck + 1) * rows)
        acc = d0[part]
        for k in range(1, NEAR):
            if ck == 0:
                ccopy(k).wait()
                for cp in wcopies(k):
                    cp.wait()
            a, dk = near_layer(k, jnp.where(edge, h0[part] + acc, 0.0), call[part], k < NEAR - 1)
            gates[k, out] = a[:rows]
            acc = acc[:dk.shape[0]] + dk
        dsend[ck] = acc.reshape(n, per, ch).astype(TRAVEL)
        near[out] = acc
        for d in order:
            to = lax.rem(me + d, n)
            push(dsend.at[ck, to], drecv.at[ck, me], d_send, d_recv.at[ck], d, to)
        if ck == 0:
            fetch(NEAR + 2, NEAR + 3)
    fetch(*range(NEAR + 4, layers))

    skp = jnp.dot(gates[0], w2[0, :, ch:wide], preferred_element_type=f32)
    for k in range(1, NEAR):
        skp = skp + jnp.dot(gates[k], w2[k, :, ch:wide], preferred_element_type=f32)
    s3[...] = skp
    h3[...] += near[...]
    drain(crecv, x_recv.at[1])
    cq = jnp.concatenate([crecv[ck].astype(f32).reshape(rows, cch) for ck in range(chunks)], axis=0).astype(bf16)
    for k in range(NEAR, layers):
        ccopy(k).wait()
        zc[k - NEAR] = jnp.dot(cq, wc[k], preferred_element_type=f32) + bias[k:k + 1]

    def late_skip(a, k):
        return (jnp.dot(a[:, :half], w2[k, :half, ch:wide], preferred_element_type=f32)
                + jnp.dot(a[:, half:], w2[k, half:, ch:wide], preferred_element_type=f32))

    row = _iota((rows, ch), 0)
    drain(srecv, x_recv.at[0])
    base, acc, act, skips = [None] * chunks, [None] * chunks, [None] * chunks, [[] for _ in range(chunks)]

    def begin(ck):
        drain(drecv.at[ck], d_recv.at[ck])
        base[ck] = (srecv[ck].astype(f32) + drecv[ck].astype(f32)).reshape(rows, ch)

    def first_half(ck, k):
        h = base[ck] if k == NEAR else base[ck] + acc[ck]
        sft = 2 ** (k - NEAR)
        if sft < 8:
            past = jnp.where(row >= sft, pltpu.roll(h, sft, 0), 0.0)
        else:
            past = jnp.concatenate([jnp.zeros((sft, ch), f32), h[:rows - sft]], axis=0)
        if ck == 0:
            for cp in wcopies(k):
                cp.wait()
        z_rows = slice(ck * rows, (ck + 1) * rows)
        return gate(jnp.concatenate([h.astype(bf16), past.astype(bf16)], axis=1), k,
                    lambda lo, hi: zc[k - NEAR, z_rows, lo:hi])

    def second_half(ck, k, a):
        if k > NEAR:
            skips[ck].append(late_skip(act[ck], k - 1))
        act[ck] = a
        dlt = jnp.concatenate(narrow(a, w2.at[k], 0, ch), axis=1)
        acc[ck] = dlt if k == NEAR else acc[ck] + dlt

    def send_back(ck):
        osend[ck, :, :, 0:ch] = acc[ck].reshape(n, per, ch).astype(TRAVEL)
        skips[ck].append(late_skip(act[ck], layers - 1))
        osend[ck, :, :, ch:wide] = sum(skips[ck][1:], skips[ck][0]).reshape(n, per, wide - ch).astype(TRAVEL)
        for d in order:
            to = lax.rem(me + d, n)
            push(osend.at[ck, to], recv.at[ck, me], o_send, o_recv.at[ck], d, to)

    begin(0)
    for k in range(NEAR, NEAR + LEAD):
        second_half(0, k, first_half(0, k))
    begin(1)
    for k in range(NEAR + LEAD, layers):
        a0 = first_half(0, k)
        a1 = first_half(1, k - LEAD)
        second_half(0, k, a0)
        second_half(1, k - LEAD, a1)
    send_back(0)
    for k in range(layers - LEAD, layers):
        second_half(1, k, first_half(1, k))
    send_back(1)

    for cp in halo_copies():
        cp.wait_send()
    for buf, sem in ((ssend.at[:, pl.ds(0, n - 1)], x_send.at[0]), (csend.at[:, pl.ds(0, n - 1)], x_send.at[1]), (dsend.at[:, pl.ds(0, n - 1)], d_send), (osend.at[:, pl.ds(0, n - 1)], o_send)):
        drain(buf, sem)
    for ck in range(chunks):
        drain(recv.at[ck], o_recv.at[ck])


def _finish(recv, h3, s3, hout_hbm, sout_hbm, obuf, out_sem):
    chunks, n, per, wide = recv.shape
    own, ch = h3.shape
    span = per * RES
    outs = []
    for t in range(wide // 128):
        lo = t * 128
        base, off = (h3, lo) if lo < ch else (s3, lo - ch)
        for ck in range(chunks):
            for j in range(n):
                cl = j * chunks + ck
                s, rho = cl // RES, cl % RES
                at = (ck * n + j) * per
                obuf[t, pl.ds(s * span + rho, per, RES), :] = (
                    recv[ck, j, :, lo:lo + 128].astype(f32) + base[at:at + per, off:off + 128])
        dst = hout_hbm if lo < ch else sout_hbm
        outs.append(pltpu.make_async_copy(obuf.at[t], dst.at[:, pl.ds(off, 128)], out_sem.at[t]))
        outs[-1].start()
    for cp in outs:
        cp.wait()


def solution(mesh):
    n = mesh.shape['sp']

    def local_stack(signal, cond_feats, w_now, w_past, w_cond, b_gate, w_res, w_skip):
        batch, span, ch = signal.shape
        cch = cond_feats.shape[2]
        layers = w_now.shape[0]
        sk = w_skip.shape[2]
        wide = ch + sk
        own = batch * span
        per = span // RES
        chunks = batch * RES // n
        rows = n * per
        any_spec = pl.BlockSpec(memory_space=pl.ANY)
        dma = pltpu.SemaphoreType.DMA
        sds = jax.ShapeDtypeStruct
        recv, h3, s3 = pl.pallas_call(
            functools.partial(_stack, n),
            name="stack",
            out_shape=(pltpu.VMEM((chunks, n, per, wide), TRAVEL), pltpu.VMEM((own, ch), f32), pltpu.VMEM((own, sk), f32)),
            in_specs=[any_spec] * 8,
            out_specs=(pl.BlockSpec(memory_space=pltpu.VMEM),) * 3,
            scratch_shapes=[
                pltpu.VMEM((batch, span, ch), bf16), pltpu.VMEM((batch, span, cch), bf16),
                pltpu.VMEM((batch, HALO, ch), bf16), pltpu.VMEM((batch, HALO, cch), bf16),
                pltpu.VMEM((layers, 2 * ch, 2 * ch), bf16), pltpu.VMEM((layers, cch, 2 * ch), bf16),
                pltpu.VMEM((layers, ch, wide), bf16),
                pltpu.VMEM((layers, 2 * ch), f32), pltpu.VMEM((layers - NEAR, chunks * rows, 2 * ch), f32),
                pltpu.VMEM((NEAR, own, ch), bf16),
                pltpu.VMEM((own, ch), f32),
                pltpu.VMEM((chunks, n, per, ch), bf16), pltpu.VMEM((chunks, n, per, cch), bf16),
                pltpu.VMEM((chunks, n, per, ch), TRAVEL),
                pltpu.VMEM((chunks, n, per, ch), bf16), pltpu.VMEM((chunks, n, per, cch), bf16),
                pltpu.VMEM((chunks, n, per, ch), TRAVEL),
                pltpu.VMEM((chunks, n, per, wide), TRAVEL),
                dma((layers, 5)), dma((3,)), dma((2,)), dma((2,)), dma((2,)), dma((2,)),
                dma, dma((chunks,)), dma, dma((chunks,)),
            ],
            compiler_params=pltpu.CompilerParams(collective_id=0, has_side_effects=True,
                                                 vmem_limit_bytes=56 * 1024 * 1024),
        )(signal, cond_feats, w_now, w_past, w_cond, b_gate, w_res, w_skip)
        h_out, skip_out = pl.pallas_call(
            _finish,
            name="finish",
            out_shape=(sds((own, ch), f32), sds((own, sk), f32)),
            in_specs=[pl.BlockSpec(memory_space=pltpu.VMEM)] * 3,
            out_specs=(any_spec,) * 2,
            scratch_shapes=[
                pltpu.VMEM((wide // 128, own, 128), f32), dma((wide // 128,)),
            ],
        )(*(pltpu.with_memory_space_constraint(x, pltpu.VMEM) for x in (recv, h3, s3)))
        return h_out.reshape(batch, span, ch), skip_out.reshape(batch, span, sk)

    seq_spec = P('dp', 'sp', None)
    return jax.shard_map(local_stack, mesh=mesh,
                         in_specs=(seq_spec, seq_spec, P(), P(), P(), P(), P(), P()),
                         out_specs=(seq_spec, seq_spec), check_vma=False)
```

```python
import functools

import jax
import jax.numpy as jnp
from jax import lax
from jax.experimental import pallas as pl
from jax.experimental.pallas import tpu as pltpu
from jax.sharding import PartitionSpec as P

MESH = pl.DeviceIdType.MESH
NEAR = 3
RES = 2 ** NEAR
HALO = 16
f32, bf16 = jnp.float32, jnp.bfloat16
LEAD = 7
TRAVEL = bf16


def _iota(shape, dim):
    return lax.broadcasted_iota(jnp.int32, shape, dim)


def _stack(n, sig_hbm, cond_hbm, wn_hbm, wp_hbm, wc_hbm, bg_hbm, wr_hbm, ws_hbm,
           recv, h3, s3,
           sig_v, cond_v, halo_s, halo_c, w1, wc, w2, bias, zc, gates,
           near, ssend, csend, dsend, srecv, crecv, drecv, osend,
           w_sem, in_sem, halo_send, halo_recv, x_send, x_recv, d_send, d_recv, o_send, o_recv):
    me = lax.axis_index("sp")
    batch, span, ch = sig_v.shape
    cch = cond_v.shape[2]
    layers = w1.shape[0]
    own = batch * span
    per = span // RES
    ncls = batch * RES
    chunks = ncls // n
    rows = n * per
    wide = w2.shape[2]
    hrows = batch * RES
    sh_span, sh_per = span.bit_length() - 1, per.bit_length() - 1

    barrier = pltpu.get_barrier_semaphore()
    for d in range(1, n):
        pl.semaphore_signal(barrier, inc=1, device_id={"sp": lax.rem(me + d, n)}, device_id_type=MESH)

    ins = [pltpu.make_async_copy(sig_hbm, sig_v, in_sem.at[0]),
           pltpu.make_async_copy(cond_hbm, cond_v, in_sem.at[1]),
           pltpu.make_async_copy(bg_hbm, bias, in_sem.at[2])]
    for c in ins:
        c.start()

    def wcopies(k):
        return [pltpu.make_async_copy(wn_hbm.at[k], w1.at[k, pl.ds(0, ch)], w_sem.at[k, 0]),
                pltpu.make_async_copy(wp_hbm.at[k], w1.at[k, pl.ds(ch, ch)], w_sem.at[k, 1]),
                pltpu.make_async_copy(wr_hbm.at[k], w2.at[k, :, pl.ds(0, ch)], w_sem.at[k, 2]),
                pltpu.make_async_copy(ws_hbm.at[k], w2.at[k, :, pl.ds(ch, wide - ch)], w_sem.at[k, 3])]

    def ccopy(k):
        return pltpu.make_async_copy(wc_hbm.at[k], wc.at[k], w_sem.at[k, 4])

    def fetch(*ks):
        for k in ks:
            for c in wcopies(k):
                c.start()

    for k in range(NEAR):
        ccopy(k).start()
    fetch(0)

    def halo_copies():
        nxt = lax.rem(me + 1, n)
        return [pltpu.make_async_remote_copy(sig_v.at[:, pl.ds(span - HALO, HALO)], halo_s, halo_send.at[0],
                                             halo_recv.at[0], device_id={"sp": nxt}, device_id_type=MESH),
                pltpu.make_async_remote_copy(cond_v.at[:, pl.ds(span - HALO, HALO)], halo_c, halo_send.at[1],
                                             halo_recv.at[1], device_id={"sp": nxt}, device_id_type=MESH)]

    fetch(*range(1, NEAR))
    for k in range(NEAR, layers):
        ccopy(k).start()
    ins[0].wait()
    ins[1].wait()
    blk = rows + hrows // chunks
    lg = (RES // chunks).bit_length() - 1

    def place(r):
        ck = (r >= blk).astype(jnp.int32)
        rr = r - ck * blk
        on_own = rr < rows
        o = jnp.where(on_own, rr >> sh_per, rr - rows)
        step = jnp.where(on_own, rr & (per - 1), -1)
        return o >> lg, (o & ((1 << lg) - 1)) * chunks + ck, step

    def row_of(seq, rho, step, one_chunk=False):
        ck = 0 if one_chunk else rho & (chunks - 1)
        o = seq * (1 << lg) + (rho >> (chunks.bit_length() - 1))
        return ck * blk + jnp.where(step >= 0, o * per + step, rows + o)

    r, c = _iota((own, own), 0), _iota((own, own), 1)
    seq, rho, step = place(r + hrows // chunks * (r >= rows).astype(jnp.int32))
    perm = (c == seq * span + step * RES + rho).astype(bf16)
    cnd = jnp.dot(perm, cond_v[...].reshape(own, cch), preferred_element_type=f32)
    sig = jnp.dot(perm, sig_v[...].reshape(own, ch), preferred_element_type=f32)
    csend[...] = cnd.reshape(chunks, n, per, cch).astype(bf16)
    ssend[...] = sig.reshape(chunks, n, per, ch).astype(bf16)
    h3[...] = sig

    pl.semaphore_wait(barrier, n - 1)
    for cp in halo_copies():
        cp.start()

    order = [n // 2]
    for d in range(n // 2 - 1, 0, -1):
        order += [n - d, d]
    order += [0]

    def push(src, dst, send_sem, recv_sem, d, to):
        if d == 0:
            pltpu.make_async_copy(src, dst, recv_sem).start()
        else:
            pltpu.make_async_remote_copy(src, dst, send_sem, recv_sem, device_id={"sp": to},
                                         device_id_type=MESH).start()

    def drain(buf, sem):
        pltpu.make_async_copy(buf, buf, sem).wait()

    for d in order:
        to = lax.rem(me + d, n)
        push(ssend.at[:, to], srecv.at[:, me], x_send.at[0], x_recv.at[0], d, to)
        push(csend.at[:, to], crecv.at[:, me], x_send.at[1], x_recv.at[1], d, to)
    fetch(NEAR, NEAR + 1)

    for cp in halo_copies():
        cp.wait_recv()
    ins[2].wait()

    hh = hrows // chunks
    hr, hc = _iota((hrows, batch * HALO), 0), _iota((hrows, batch * HALO), 1)
    hck = (hr >= hh).astype(jnp.int32)
    ho = hr - hck * hh
    pick = (hc == (ho >> lg) * HALO + (HALO - RES) + (ho & ((1 << lg) - 1)) * chunks + hck).astype(bf16)
    live = me > 0
    halo_h = jnp.dot(pick, halo_s[...].reshape(batch * HALO, ch), preferred_element_type=f32)
    halo_k = jnp.dot(pick, halo_c[...].reshape(batch * HALO, cch), preferred_element_type=f32)
    halo_h = jnp.where(live, halo_h, 0.0)
    mix = lambda x, y: jnp.concatenate([x[:rows], y[:hh], x[rows:], y[hh:]], axis=0)
    call = mix(cnd, halo_k).astype(bf16)
    half = ch // 2

    def gate(x, k, z0):
        parts = []
        for q in range(2):
            lo, hi = q * half, (q + 1) * half
            zf = jnp.dot(x, w1[k, :, lo:hi], preferred_element_type=f32) + z0(lo, hi)
            zg = jnp.dot(x, w1[k, :, ch + lo:ch + hi], preferred_element_type=f32) + z0(ch + lo, ch + hi)
            parts.append((jnp.tanh(zf) * (0.5 * jnp.tanh(0.5 * zg) + 0.5)).astype(bf16))
        return jnp.concatenate(parts, axis=1)

    def narrow(a, w, lo, hi):
        return [jnp.dot(a, w[:, c:min(c + 256, hi)], preferred_element_type=f32) for c in range(lo, hi, 256)]

    def near_layer(k, h, cnd_rows, halo_out):
        m = h.shape[0]
        u = h.astype(bf16)
        r, c = _iota((m, m), 0), _iota((m, m), 1)
        seq, rho, step = place(r)
        if m > blk:
            src = step * RES + rho - 2 ** k
            col = row_of(seq, src & (RES - 1), src >> NEAR)
        else:
            src = step * RES + rho - 2 ** k
            col = row_of(seq, src & (RES - 1), src >> NEAR, True)
        col = jnp.where(src >= -RES, col, -1)
        p = jnp.dot((c == col).astype(bf16), u, preferred_element_type=f32).astype(bf16)
        keep = m if halo_out else rows
        zk = jnp.dot(cnd_rows[:keep], wc[k], preferred_element_type=f32) + bias[k:k + 1]
        a = gate(jnp.concatenate([u[:keep], p[:keep]], axis=1), k, lambda lo, hi: zk[:, lo:hi])
        return a, jnp.concatenate(narrow(a, w2.at[k], 0, ch), axis=1)

    ccopy(0).wait()
    for cp in wcopies(0):
        cp.wait()
    h0 = mix(h3[...], halo_h)
    a, d0 = near_layer(0, h0, call, True)
    for ck in range(chunks):
        gates[0, ck * rows:(ck + 1) * rows] = a[ck * blk:ck * blk + rows]
    edge = (_iota((blk, ch), 0) < rows) | live
    for ck in range(chunks):
        part = slice(ck * blk, (ck + 1) * blk)
        out = slice(ck * rows, (ck + 1) * rows)
        acc = d0[part]
        for k in range(1, NEAR):
            if ck == 0:
                ccopy(k).wait()
                for cp in wcopies(k):
                    cp.wait()
            a, dk = near_layer(k, jnp.where(edge, h0[part] + acc, 0.0), call[part], k < NEAR - 1)
            gates[k, out] = a[:rows]
            acc = acc[:dk.shape[0]] + dk
        dsend[ck] = acc.reshape(n, per, ch).astype(TRAVEL)
        near[out] = acc
        for d in order:
            to = lax.rem(me + d, n)
            push(dsend.at[ck, to], drecv.at[ck, me], d_send, d_recv.at[ck], d, to)
        if ck == 0:
            fetch(NEAR + 2, NEAR + 3)
    fetch(*range(NEAR + 4, layers))

    skp = jnp.dot(gates[0], w2[0, :, ch:wide], preferred_element_type=f32)
    for k in range(1, NEAR):
        skp = skp + jnp.dot(gates[k], w2[k, :, ch:wide], preferred_element_type=f32)
    s3[...] = skp
    h3[...] += near[...]
    drain(crecv, x_recv.at[1])
    cq = jnp.concatenate([crecv[ck].astype(f32).reshape(rows, cch) for ck in range(chunks)], axis=0).astype(bf16)
    for k in range(NEAR, layers):
        ccopy(k).wait()
        zc[k - NEAR] = jnp.dot(cq, wc[k], preferred_element_type=f32) + bias[k:k + 1]

    def late_skip(a, k):
        return (jnp.dot(a[:, :half], w2[k, :half, ch:wide], preferred_element_type=f32)
                + jnp.dot(a[:, half:], w2[k, half:, ch:wide], preferred_element_type=f32))

    row = _iota((rows, ch), 0)
    drain(srecv, x_recv.at[0])
    base, acc, act, skips = [None] * chunks, [None] * chunks, [None] * chunks, [[] for _ in range(chunks)]

    def begin(ck):
        drain(drecv.at[ck], d_recv.at[ck])
        base[ck] = (srecv[ck].astype(f32) + drecv[ck].astype(f32)).reshape(rows, ch)

    def first_half(ck, k):
        h = base[ck] if k == NEAR else base[ck] + acc[ck]
        sft = 2 ** (k - NEAR)
        if sft < 8:
            past = jnp.where(row >= sft, pltpu.roll(h, sft, 0), 0.0)
        else:
            past = jnp.concatenate([jnp.zeros((sft, ch), f32), h[:rows - sft]], axis=0)
        if ck == 0:
            for cp in wcopies(k):
                cp.wait()
        z_rows = slice(ck * rows, (ck + 1) * rows)
        return gate(jnp.concatenate([h.astype(bf16), past.astype(bf16)], axis=1), k,
                    lambda lo, hi: zc[k - NEAR, z_rows, lo:hi])

    def second_half(ck, k, a):
        if k > NEAR:
            skips[ck].append(late_skip(act[ck], k - 1))
        act[ck] = a
        dlt = jnp.concatenate(narrow(a, w2.at[k], 0, ch), axis=1)
        acc[ck] = dlt if k == NEAR else acc[ck] + dlt

    def send_back(ck):
        osend[ck, :, :, 0:ch] = acc[ck].reshape(n, per, ch).astype(TRAVEL)
        skips[ck].append(late_skip(act[ck], layers - 1))
        osend[ck, :, :, ch:wide] = sum(skips[ck][1:], skips[ck][0]).reshape(n, per, wide - ch).astype(TRAVEL)
        for d in order:
            to = lax.rem(me + d, n)
            push(osend.at[ck, to], recv.at[ck, me], o_send, o_recv.at[ck], d, to)

    begin(0)
    for k in range(NEAR, NEAR + LEAD):
        second_half(0, k, first_half(0, k))
    begin(1)
    for k in range(NEAR + LEAD, layers):
        a0 = first_half(0, k)
        a1 = first_half(1, k - LEAD)
        second_half(0, k, a0)
        second_half(1, k - LEAD, a1)
    send_back(0)
    for k in range(layers - LEAD, layers):
        second_half(1, k, first_half(1, k))
    send_back(1)

    for cp in halo_copies():
        cp.wait_send()
    for buf, sem in ((ssend.at[:, pl.ds(0, n - 1)], x_send.at[0]), (csend.at[:, pl.ds(0, n - 1)], x_send.at[1]), (dsend.at[:, pl.ds(0, n - 1)], d_send), (osend.at[:, pl.ds(0, n - 1)], o_send)):
        drain(buf, sem)
    for ck in range(chunks):
        drain(recv.at[ck], o_recv.at[ck])


def _finish(recv, h3, s3, hout_hbm, sout_hbm, obuf, out_sem):
    chunks, n, per, wide = recv.shape
    own, ch = h3.shape
    span = per * RES
    outs = []
    for t in range(wide // 128):
        lo = t * 128
        base, off = (h3, lo) if lo < ch else (s3, lo - ch)
        for ck in range(chunks):
            for j in range(n):
                cl = j * chunks + ck
                s, rho = cl // RES, cl % RES
                at = (ck * n + j) * per
                obuf[t, pl.ds(s * span + rho, per, RES), :] = (
                    recv[ck, j, :, lo:lo + 128].astype(f32) + base[at:at + per, off:off + 128])
        dst = hout_hbm if lo < ch else sout_hbm
        outs.append(pltpu.make_async_copy(obuf.at[t], dst.at[:, pl.ds(off, 128)], out_sem.at[t]))
        outs[-1].start()
    for cp in outs:
        cp.wait()


def solution(mesh):
    n = mesh.shape['sp']

    def local_stack(signal, cond_feats, w_now, w_past, w_cond, b_gate, w_res, w_skip):
        batch, span, ch = signal.shape
        cch = cond_feats.shape[2]
        layers = w_now.shape[0]
        sk = w_skip.shape[2]
        wide = ch + sk
        own = batch * span
        per = span // RES
        chunks = batch * RES // n
        rows = n * per
        any_spec = pl.BlockSpec(memory_space=pl.ANY)
        dma = pltpu.SemaphoreType.DMA
        sds = jax.ShapeDtypeStruct
        recv, h3, s3 = pl.pallas_call(
            functools.partial(_stack, n),
            name="stack",
            out_shape=(pltpu.VMEM((chunks, n, per, wide), TRAVEL), pltpu.VMEM((own, ch), f32), pltpu.VMEM((own, sk), f32)),
            in_specs=[any_spec] * 8,
            out_specs=(pl.BlockSpec(memory_space=pltpu.VMEM),) * 3,
            scratch_shapes=[
                pltpu.VMEM((batch, span, ch), bf16), pltpu.VMEM((batch, span, cch), bf16),
                pltpu.VMEM((batch, HALO, ch), bf16), pltpu.VMEM((batch, HALO, cch), bf16),
                pltpu.VMEM((layers, 2 * ch, 2 * ch), bf16), pltpu.VMEM((layers, cch, 2 * ch), bf16),
                pltpu.VMEM((layers, ch, wide), bf16),
                pltpu.VMEM((layers, 2 * ch), f32), pltpu.VMEM((layers - NEAR, chunks * rows, 2 * ch), f32),
                pltpu.VMEM((NEAR, own, ch), bf16),
                pltpu.VMEM((own, ch), f32),
                pltpu.VMEM((chunks, n, per, ch), bf16), pltpu.VMEM((chunks, n, per, cch), bf16),
                pltpu.VMEM((chunks, n, per, ch), TRAVEL),
                pltpu.VMEM((chunks, n, per, ch), bf16), pltpu.VMEM((chunks, n, per, cch), bf16),
                pltpu.VMEM((chunks, n, per, ch), TRAVEL),
                pltpu.VMEM((chunks, n, per, wide), TRAVEL),
                dma((layers, 5)), dma((3,)), dma((2,)), dma((2,)), dma((2,)), dma((2,)),
                dma, dma((chunks,)), dma, dma((chunks,)),
            ],
            compiler_params=pltpu.CompilerParams(collective_id=0, has_side_effects=True,
                                                 vmem_limit_bytes=56 * 1024 * 1024),
        )(signal, cond_feats, w_now, w_past, w_cond, b_gate, w_res, w_skip)
        h_out, skip_out = pl.pallas_call(
            _finish,
            name="finish",
            out_shape=(sds((own, ch), f32), sds((own, sk), f32)),
            in_specs=[pl.BlockSpec(memory_space=pltpu.VMEM)] * 3,
            out_specs=(any_spec,) * 2,
            scratch_shapes=[
                pltpu.VMEM((wide // 128, own, 128), f32), dma((wide // 128,)),
            ],
        )(*(pltpu.with_memory_space_constraint(x, pltpu.VMEM) for x in (recv, h3, s3)))
        return h_out.reshape(batch, span, ch), skip_out.reshape(batch, span, sk)

    seq_spec = P('dp', 'sp', None)
    return jax.shard_map(local_stack, mesh=mesh,
                         in_specs=(seq_spec, seq_spec, P(), P(), P(), P(), P(), P()),
                         out_specs=(seq_spec, seq_spec), check_vma=False)
```

```python
import functools

import jax
import jax.numpy as jnp
from jax import lax
from jax.experimental import pallas as pl
from jax.experimental.pallas import tpu as pltpu
from jax.sharding import PartitionSpec as P

MESH = pl.DeviceIdType.MESH
NEAR = 3
RES = 2 ** NEAR
HALO = 16
f32, bf16 = jnp.float32, jnp.bfloat16
TRAVEL = bf16


def _iota(shape, dim):
    return lax.broadcasted_iota(jnp.int32, shape, dim)


def _stack(n, sig_hbm, cond_hbm, wn_hbm, wp_hbm, wc_hbm, bg_hbm, wr_hbm, ws_hbm,
           recv, h3, s3,
           sig_v, cond_v, halo_s, halo_c, w1, w2, bias, gates,
           near, ssend, csend, dsend, srecv, crecv, drecv, far, osend,
           w_sem, in_sem, halo_send, halo_recv, x_send, x_recv, d_send, d_recv, o_send, o_recv):
    me = lax.axis_index("sp")
    batch, span, ch = sig_v.shape
    cch = cond_v.shape[2]
    layers = w1.shape[0]
    own = batch * span
    per = span // RES
    ncls = batch * RES
    chunks = ncls // n
    rows = n * per
    wide = w2.shape[2]
    hrows = batch * RES
    sh_span, sh_per = span.bit_length() - 1, per.bit_length() - 1

    barrier = pltpu.get_barrier_semaphore()
    for d in range(1, n):
        pl.semaphore_signal(barrier, inc=1, device_id={"sp": lax.rem(me + d, n)}, device_id_type=MESH)

    ins = [pltpu.make_async_copy(sig_hbm, sig_v, in_sem.at[0]),
           pltpu.make_async_copy(cond_hbm, cond_v, in_sem.at[1]),
           pltpu.make_async_copy(bg_hbm, bias, in_sem.at[2])]
    for c in ins:
        c.start()

    def wcopies(k):
        return [pltpu.make_async_copy(wn_hbm.at[k], w1.at[k, pl.ds(0, ch)], w_sem.at[k, 0]),
                pltpu.make_async_copy(wp_hbm.at[k], w1.at[k, pl.ds(ch, ch)], w_sem.at[k, 1]),
                pltpu.make_async_copy(wc_hbm.at[k], w1.at[k, pl.ds(2 * ch, cch)], w_sem.at[k, 2]),
                pltpu.make_async_copy(wr_hbm.at[k], w2.at[k, :, pl.ds(0, ch)], w_sem.at[k, 3]),
                pltpu.make_async_copy(ws_hbm.at[k], w2.at[k, :, pl.ds(ch, wide - ch)], w_sem.at[k, 4])]

    def fetch(*ks):
        for k in ks:
            for c in wcopies(k):
                c.start()

    fetch(0)

    def halo_copies():
        nxt = lax.rem(me + 1, n)
        return [pltpu.make_async_remote_copy(sig_v.at[:, pl.ds(span - HALO, HALO)], halo_s, halo_send.at[0],
                                             halo_recv.at[0], device_id={"sp": nxt}, device_id_type=MESH),
                pltpu.make_async_remote_copy(cond_v.at[:, pl.ds(span - HALO, HALO)], halo_c, halo_send.at[1],
                                             halo_recv.at[1], device_id={"sp": nxt}, device_id_type=MESH)]

    fetch(*range(1, NEAR))
    ins[0].wait()
    ins[1].wait()
    blk = rows + hrows // chunks
    lg = (RES // chunks).bit_length() - 1

    def place(r):
        ck = (r >= blk).astype(jnp.int32)
        rr = r - ck * blk
        on_own = rr < rows
        o = jnp.where(on_own, rr >> sh_per, rr - rows)
        step = jnp.where(on_own, rr & (per - 1), -1)
        return o >> lg, (o & ((1 << lg) - 1)) * chunks + ck, step

    def row_of(seq, rho, step, one_chunk=False):
        ck = 0 if one_chunk else rho & (chunks - 1)
        o = seq * (1 << lg) + (rho >> (chunks.bit_length() - 1))
        return ck * blk + jnp.where(step >= 0, o * per + step, rows + o)

    r, c = _iota((own, own), 0), _iota((own, own), 1)
    seq, rho, step = place(r + hrows // chunks * (r >= rows).astype(jnp.int32))
    perm = (c == seq * span + step * RES + rho).astype(bf16)
    cnd = jnp.dot(perm, cond_v[...].reshape(own, cch), preferred_element_type=f32)
    sig = jnp.dot(perm, sig_v[...].reshape(own, ch), preferred_element_type=f32)
    csend[...] = cnd.reshape(chunks, n, per, cch).astype(bf16)
    ssend[...] = sig.reshape(chunks, n, per, ch).astype(bf16)
    h3[...] = sig

    pl.semaphore_wait(barrier, n - 1)
    for cp in halo_copies():
        cp.start()

    order = [n // 2]
    for d in range(n // 2 - 1, 0, -1):
        order += [n - d, d]
    order += [0]

    def push(src, dst, send_sem, recv_sem, d, to):
        if d == 0:
            pltpu.make_async_copy(src, dst, recv_sem).start()
        else:
            pltpu.make_async_remote_copy(src, dst, send_sem, recv_sem, device_id={"sp": to},
                                         device_id_type=MESH).start()

    def drain(buf, sem):
        pltpu.make_async_copy(buf, buf, sem).wait()

    for d in order:
        to = lax.rem(me + d, n)
        push(csend.at[:, to], crecv.at[:, me], x_send.at[chunks], x_recv.at[chunks], d, to)
        push(ssend.at[0, to], srecv.at[0, me], x_send.at[0], x_recv.at[0], d, to)
    fetch(NEAR, NEAR + 1)

    for cp in halo_copies():
        cp.wait_recv()
    ins[2].wait()

    hh = hrows // chunks
    hr, hc = _iota((hrows, batch * HALO), 0), _iota((hrows, batch * HALO), 1)
    hck = (hr >= hh).astype(jnp.int32)
    ho = hr - hck * hh
    pick = (hc == (ho >> lg) * HALO + (HALO - RES) + (ho & ((1 << lg) - 1)) * chunks + hck).astype(bf16)
    live = me > 0
    halo_h = jnp.dot(pick, halo_s[...].reshape(batch * HALO, ch), preferred_element_type=f32)
    halo_k = jnp.dot(pick, halo_c[...].reshape(batch * HALO, cch), preferred_element_type=f32)
    halo_h = jnp.where(live, halo_h, 0.0)
    mix = lambda x, y: jnp.concatenate([x[:rows], y[:hh], x[rows:], y[hh:]], axis=0)
    call = mix(cnd, halo_k).astype(bf16)
    half = ch // 2

    def gate(x, k):
        parts = []
        for q in range(2):
            lo, hi = q * half, (q + 1) * half
            zf = jnp.dot(x, w1[k, :, lo:hi], preferred_element_type=f32) + bias[k:k + 1, lo:hi]
            zg = jnp.dot(x, w1[k, :, ch + lo:ch + hi], preferred_element_type=f32) + bias[k:k + 1, ch + lo:ch + hi]
            parts.append((jnp.tanh(zf) * (0.5 * jnp.tanh(0.5 * zg) + 0.5)).astype(bf16))
        return jnp.concatenate(parts, axis=1)

    def near_layer(k, h, cnd_rows, halo_out):
        m = h.shape[0]
        u = h.astype(bf16)
        r, c = _iota((m, m), 0), _iota((m, m), 1)
        seq, rho, step = place(r)
        if m > blk:
            src = step * RES + rho - 2 ** k
            col = row_of(seq, src & (RES - 1), src >> NEAR)
        else:
            src = step * RES + rho - 2 ** k
            col = row_of(seq, src & (RES - 1), src >> NEAR, True)
        col = jnp.where(src >= -RES, col, -1)
        p = jnp.dot((c == col).astype(bf16), u, preferred_element_type=f32).astype(bf16)
        keep = m if halo_out else rows
        a = gate(jnp.concatenate([u[:keep], p[:keep], cnd_rows[:keep]], axis=1), k)
        return a, jnp.dot(a, w2[k, :, 0:ch], preferred_element_type=f32)

    for cp in wcopies(0):
        cp.wait()
    h0 = mix(h3[...], halo_h)
    a, d0 = near_layer(0, h0, call, True)
    for ck in range(chunks):
        gates[0, ck * rows:(ck + 1) * rows] = a[ck * blk:ck * blk + rows]
    edge = (_iota((blk, ch), 0) < rows) | live
    for ck in range(chunks):
        part = slice(ck * blk, (ck + 1) * blk)
        out = slice(ck * rows, (ck + 1) * rows)
        acc = d0[part]
        for k in range(1, NEAR):
            if ck == 0:
                for cp in wcopies(k):
                    cp.wait()
            a, dk = near_layer(k, jnp.where(edge, h0[part] + acc, 0.0), call[part], k < NEAR - 1)
            gates[k, out] = a[:rows]
            acc = acc[:dk.shape[0]] + dk
        dsend[ck] = acc.reshape(n, per, ch).astype(TRAVEL)
        near[out] = acc
        for d in order:
            to = lax.rem(me + d, n)
            if ck > 0:
                push(ssend.at[ck, to], srecv.at[ck, me], x_send.at[ck], x_recv.at[ck], d, to)
            push(dsend.at[ck, to], drecv.at[ck, me], d_send, d_recv.at[ck], d, to)
        if ck == 0:
            fetch(NEAR + 2, NEAR + 3)
    fetch(*range(NEAR + 4, layers))

    skp = jnp.dot(gates[0], w2[0, :, ch:wide], preferred_element_type=f32)
    for k in range(1, NEAR):
        skp = skp + jnp.dot(gates[k], w2[k, :, ch:wide], preferred_element_type=f32)
    s3[...] = skp
    h3[...] += near[...]
    drain(crecv, x_recv.at[chunks])
    row = _iota((rows, ch), 0)
    for ck in range(chunks):
        drain(srecv.at[ck], x_recv.at[ck])
        drain(drecv.at[ck], d_recv.at[ck])
        base = (srecv[ck].astype(f32) + drecv[ck].astype(f32)).reshape(rows, ch)
        cq = crecv[ck].astype(f32).reshape(rows, cch).astype(bf16)
        h = base
        for k in range(NEAR, layers):
            sft = 2 ** (k - NEAR)
            if k > NEAR:
                h = base + far[:, 0:ch]
            if sft < 8:
                past = jnp.where(row >= sft, pltpu.roll(h, sft, 0), 0.0)
            else:
                past = jnp.concatenate([jnp.zeros((sft, ch), f32), h[:rows - sft]], axis=0)
            if ck == 0:
                for cp in wcopies(k):
                    cp.wait()
            a = gate(jnp.concatenate([h.astype(bf16), past.astype(bf16), cq], axis=1), k)
            dlt = jnp.dot(a, w2[k], preferred_element_type=f32)
            if k == NEAR:
                far[...] = dlt
            elif k < layers - 1:
                far[...] += dlt
            else:
                osend[ck] = (far[...] + dlt).reshape(n, per, wide).astype(TRAVEL)
        for d in order:
            to = lax.rem(me + d, n)
            push(osend.at[ck, to], recv.at[ck, me], o_send, o_recv.at[ck], d, to)

    for cp in halo_copies():
        cp.wait_send()
    for ck in range(chunks):
        drain(ssend.at[ck, pl.ds(0, n - 1)], x_send.at[ck])
    for buf, sem in ((csend.at[:, pl.ds(0, n - 1)], x_send.at[chunks]), (dsend.at[:, pl.ds(0, n - 1)], d_send), (osend.at[:, pl.ds(0, n - 1)], o_send)):
        drain(buf, sem)
    for ck in range(chunks):
        drain(recv.at[ck], o_recv.at[ck])


def _finish(recv, h3, s3, hout_hbm, sout_hbm, obuf, out_sem):
    chunks, n, per, wide = recv.shape
    own, ch = h3.shape
    span = per * RES
    outs = []
    for t in range(wide // 128):
        lo = t * 128
        base, off = (h3, lo) if lo < ch else (s3, lo - ch)
        for ck in range(chunks):
            for j in range(n):
                cl = j * chunks + ck
                s, rho = cl // RES, cl % RES
                at = (ck * n + j) * per
                obuf[t, pl.ds(s * span + rho, per, RES), :] = (
                    recv[ck, j, :, lo:lo + 128].astype(f32) + base[at:at + per, off:off + 128])
        dst = hout_hbm if lo < ch else sout_hbm
        outs.append(pltpu.make_async_copy(obuf.at[t], dst.at[:, pl.ds(off, 128)], out_sem.at[t]))
        outs[-1].start()
    for cp in outs:
        cp.wait()


def solution(mesh):
    n = mesh.shape['sp']

    def local_stack(signal, cond_feats, w_now, w_past, w_cond, b_gate, w_res, w_skip):
        batch, span, ch = signal.shape
        cch = cond_feats.shape[2]
        layers = w_now.shape[0]
        sk = w_skip.shape[2]
        wide = ch + sk
        own = batch * span
        per = span // RES
        chunks = batch * RES // n
        rows = n * per
        any_spec = pl.BlockSpec(memory_space=pl.ANY)
        dma = pltpu.SemaphoreType.DMA
        sds = jax.ShapeDtypeStruct
        recv, h3, s3 = pl.pallas_call(
            functools.partial(_stack, n),
            name="stack",
            out_shape=(pltpu.VMEM((chunks, n, per, wide), TRAVEL), pltpu.VMEM((own, ch), f32), pltpu.VMEM((own, sk), f32)),
            in_specs=[any_spec] * 8,
            out_specs=(pl.BlockSpec(memory_space=pltpu.VMEM),) * 3,
            scratch_shapes=[
                pltpu.VMEM((batch, span, ch), bf16), pltpu.VMEM((batch, span, cch), bf16),
                pltpu.VMEM((batch, HALO, ch), bf16), pltpu.VMEM((batch, HALO, cch), bf16),
                pltpu.VMEM((layers, 2 * ch + cch, 2 * ch), bf16), pltpu.VMEM((layers, ch, wide), bf16),
                pltpu.VMEM((layers, 2 * ch), f32),
                pltpu.VMEM((NEAR, own, ch), bf16),
                pltpu.VMEM((own, ch), f32),
                pltpu.VMEM((chunks, n, per, ch), bf16), pltpu.VMEM((chunks, n, per, cch), bf16),
                pltpu.VMEM((chunks, n, per, ch), TRAVEL),
                pltpu.VMEM((chunks, n, per, ch), bf16), pltpu.VMEM((chunks, n, per, cch), bf16),
                pltpu.VMEM((chunks, n, per, ch), TRAVEL),
                pltpu.VMEM((rows, wide), f32), pltpu.VMEM((chunks, n, per, wide), TRAVEL),
                dma((layers, 5)), dma((3,)), dma((2,)), dma((2,)), dma((chunks + 1,)), dma((chunks + 1,)),
                dma, dma((chunks,)), dma, dma((chunks,)),
            ],
            compiler_params=pltpu.CompilerParams(collective_id=0, has_side_effects=True,
                                                 vmem_limit_bytes=56 * 1024 * 1024),
        )(signal, cond_feats, w_now, w_past, w_cond, b_gate, w_res, w_skip)
        h_out, skip_out = pl.pallas_call(
            _finish,
            name="finish",
            out_shape=(sds((own, ch), f32), sds((own, sk), f32)),
            in_specs=[pl.BlockSpec(memory_space=pltpu.VMEM)] * 3,
            out_specs=(any_spec,) * 2,
            scratch_shapes=[
                pltpu.VMEM((wide // 128, own, 128), f32), dma((wide // 128,)),
            ],
        )(*(pltpu.with_memory_space_constraint(x, pltpu.VMEM) for x in (recv, h3, s3)))
        return h_out.reshape(batch, span, ch), skip_out.reshape(batch, span, sk)

    seq_spec = P('dp', 'sp', None)
    return jax.shard_map(local_stack, mesh=mesh,
                         in_specs=(seq_spec, seq_spec, P(), P(), P(), P(), P(), P()),
                         out_specs=(seq_spec, seq_spec), check_vma=False)
```

```python
import functools

import jax
import jax.numpy as jnp
from jax import lax
from jax.experimental import pallas as pl
from jax.experimental.pallas import tpu as pltpu
from jax.sharding import PartitionSpec as P

MESH = pl.DeviceIdType.MESH
NEAR = 3
RES = 2 ** NEAR
HALO = 16
f32, bf16 = jnp.float32, jnp.bfloat16
TRAVEL = bf16


def _iota(shape, dim):
    return lax.broadcasted_iota(jnp.int32, shape, dim)


def _stack(n, sig_hbm, cond_hbm, wn_hbm, wp_hbm, wc_hbm, bg_hbm, wr_hbm, ws_hbm,
           recv, h3, s3,
           sig_v, cond_v, halo_s, halo_c, w1, w2, bias, gates,
           near, ssend, csend, dsend, srecv, crecv, drecv, far, osend,
           w_sem, in_sem, halo_send, halo_recv, x_send, x_recv, d_send, d_recv, o_send, o_recv):
    me = lax.axis_index("sp")
    batch, span, ch = sig_v.shape
    cch = cond_v.shape[2]
    layers = w1.shape[0]
    own = batch * span
    per = span // RES
    ncls = batch * RES
    chunks = ncls // n
    rows = n * per
    wide = w2.shape[2]
    hrows = batch * RES
    sh_span, sh_per = span.bit_length() - 1, per.bit_length() - 1

    barrier = pltpu.get_barrier_semaphore()
    for d in range(1, n):
        pl.semaphore_signal(barrier, inc=1, device_id={"sp": lax.rem(me + d, n)}, device_id_type=MESH)

    ins = [pltpu.make_async_copy(sig_hbm, sig_v, in_sem.at[0]),
           pltpu.make_async_copy(cond_hbm, cond_v, in_sem.at[1]),
           pltpu.make_async_copy(bg_hbm, bias, in_sem.at[2])]
    for c in ins:
        c.start()

    def wcopies(k):
        return [pltpu.make_async_copy(wn_hbm.at[k], w1.at[k, pl.ds(0, ch)], w_sem.at[k, 0]),
                pltpu.make_async_copy(wp_hbm.at[k], w1.at[k, pl.ds(ch, ch)], w_sem.at[k, 1]),
                pltpu.make_async_copy(wc_hbm.at[k], w1.at[k, pl.ds(2 * ch, cch)], w_sem.at[k, 2]),
                pltpu.make_async_copy(wr_hbm.at[k], w2.at[k, :, pl.ds(0, ch)], w_sem.at[k, 3]),
                pltpu.make_async_copy(ws_hbm.at[k], w2.at[k, :, pl.ds(ch, wide - ch)], w_sem.at[k, 4])]

    def fetch(*ks):
        for k in ks:
            for c in wcopies(k):
                c.start()

    fetch(0)

    def halo_copies():
        nxt = lax.rem(me + 1, n)
        return [pltpu.make_async_remote_copy(sig_v.at[:, pl.ds(span - HALO, HALO)], halo_s, halo_send.at[0],
                                             halo_recv.at[0], device_id={"sp": nxt}, device_id_type=MESH),
                pltpu.make_async_remote_copy(cond_v.at[:, pl.ds(span - HALO, HALO)], halo_c, halo_send.at[1],
                                             halo_recv.at[1], device_id={"sp": nxt}, device_id_type=MESH)]

    ins[0].wait()
    ins[1].wait()
    blk = rows + hrows // chunks
    lg = (RES // chunks).bit_length() - 1

    def place(r):
        ck = (r >= blk).astype(jnp.int32)
        rr = r - ck * blk
        on_own = rr < rows
        o = jnp.where(on_own, rr >> sh_per, rr - rows)
        step = jnp.where(on_own, rr & (per - 1), -1)
        return o >> lg, (o & ((1 << lg) - 1)) * chunks + ck, step

    def row_of(seq, rho, step, one_chunk=False):
        ck = 0 if one_chunk else rho & (chunks - 1)
        o = seq * (1 << lg) + (rho >> (chunks.bit_length() - 1))
        return ck * blk + jnp.where(step >= 0, o * per + step, rows + o)

    r, c = _iota((own, own), 0), _iota((own, own), 1)
    seq, rho, step = place(r + hrows // chunks * (r >= rows).astype(jnp.int32))
    perm = (c == seq * span + step * RES + rho).astype(bf16)
    cnd = jnp.dot(perm, cond_v[...].reshape(own, cch), preferred_element_type=f32)
    sig = jnp.dot(perm, sig_v[...].reshape(own, ch), preferred_element_type=f32)
    csend[...] = cnd.reshape(chunks, n, per, cch).astype(bf16)
    ssend[...] = sig.reshape(chunks, n, per, ch).astype(bf16)
    h3[...] = sig

    pl.semaphore_wait(barrier, n - 1)
    for cp in halo_copies():
        cp.start()

    order = [n // 2]
    for d in range(n // 2 - 1, 0, -1):
        order += [n - d, d]
    order += [0]

    def push(src, dst, send_sem, recv_sem, d, to):
        if d == 0:
            pltpu.make_async_copy(src, dst, recv_sem).start()
        else:
            pltpu.make_async_remote_copy(src, dst, send_sem, recv_sem, device_id={"sp": to},
                                         device_id_type=MESH).start()

    def drain(buf, sem):
        pltpu.make_async_copy(buf, buf, sem).wait()

    for d in order:
        to = lax.rem(me + d, n)
        push(csend.at[:, to], crecv.at[:, me], x_send.at[chunks], x_recv.at[chunks], d, to)
        push(ssend.at[0, to], srecv.at[0, me], x_send.at[0], x_recv.at[0], d, to)
    fetch(*range(1, NEAR + 2))

    for cp in halo_copies():
        cp.wait_recv()
    ins[2].wait()

    hh = hrows // chunks
    hr, hc = _iota((hrows, batch * HALO), 0), _iota((hrows, batch * HALO), 1)
    hck = (hr >= hh).astype(jnp.int32)
    ho = hr - hck * hh
    pick = (hc == (ho >> lg) * HALO + (HALO - RES) + (ho & ((1 << lg) - 1)) * chunks + hck).astype(bf16)
    live = me > 0
    halo_h = jnp.dot(pick, halo_s[...].reshape(batch * HALO, ch), preferred_element_type=f32)
    halo_k = jnp.dot(pick, halo_c[...].reshape(batch * HALO, cch), preferred_element_type=f32)
    halo_h = jnp.where(live, halo_h, 0.0)
    mix = lambda x, y: jnp.concatenate([x[:rows], y[:hh], x[rows:], y[hh:]], axis=0)
    call = mix(cnd, halo_k).astype(bf16)
    half = ch // 2

    def gate(x, k):
        parts = []
        for q in range(2):
            lo, hi = q * half, (q + 1) * half
            zf = jnp.dot(x, w1[k, :, lo:hi], preferred_element_type=f32) + bias[k:k + 1, lo:hi]
            zg = jnp.dot(x, w1[k, :, ch + lo:ch + hi], preferred_element_type=f32) + bias[k:k + 1, ch + lo:ch + hi]
            parts.append((jnp.tanh(zf) * (0.5 * jnp.tanh(0.5 * zg) + 0.5)).astype(bf16))
        return jnp.concatenate(parts, axis=1)

    def near_layer(k, h, cnd_rows, halo_out):
        m = h.shape[0]
        u = h.astype(bf16)
        r, c = _iota((m, m), 0), _iota((m, m), 1)
        seq, rho, step = place(r)
        if m > blk:
            src = step * RES + rho - 2 ** k
            col = row_of(seq, src & (RES - 1), src >> NEAR)
        else:
            src = step * RES + rho - 2 ** k
            col = row_of(seq, src & (RES - 1), src >> NEAR, True)
        col = jnp.where(src >= -RES, col, -1)
        p = jnp.dot((c == col).astype(bf16), u, preferred_element_type=f32).astype(bf16)
        keep = m if halo_out else rows
        a = gate(jnp.concatenate([u[:keep], p[:keep], cnd_rows[:keep]], axis=1), k)
        return a, jnp.dot(a, w2[k, :, 0:ch], preferred_element_type=f32)

    for cp in wcopies(0):
        cp.wait()
    h0 = mix(h3[...], halo_h)
    a, d0 = near_layer(0, h0, call, True)
    for ck in range(chunks):
        gates[0, ck * rows:(ck + 1) * rows] = a[ck * blk:ck * blk + rows]
    edge = (_iota((blk, ch), 0) < rows) | live
    for ck in range(chunks):
        part = slice(ck * blk, (ck + 1) * blk)
        out = slice(ck * rows, (ck + 1) * rows)
        acc = d0[part]
        for k in range(1, NEAR):
            if ck == 0:
                for cp in wcopies(k):
                    cp.wait()
            a, dk = near_layer(k, jnp.where(edge, h0[part] + acc, 0.0), call[part], k < NEAR - 1)
            gates[k, out] = a[:rows]
            acc = acc[:dk.shape[0]] + dk
        dsend[ck] = acc.reshape(n, per, ch).astype(TRAVEL)
        near[out] = acc
        for d in order:
            to = lax.rem(me + d, n)
            if ck > 0:
                push(ssend.at[ck, to], srecv.at[ck, me], x_send.at[ck], x_recv.at[ck], d, to)
            push(dsend.at[ck, to], drecv.at[ck, me], d_send, d_recv.at[ck], d, to)
        if ck == 0:
            fetch(NEAR + 2, NEAR + 3)
    fetch(*range(NEAR + 4, layers))

    skp = jnp.dot(gates[0], w2[0, :, ch:wide], preferred_element_type=f32)
    for k in range(1, NEAR):
        skp = skp + jnp.dot(gates[k], w2[k, :, ch:wide], preferred_element_type=f32)
    s3[...] = skp
    h3[...] += near[...]
    drain(crecv, x_recv.at[chunks])
    row = _iota((rows, ch), 0)
    for ck in range(chunks):
        drain(srecv.at[ck], x_recv.at[ck])
        drain(drecv.at[ck], d_recv.at[ck])
        base = (srecv[ck].astype(f32) + drecv[ck].astype(f32)).reshape(rows, ch)
        cq = crecv[ck].astype(f32).reshape(rows, cch).astype(bf16)
        h = base
        for k in range(NEAR, layers):
            sft = 2 ** (k - NEAR)
            if k > NEAR:
                h = base + far[:, 0:ch]
            if sft < 8:
                past = jnp.where(row >= sft, pltpu.roll(h, sft, 0), 0.0)
            else:
                past = jnp.concatenate([jnp.zeros((sft, ch), f32), h[:rows - sft]], axis=0)
            if ck == 0:
                for cp in wcopies(k):
                    cp.wait()
            a = gate(jnp.concatenate([h.astype(bf16), past.astype(bf16), cq], axis=1), k)
            dlt = jnp.dot(a, w2[k], preferred_element_type=f32)
            if k == NEAR:
                far[...] = dlt
            elif k < layers - 1:
                far[...] += dlt
            else:
                osend[ck] = (far[...] + dlt).reshape(n, per, wide).astype(TRAVEL)
        for d in order:
            to = lax.rem(me + d, n)
            push(osend.at[ck, to], recv.at[ck, me], o_send, o_recv.at[ck], d, to)

    for cp in halo_copies():
        cp.wait_send()
    for ck in range(chunks):
        drain(ssend.at[ck, pl.ds(0, n - 1)], x_send.at[ck])
    for buf, sem in ((csend.at[:, pl.ds(0, n - 1)], x_send.at[chunks]), (dsend.at[:, pl.ds(0, n - 1)], d_send), (osend.at[:, pl.ds(0, n - 1)], o_send)):
        drain(buf, sem)
    for ck in range(chunks):
        drain(recv.at[ck], o_recv.at[ck])


def _finish(recv, h3, s3, hout_hbm, sout_hbm, obuf, out_sem):
    chunks, n, per, wide = recv.shape
    own, ch = h3.shape
    span = per * RES
    outs = []
    for t in range(wide // 128):
        lo = t * 128
        base, off = (h3, lo) if lo < ch else (s3, lo - ch)
        for ck in range(chunks):
            for j in range(n):
                cl = j * chunks + ck
                s, rho = cl // RES, cl % RES
                at = (ck * n + j) * per
                obuf[t, pl.ds(s * span + rho, per, RES), :] = (
                    recv[ck, j, :, lo:lo + 128].astype(f32) + base[at:at + per, off:off + 128])
        dst = hout_hbm if lo < ch else sout_hbm
        outs.append(pltpu.make_async_copy(obuf.at[t], dst.at[:, pl.ds(off, 128)], out_sem.at[t]))
        outs[-1].start()
    for cp in outs:
        cp.wait()


def solution(mesh):
    n = mesh.shape['sp']

    def local_stack(signal, cond_feats, w_now, w_past, w_cond, b_gate, w_res, w_skip):
        batch, span, ch = signal.shape
        cch = cond_feats.shape[2]
        layers = w_now.shape[0]
        sk = w_skip.shape[2]
        wide = ch + sk
        own = batch * span
        per = span // RES
        chunks = batch * RES // n
        rows = n * per
        any_spec = pl.BlockSpec(memory_space=pl.ANY)
        dma = pltpu.SemaphoreType.DMA
        sds = jax.ShapeDtypeStruct
        recv, h3, s3 = pl.pallas_call(
            functools.partial(_stack, n),
            name="stack",
            out_shape=(pltpu.VMEM((chunks, n, per, wide), TRAVEL), pltpu.VMEM((own, ch), f32), pltpu.VMEM((own, sk), f32)),
            in_specs=[any_spec] * 8,
            out_specs=(pl.BlockSpec(memory_space=pltpu.VMEM),) * 3,
            scratch_shapes=[
                pltpu.VMEM((batch, span, ch), bf16), pltpu.VMEM((batch, span, cch), bf16),
                pltpu.VMEM((batch, HALO, ch), bf16), pltpu.VMEM((batch, HALO, cch), bf16),
                pltpu.VMEM((layers, 2 * ch + cch, 2 * ch), bf16), pltpu.VMEM((layers, ch, wide), bf16),
                pltpu.VMEM((layers, 2 * ch), f32),
                pltpu.VMEM((NEAR, own, ch), bf16),
                pltpu.VMEM((own, ch), f32),
                pltpu.VMEM((chunks, n, per, ch), bf16), pltpu.VMEM((chunks, n, per, cch), bf16),
                pltpu.VMEM((chunks, n, per, ch), TRAVEL),
                pltpu.VMEM((chunks, n, per, ch), bf16), pltpu.VMEM((chunks, n, per, cch), bf16),
                pltpu.VMEM((chunks, n, per, ch), TRAVEL),
                pltpu.VMEM((rows, wide), f32), pltpu.VMEM((chunks, n, per, wide), TRAVEL),
                dma((layers, 5)), dma((3,)), dma((2,)), dma((2,)), dma((chunks + 1,)), dma((chunks + 1,)),
                dma, dma((chunks,)), dma, dma((chunks,)),
            ],
            compiler_params=pltpu.CompilerParams(collective_id=0, has_side_effects=True,
                                                 vmem_limit_bytes=56 * 1024 * 1024),
        )(signal, cond_feats, w_now, w_past, w_cond, b_gate, w_res, w_skip)
        h_out, skip_out = pl.pallas_call(
            _finish,
            name="finish",
            out_shape=(sds((own, ch), f32), sds((own, sk), f32)),
            in_specs=[pl.BlockSpec(memory_space=pltpu.VMEM)] * 3,
            out_specs=(any_spec,) * 2,
            scratch_shapes=[
                pltpu.VMEM((wide // 128, own, 128), f32), dma((wide // 128,)),
            ],
        )(*(pltpu.with_memory_space_constraint(x, pltpu.VMEM) for x in (recv, h3, s3)))
        return h_out.reshape(batch, span, ch), skip_out.reshape(batch, span, sk)

    seq_spec = P('dp', 'sp', None)
    return jax.shard_map(local_stack, mesh=mesh,
                         in_specs=(seq_spec, seq_spec, P(), P(), P(), P(), P(), P()),
                         out_specs=(seq_spec, seq_spec), check_vma=False)
```

```python
import functools

import jax
import jax.numpy as jnp
from jax import lax
from jax.experimental import pallas as pl
from jax.experimental.pallas import tpu as pltpu
from jax.sharding import PartitionSpec as P

MESH = pl.DeviceIdType.MESH
NEAR = 3
RES = 2 ** NEAR
HALO = 16
f32, bf16 = jnp.float32, jnp.bfloat16
TRAVEL = bf16


def _iota(shape, dim):
    return lax.broadcasted_iota(jnp.int32, shape, dim)


def _stack(n, sig_hbm, cond_hbm, wn_hbm, wp_hbm, wc_hbm, bg_hbm, wr_hbm, ws_hbm,
           recv, h3, s3,
           sig_v, cond_v, halo_s, halo_c, w1, w2, bias, gates,
           near, xsend, dsend, bsend, xrecv, drecv, brecv, far, osend,
           w_sem, in_sem, halo_send, halo_recv, x_send, x_recv, d_send, d_recv, o_send, o_recv):
    me = lax.axis_index("sp")
    batch, span, ch = sig_v.shape
    cch = cond_v.shape[2]
    layers = w1.shape[0]
    own = batch * span
    per = span // RES
    ncls = batch * RES
    chunks = ncls // n
    rows = n * per
    wide = w2.shape[2]
    hrows = batch * RES
    sh_span, sh_per = span.bit_length() - 1, per.bit_length() - 1

    barrier = pltpu.get_barrier_semaphore()
    for d in range(1, n):
        pl.semaphore_signal(barrier, inc=1, device_id={"sp": lax.rem(me + d, n)}, device_id_type=MESH)

    ins = [pltpu.make_async_copy(sig_hbm, sig_v, in_sem.at[0]),
           pltpu.make_async_copy(cond_hbm, cond_v, in_sem.at[1]),
           pltpu.make_async_copy(bg_hbm, bias, in_sem.at[2])]
    for c in ins:
        c.start()

    def wcopies(k):
        return [pltpu.make_async_copy(wn_hbm.at[k], w1.at[k, pl.ds(0, ch)], w_sem.at[k, 0]),
                pltpu.make_async_copy(wp_hbm.at[k], w1.at[k, pl.ds(ch, ch)], w_sem.at[k, 1]),
                pltpu.make_async_copy(wc_hbm.at[k], w1.at[k, pl.ds(2 * ch, cch)], w_sem.at[k, 2]),
                pltpu.make_async_copy(wr_hbm.at[k], w2.at[k, :, pl.ds(0, ch)], w_sem.at[k, 3]),
                pltpu.make_async_copy(ws_hbm.at[k], w2.at[k, :, pl.ds(ch, wide - ch)], w_sem.at[k, 4])]

    def fetch(*ks):
        for k in ks:
            for c in wcopies(k):
                c.start()

    fetch(0)

    def halo_copies():
        nxt = lax.rem(me + 1, n)
        return [pltpu.make_async_remote_copy(sig_v.at[:, pl.ds(span - HALO, HALO)], halo_s, halo_send.at[0],
                                             halo_recv.at[0], device_id={"sp": nxt}, device_id_type=MESH),
                pltpu.make_async_remote_copy(cond_v.at[:, pl.ds(span - HALO, HALO)], halo_c, halo_send.at[1],
                                             halo_recv.at[1], device_id={"sp": nxt}, device_id_type=MESH)]

    ins[0].wait()
    ins[1].wait()
    blk = rows + hrows // chunks
    lg = (RES // chunks).bit_length() - 1

    def place(r):
        ck = (r >= blk).astype(jnp.int32)
        rr = r - ck * blk
        on_own = rr < rows
        o = jnp.where(on_own, rr >> sh_per, rr - rows)
        step = jnp.where(on_own, rr & (per - 1), -1)
        return o >> lg, (o & ((1 << lg) - 1)) * chunks + ck, step

    def row_of(seq, rho, step, one_chunk=False):
        ck = 0 if one_chunk else rho & (chunks - 1)
        o = seq * (1 << lg) + (rho >> (chunks.bit_length() - 1))
        return ck * blk + jnp.where(step >= 0, o * per + step, rows + o)

    r, c = _iota((own, own), 0), _iota((own, own), 1)
    seq, rho, step = place(r + hrows // chunks * (r >= rows).astype(jnp.int32))
    perm = (c == seq * span + step * RES + rho).astype(bf16)
    cnd = jnp.dot(perm, cond_v[...].reshape(own, cch), preferred_element_type=f32)
    sig = jnp.dot(perm, sig_v[...].reshape(own, ch), preferred_element_type=f32)
    cnd_b = cnd.reshape(chunks, n, per, cch).astype(bf16)
    sig_b = sig.reshape(chunks, n, per, ch).astype(bf16)
    xsend[:, :, 0:ch] = sig_b[0]
    for ck in range(chunks):
        xsend[:, :, ch + ck * cch:ch + (ck + 1) * cch] = cnd_b[ck]
        if ck > 0:
            bsend[ck - 1, :, :, 0:ch] = sig_b[ck]
    h3[...] = sig

    pl.semaphore_wait(barrier, n - 1)
    for cp in halo_copies():
        cp.start()

    order = [n // 2]
    for d in range(n // 2 - 1, 0, -1):
        order += [n - d, d]
    order += [0]

    def push(src, dst, send_sem, recv_sem, d, to):
        if d == 0:
            pltpu.make_async_copy(src, dst, recv_sem).start()
        else:
            pltpu.make_async_remote_copy(src, dst, send_sem, recv_sem, device_id={"sp": to},
                                         device_id_type=MESH).start()

    def drain(buf, sem):
        pltpu.make_async_copy(buf, buf, sem).wait()

    for d in order:
        to = lax.rem(me + d, n)
        push(xsend.at[to], xrecv.at[me], x_send, x_recv, d, to)
    fetch(*range(1, NEAR + 2))

    for cp in halo_copies():
        cp.wait_recv()
    ins[2].wait()

    hh = hrows // chunks
    hr, hc = _iota((hrows, batch * HALO), 0), _iota((hrows, batch * HALO), 1)
    hck = (hr >= hh).astype(jnp.int32)
    ho = hr - hck * hh
    pick = (hc == (ho >> lg) * HALO + (HALO - RES) + (ho & ((1 << lg) - 1)) * chunks + hck).astype(bf16)
    live = me > 0
    halo_h = jnp.dot(pick, halo_s[...].reshape(batch * HALO, ch), preferred_element_type=f32)
    halo_k = jnp.dot(pick, halo_c[...].reshape(batch * HALO, cch), preferred_element_type=f32)
    halo_h = jnp.where(live, halo_h, 0.0)
    mix = lambda x, y: jnp.concatenate([x[:rows], y[:hh], x[rows:], y[hh:]], axis=0)
    call = mix(cnd, halo_k).astype(bf16)
    half = ch // 2

    def gate(x, k):
        parts = []
        for q in range(2):
            lo, hi = q * half, (q + 1) * half
            zf = jnp.dot(x, w1[k, :, lo:hi], preferred_element_type=f32) + bias[k:k + 1, lo:hi]
            zg = jnp.dot(x, w1[k, :, ch + lo:ch + hi], preferred_element_type=f32) + bias[k:k + 1, ch + lo:ch + hi]
            parts.append((jnp.tanh(zf) * (0.5 * jnp.tanh(0.5 * zg) + 0.5)).astype(bf16))
        return jnp.concatenate(parts, axis=1)

    def near_layer(k, h, cnd_rows, halo_out):
        m = h.shape[0]
        u = h.astype(bf16)
        r, c = _iota((m, m), 0), _iota((m, m), 1)
        seq, rho, step = place(r)
        if m > blk:
            src = step * RES + rho - 2 ** k
            col = row_of(seq, src & (RES - 1), src >> NEAR)
        else:
            src = step * RES + rho - 2 ** k
            col = row_of(seq, src & (RES - 1), src >> NEAR, True)
        col = jnp.where(src >= -RES, col, -1)
        p = jnp.dot((c == col).astype(bf16), u, preferred_element_type=f32).astype(bf16)
        keep = m if halo_out else rows
        a = gate(jnp.concatenate([u[:keep], p[:keep], cnd_rows[:keep]], axis=1), k)
        return a, jnp.dot(a, w2[k, :, 0:ch], preferred_element_type=f32)

    for cp in wcopies(0):
        cp.wait()
    h0 = mix(h3[...], halo_h)
    a, d0 = near_layer(0, h0, call, True)
    for ck in range(chunks):
        gates[0, ck * rows:(ck + 1) * rows] = a[ck * blk:ck * blk + rows]
    edge = (_iota((blk, ch), 0) < rows) | live
    for ck in range(chunks):
        part = slice(ck * blk, (ck + 1) * blk)
        out = slice(ck * rows, (ck + 1) * rows)
        acc = d0[part]
        for k in range(1, NEAR):
            if ck == 0:
                for cp in wcopies(k):
                    cp.wait()
            a, dk = near_layer(k, jnp.where(edge, h0[part] + acc, 0.0), call[part], k < NEAR - 1)
            gates[k, out] = a[:rows]
            acc = acc[:dk.shape[0]] + dk
        if ck == 0:
            dsend[...] = acc.reshape(n, per, ch).astype(TRAVEL)
        else:
            bsend[ck - 1, :, :, ch:2 * ch] = acc.reshape(n, per, ch).astype(TRAVEL)
        near[out] = acc
        for d in order:
            to = lax.rem(me + d, n)
            if ck == 0:
                push(dsend.at[to], drecv.at[me], d_send.at[0], d_recv.at[0], d, to)
            else:
                push(bsend.at[ck - 1, to], brecv.at[ck - 1, me], d_send.at[ck], d_recv.at[ck], d, to)
        if ck == 0:
            fetch(NEAR + 2, NEAR + 3)
    fetch(*range(NEAR + 4, layers))

    skp = jnp.dot(gates[0], w2[0, :, ch:wide], preferred_element_type=f32)
    for k in range(1, NEAR):
        skp = skp + jnp.dot(gates[k], w2[k, :, ch:wide], preferred_element_type=f32)
    s3[...] = skp
    h3[...] += near[...]
    row = _iota((rows, ch), 0)
    for ck in range(chunks):
        if ck == 0:
            drain(xrecv, x_recv)
            drain(drecv, d_recv.at[0])
            base = xrecv[:, :, 0:ch].astype(f32) + drecv[...].astype(f32)
        else:
            drain(brecv.at[ck - 1], d_recv.at[ck])
            base = brecv[ck - 1, :, :, 0:ch].astype(f32) + brecv[ck - 1, :, :, ch:2 * ch].astype(f32)
        base = base.reshape(rows, ch)
        cq = xrecv[:, :, ch + ck * cch:ch + (ck + 1) * cch].astype(f32).reshape(rows, cch).astype(bf16)
        h = base
        for k in range(NEAR, layers):
            sft = 2 ** (k - NEAR)
            if k > NEAR:
                h = base + far[:, 0:ch]
            if sft < 8:
                past = jnp.where(row >= sft, pltpu.roll(h, sft, 0), 0.0)
            else:
                past = jnp.concatenate([jnp.zeros((sft, ch), f32), h[:rows - sft]], axis=0)
            if ck == 0:
                for cp in wcopies(k):
                    cp.wait()
            a = gate(jnp.concatenate([h.astype(bf16), past.astype(bf16), cq], axis=1), k)
            dlt = jnp.dot(a, w2[k], preferred_element_type=f32)
            if k == NEAR:
                far[...] = dlt
            elif k < layers - 1:
                far[...] += dlt
            else:
                osend[ck] = (far[...] + dlt).reshape(n, per, wide).astype(TRAVEL)
        for d in order:
            to = lax.rem(me + d, n)
            push(osend.at[ck, to], recv.at[ck, me], o_send, o_recv.at[ck], d, to)

    for cp in halo_copies():
        cp.wait_send()
    for buf, sem in ((xsend.at[pl.ds(0, n - 1)], x_send), (dsend.at[pl.ds(0, n - 1)], d_send.at[0]),
                     (osend.at[:, pl.ds(0, n - 1)], o_send)):
        drain(buf, sem)
    for ck in range(1, chunks):
        drain(bsend.at[ck - 1, pl.ds(0, n - 1)], d_send.at[ck])
    for ck in range(chunks):
        drain(recv.at[ck], o_recv.at[ck])


def _finish(recv, h3, s3, hout_hbm, sout_hbm, obuf, out_sem):
    chunks, n, per, wide = recv.shape
    own, ch = h3.shape
    span = per * RES
    outs = []
    for t in range(wide // 128):
        lo = t * 128
        base, off = (h3, lo) if lo < ch else (s3, lo - ch)
        for ck in range(chunks):
            for j in range(n):
                cl = j * chunks + ck
                s, rho = cl // RES, cl % RES
                at = (ck * n + j) * per
                obuf[t, pl.ds(s * span + rho, per, RES), :] = (
                    recv[ck, j, :, lo:lo + 128].astype(f32) + base[at:at + per, off:off + 128])
        dst = hout_hbm if lo < ch else sout_hbm
        outs.append(pltpu.make_async_copy(obuf.at[t], dst.at[:, pl.ds(off, 128)], out_sem.at[t]))
        outs[-1].start()
    for cp in outs:
        cp.wait()


def solution(mesh):
    n = mesh.shape['sp']

    def local_stack(signal, cond_feats, w_now, w_past, w_cond, b_gate, w_res, w_skip):
        batch, span, ch = signal.shape
        cch = cond_feats.shape[2]
        layers = w_now.shape[0]
        sk = w_skip.shape[2]
        wide = ch + sk
        own = batch * span
        per = span // RES
        chunks = batch * RES // n
        rows = n * per
        any_spec = pl.BlockSpec(memory_space=pl.ANY)
        dma = pltpu.SemaphoreType.DMA
        sds = jax.ShapeDtypeStruct
        recv, h3, s3 = pl.pallas_call(
            functools.partial(_stack, n),
            name="stack",
            out_shape=(pltpu.VMEM((chunks, n, per, wide), TRAVEL), pltpu.VMEM((own, ch), f32), pltpu.VMEM((own, sk), f32)),
            in_specs=[any_spec] * 8,
            out_specs=(pl.BlockSpec(memory_space=pltpu.VMEM),) * 3,
            scratch_shapes=[
                pltpu.VMEM((batch, span, ch), bf16), pltpu.VMEM((batch, span, cch), bf16),
                pltpu.VMEM((batch, HALO, ch), bf16), pltpu.VMEM((batch, HALO, cch), bf16),
                pltpu.VMEM((layers, 2 * ch + cch, 2 * ch), bf16), pltpu.VMEM((layers, ch, wide), bf16),
                pltpu.VMEM((layers, 2 * ch), f32),
                pltpu.VMEM((NEAR, own, ch), bf16),
                pltpu.VMEM((own, ch), f32),
                pltpu.VMEM((n, per, ch + chunks * cch), bf16), pltpu.VMEM((n, per, ch), TRAVEL),
                pltpu.VMEM((chunks - 1, n, per, 2 * ch), bf16),
                pltpu.VMEM((n, per, ch + chunks * cch), bf16), pltpu.VMEM((n, per, ch), TRAVEL),
                pltpu.VMEM((chunks - 1, n, per, 2 * ch), bf16),
                pltpu.VMEM((rows, wide), f32), pltpu.VMEM((chunks, n, per, wide), TRAVEL),
                dma((layers, 5)), dma((3,)), dma((2,)), dma((2,)), dma, dma,
                dma((chunks,)), dma((chunks,)), dma, dma((chunks,)),
            ],
            compiler_params=pltpu.CompilerParams(collective_id=0, has_side_effects=True,
                                                 vmem_limit_bytes=56 * 1024 * 1024),
        )(signal, cond_feats, w_now, w_past, w_cond, b_gate, w_res, w_skip)
        h_out, skip_out = pl.pallas_call(
            _finish,
            name="finish",
            out_shape=(sds((own, ch), f32), sds((own, sk), f32)),
            in_specs=[pl.BlockSpec(memory_space=pltpu.VMEM)] * 3,
            out_specs=(any_spec,) * 2,
            scratch_shapes=[
                pltpu.VMEM((wide // 128, own, 128), f32), dma((wide // 128,)),
            ],
        )(*(pltpu.with_memory_space_constraint(x, pltpu.VMEM) for x in (recv, h3, s3)))
        return h_out.reshape(batch, span, ch), skip_out.reshape(batch, span, sk)

    seq_spec = P('dp', 'sp', None)
    return jax.shard_map(local_stack, mesh=mesh,
                         in_specs=(seq_spec, seq_spec, P(), P(), P(), P(), P(), P()),
                         out_specs=(seq_spec, seq_spec), check_vma=False)
```

```python
import functools

import jax
import jax.numpy as jnp
from jax import lax
from jax.experimental import pallas as pl
from jax.experimental.pallas import tpu as pltpu
from jax.sharding import PartitionSpec as P

MESH = pl.DeviceIdType.MESH
NEAR = 3
RES = 2 ** NEAR
HALO = 16
f32, bf16 = jnp.float32, jnp.bfloat16
TRAVEL = bf16


def _iota(shape, dim):
    return lax.broadcasted_iota(jnp.int32, shape, dim)


def _stack(n, sig_hbm, cond_hbm, wn_hbm, wp_hbm, wc_hbm, bg_hbm, wr_hbm, ws_hbm,
           recv, h3, s3,
           sig_v, cond_v, halo_s, halo_c, w1, w2, bias, gates,
           near, xsend, dsend, bsend, xrecv, drecv, brecv, far, osend,
           w_sem, in_sem, halo_send, halo_recv, x_send, x_recv, d_send, d_recv, o_send, o_recv):
    me = lax.axis_index("sp")
    batch, span, ch = sig_v.shape
    cch = cond_v.shape[2]
    layers = w1.shape[0]
    own = batch * span
    per = span // RES
    ncls = batch * RES
    chunks = ncls // n
    rows = n * per
    wide = w2.shape[2]
    hrows = batch * RES
    sh_span, sh_per = span.bit_length() - 1, per.bit_length() - 1

    barrier = pltpu.get_barrier_semaphore()
    for d in range(1, n):
        pl.semaphore_signal(barrier, inc=1, device_id={"sp": lax.rem(me + d, n)}, device_id_type=MESH)

    ins = [pltpu.make_async_copy(sig_hbm, sig_v, in_sem.at[0]),
           pltpu.make_async_copy(cond_hbm, cond_v, in_sem.at[1]),
           pltpu.make_async_copy(bg_hbm, bias, in_sem.at[2])]
    for c in ins:
        c.start()

    def wcopies(k):
        return [pltpu.make_async_copy(wn_hbm.at[k], w1.at[k, pl.ds(0, ch)], w_sem.at[k, 0]),
                pltpu.make_async_copy(wp_hbm.at[k], w1.at[k, pl.ds(ch, ch)], w_sem.at[k, 1]),
                pltpu.make_async_copy(wc_hbm.at[k], w1.at[k, pl.ds(2 * ch, cch)], w_sem.at[k, 2]),
                pltpu.make_async_copy(wr_hbm.at[k], w2.at[k, :, pl.ds(0, ch)], w_sem.at[k, 3]),
                pltpu.make_async_copy(ws_hbm.at[k], w2.at[k, :, pl.ds(ch, wide - ch)], w_sem.at[k, 4])]

    def fetch(*ks):
        for k in ks:
            for c in wcopies(k):
                c.start()

    fetch(0)

    def halo_copies():
        nxt = lax.rem(me + 1, n)
        return [pltpu.make_async_remote_copy(sig_v.at[:, pl.ds(span - HALO, HALO)], halo_s, halo_send.at[0],
                                             halo_recv.at[0], device_id={"sp": nxt}, device_id_type=MESH),
                pltpu.make_async_remote_copy(cond_v.at[:, pl.ds(span - HALO, HALO)], halo_c, halo_send.at[1],
                                             halo_recv.at[1], device_id={"sp": nxt}, device_id_type=MESH)]

    ins[0].wait()
    ins[1].wait()
    blk = rows + hrows // chunks
    lg = (RES // chunks).bit_length() - 1

    def place(r):
        ck = (r >= blk).astype(jnp.int32)
        rr = r - ck * blk
        on_own = rr < rows
        o = jnp.where(on_own, rr >> sh_per, rr - rows)
        step = jnp.where(on_own, rr & (per - 1), -1)
        return o >> lg, (o & ((1 << lg) - 1)) * chunks + ck, step

    def row_of(seq, rho, step, one_chunk=False):
        ck = 0 if one_chunk else rho & (chunks - 1)
        o = seq * (1 << lg) + (rho >> (chunks.bit_length() - 1))
        return ck * blk + jnp.where(step >= 0, o * per + step, rows + o)

    r, c = _iota((own, own), 0), _iota((own, own), 1)
    seq, rho, step = place(r + hrows // chunks * (r >= rows).astype(jnp.int32))
    perm = (c == seq * span + step * RES + rho).astype(bf16)
    cnd = jnp.dot(perm, cond_v[...].reshape(own, cch), preferred_element_type=f32)
    sig = jnp.dot(perm, sig_v[...].reshape(own, ch), preferred_element_type=f32)
    cnd_b = cnd.reshape(chunks, n, per, cch).astype(bf16)
    sig_b = sig.reshape(chunks, n, per, ch).astype(bf16)
    xsend[:, :, 0:ch] = sig_b[0]
    for ck in range(chunks):
        xsend[:, :, ch + ck * cch:ch + (ck + 1) * cch] = cnd_b[ck]
        if ck > 0:
            bsend[ck - 1, :, :, 0:ch] = sig_b[ck]
    h3[...] = sig

    pl.semaphore_wait(barrier, n - 1)
    for cp in halo_copies():
        cp.start()

    order = [n // 2]
    for d in range(n // 2 - 1, 0, -1):
        order += [n - d, d]
    order += [0]

    def push(src, dst, send_sem, recv_sem, d, to):
        if d == 0:
            pltpu.make_async_copy(src, dst, recv_sem).start()
        else:
            pltpu.make_async_remote_copy(src, dst, send_sem, recv_sem, device_id={"sp": to},
                                         device_id_type=MESH).start()

    def drain(buf, sem):
        pltpu.make_async_copy(buf, buf, sem).wait()

    for d in order:
        to = lax.rem(me + d, n)
        push(xsend.at[to], xrecv.at[me], x_send, x_recv, d, to)
    fetch(*range(1, NEAR + 2))

    for cp in halo_copies():
        cp.wait_recv()
    ins[2].wait()

    hh = hrows // chunks
    hr, hc = _iota((hrows, batch * HALO), 0), _iota((hrows, batch * HALO), 1)
    hck = (hr >= hh).astype(jnp.int32)
    ho = hr - hck * hh
    pick = (hc == (ho >> lg) * HALO + (HALO - RES) + (ho & ((1 << lg) - 1)) * chunks + hck).astype(bf16)
    live = me > 0
    halo_h = jnp.dot(pick, halo_s[...].reshape(batch * HALO, ch), preferred_element_type=f32)
    halo_k = jnp.dot(pick, halo_c[...].reshape(batch * HALO, cch), preferred_element_type=f32)
    halo_h = jnp.where(live, halo_h, 0.0)
    mix = lambda x, y: jnp.concatenate([x[:rows], y[:hh], x[rows:], y[hh:]], axis=0)
    call = mix(cnd, halo_k).astype(bf16)
    half = ch // 2

    def gate(x, k):
        parts = []
        for q in range(2):
            lo, hi = q * half, (q + 1) * half
            zf = jnp.dot(x, w1[k, :, lo:hi], preferred_element_type=f32) + bias[k:k + 1, lo:hi]
            zg = jnp.dot(x, w1[k, :, ch + lo:ch + hi], preferred_element_type=f32) + bias[k:k + 1, ch + lo:ch + hi]
            parts.append((jnp.tanh(zf) * (0.5 * jnp.tanh(0.5 * zg) + 0.5)).astype(bf16))
        return jnp.concatenate(parts, axis=1)

    def near_layer(k, h, cnd_rows, halo_out):
        m = h.shape[0]
        u = h.astype(bf16)
        r, c = _iota((m, m), 0), _iota((m, m), 1)
        seq, rho, step = place(r)
        if m > blk:
            src = step * RES + rho - 2 ** k
            col = row_of(seq, src & (RES - 1), src >> NEAR)
        else:
            src = step * RES + rho - 2 ** k
            col = row_of(seq, src & (RES - 1), src >> NEAR, True)
        col = jnp.where(src >= -RES, col, -1)
        p = jnp.dot((c == col).astype(bf16), u, preferred_element_type=f32).astype(bf16)
        keep = m if halo_out else rows
        a = gate(jnp.concatenate([u[:keep], p[:keep], cnd_rows[:keep]], axis=1), k)
        return a, jnp.dot(a, w2[k, :, 0:ch], preferred_element_type=f32)

    for cp in wcopies(0):
        cp.wait()
    h0 = mix(h3[...], halo_h)
    a, d0 = near_layer(0, h0, call, True)
    for ck in range(chunks):
        gates[0, ck * rows:(ck + 1) * rows] = a[ck * blk:ck * blk + rows]
    edge = (_iota((blk, ch), 0) < rows) | live
    for ck in range(chunks):
        part = slice(ck * blk, (ck + 1) * blk)
        out = slice(ck * rows, (ck + 1) * rows)
        acc = d0[part]
        for k in range(1, NEAR):
            if ck == 0:
                for cp in wcopies(k):
                    cp.wait()
            a, dk = near_layer(k, jnp.where(edge, h0[part] + acc, 0.0), call[part], k < NEAR - 1)
            gates[k, out] = a[:rows]
            acc = acc[:dk.shape[0]] + dk
        if ck == 0:
            dsend[...] = acc.reshape(n, per, ch).astype(TRAVEL)
        else:
            bsend[ck - 1, :, :, ch:2 * ch] = acc.reshape(n, per, ch).astype(TRAVEL)
        near[out] = acc
        for d in order:
            to = lax.rem(me + d, n)
            if ck == 0:
                push(dsend.at[to], drecv.at[me], d_send.at[0], d_recv.at[0], d, to)
            else:
                push(bsend.at[ck - 1, to], brecv.at[ck - 1, me], d_send.at[ck], d_recv.at[ck], d, to)
    fetch(*range(NEAR + 2, layers))

    skp = jnp.dot(gates[0], w2[0, :, ch:wide], preferred_element_type=f32)
    for k in range(1, NEAR):
        skp = skp + jnp.dot(gates[k], w2[k, :, ch:wide], preferred_element_type=f32)
    s3[...] = skp
    h3[...] += near[...]
    row = _iota((rows, ch), 0)
    for ck in range(chunks):
        if ck == 0:
            drain(xrecv, x_recv)
            drain(drecv, d_recv.at[0])
            base = xrecv[:, :, 0:ch].astype(f32) + drecv[...].astype(f32)
        else:
            drain(brecv.at[ck - 1], d_recv.at[ck])
            base = brecv[ck - 1, :, :, 0:ch].astype(f32) + brecv[ck - 1, :, :, ch:2 * ch].astype(f32)
        base = base.reshape(rows, ch)
        cq = xrecv[:, :, ch + ck * cch:ch + (ck + 1) * cch].astype(f32).reshape(rows, cch).astype(bf16)
        h = base
        for k in range(NEAR, layers):
            sft = 2 ** (k - NEAR)
            if k > NEAR:
                h = base + far[:, 0:ch]
            if sft < 8:
                past = jnp.where(row >= sft, pltpu.roll(h, sft, 0), 0.0)
            else:
                past = jnp.concatenate([jnp.zeros((sft, ch), f32), h[:rows - sft]], axis=0)
            if ck == 0:
                for cp in wcopies(k):
                    cp.wait()
            a = gate(jnp.concatenate([h.astype(bf16), past.astype(bf16), cq], axis=1), k)
            dlt = jnp.dot(a, w2[k], preferred_element_type=f32)
            if k == NEAR:
                far[...] = dlt
            elif k < layers - 1:
                far[...] += dlt
            else:
                osend[ck] = (far[...] + dlt).reshape(n, per, wide).astype(TRAVEL)
        for d in order:
            to = lax.rem(me + d, n)
            push(osend.at[ck, to], recv.at[ck, me], o_send, o_recv.at[ck], d, to)

    for cp in halo_copies():
        cp.wait_send()
    for buf, sem in ((xsend.at[pl.ds(0, n - 1)], x_send), (dsend.at[pl.ds(0, n - 1)], d_send.at[0]),
                     (osend.at[:, pl.ds(0, n - 1)], o_send)):
        drain(buf, sem)
    for ck in range(1, chunks):
        drain(bsend.at[ck - 1, pl.ds(0, n - 1)], d_send.at[ck])
    for ck in range(chunks):
        drain(recv.at[ck], o_recv.at[ck])


def _finish(recv, h3, s3, hout_hbm, sout_hbm, obuf, out_sem):
    chunks, n, per, wide = recv.shape
    own, ch = h3.shape
    span = per * RES
    outs = []
    for t in range(wide // 128):
        lo = t * 128
        base, off = (h3, lo) if lo < ch else (s3, lo - ch)
        for ck in range(chunks):
            for j in range(n):
                cl = j * chunks + ck
                s, rho = cl // RES, cl % RES
                at = (ck * n + j) * per
                obuf[t, pl.ds(s * span + rho, per, RES), :] = (
                    recv[ck, j, :, lo:lo + 128].astype(f32) + base[at:at + per, off:off + 128])
        dst = hout_hbm if lo < ch else sout_hbm
        outs.append(pltpu.make_async_copy(obuf.at[t], dst.at[:, pl.ds(off, 128)], out_sem.at[t]))
        outs[-1].start()
    for cp in outs:
        cp.wait()


def solution(mesh):
    n = mesh.shape['sp']

    def local_stack(signal, cond_feats, w_now, w_past, w_cond, b_gate, w_res, w_skip):
        batch, span, ch = signal.shape
        cch = cond_feats.shape[2]
        layers = w_now.shape[0]
        sk = w_skip.shape[2]
        wide = ch + sk
        own = batch * span
        per = span // RES
        chunks = batch * RES // n
        rows = n * per
        any_spec = pl.BlockSpec(memory_space=pl.ANY)
        dma = pltpu.SemaphoreType.DMA
        sds = jax.ShapeDtypeStruct
        recv, h3, s3 = pl.pallas_call(
            functools.partial(_stack, n),
            name="stack",
            out_shape=(pltpu.VMEM((chunks, n, per, wide), TRAVEL), pltpu.VMEM((own, ch), f32), pltpu.VMEM((own, sk), f32)),
            in_specs=[any_spec] * 8,
            out_specs=(pl.BlockSpec(memory_space=pltpu.VMEM),) * 3,
            scratch_shapes=[
                pltpu.VMEM((batch, span, ch), bf16), pltpu.VMEM((batch, span, cch), bf16),
                pltpu.VMEM((batch, HALO, ch), bf16), pltpu.VMEM((batch, HALO, cch), bf16),
                pltpu.VMEM((layers, 2 * ch + cch, 2 * ch), bf16), pltpu.VMEM((layers, ch, wide), bf16),
                pltpu.VMEM((layers, 2 * ch), f32),
                pltpu.VMEM((NEAR, own, ch), bf16),
                pltpu.VMEM((own, ch), f32),
                pltpu.VMEM((n, per, ch + chunks * cch), bf16), pltpu.VMEM((n, per, ch), TRAVEL),
                pltpu.VMEM((chunks - 1, n, per, 2 * ch), bf16),
                pltpu.VMEM((n, per, ch + chunks * cch), bf16), pltpu.VMEM((n, per, ch), TRAVEL),
                pltpu.VMEM((chunks - 1, n, per, 2 * ch), bf16),
                pltpu.VMEM((rows, wide), f32), pltpu.VMEM((chunks, n, per, wide), TRAVEL),
                dma((layers, 5)), dma((3,)), dma((2,)), dma((2,)), dma, dma,
                dma((chunks,)), dma((chunks,)), dma, dma((chunks,)),
            ],
            compiler_params=pltpu.CompilerParams(collective_id=0, has_side_effects=True,
                                                 vmem_limit_bytes=56 * 1024 * 1024),
        )(signal, cond_feats, w_now, w_past, w_cond, b_gate, w_res, w_skip)
        h_out, skip_out = pl.pallas_call(
            _finish,
            name="finish",
            out_shape=(sds((own, ch), f32), sds((own, sk), f32)),
            in_specs=[pl.BlockSpec(memory_space=pltpu.VMEM)] * 3,
            out_specs=(any_spec,) * 2,
            scratch_shapes=[
                pltpu.VMEM((wide // 128, own, 128), f32), dma((wide // 128,)),
            ],
        )(*(pltpu.with_memory_space_constraint(x, pltpu.VMEM) for x in (recv, h3, s3)))
        return h_out.reshape(batch, span, ch), skip_out.reshape(batch, span, sk)

    seq_spec = P('dp', 'sp', None)
    return jax.shard_map(local_stack, mesh=mesh,
                         in_specs=(seq_spec, seq_spec, P(), P(), P(), P(), P(), P()),
                         out_specs=(seq_spec, seq_spec), check_vma=False)
```
